32 devices in a mesh: f: 8 (over z, y), h: 4 (over x, core).
Axes of the slice: x: 2, y: 2, z: 4, core: 2. Of those that a mesh axis runs over, the one named last changes fastest.
Arguments:
- x: bfloat16 [4096, 2048], P(None, 'h')
- g1: float32 [2048], P('h')
- g2: float32 [2048], P('h')
- w_gate: bfloat16 [2048, 8192], P('h', 'f')
- w_up: bfloat16 [2048, 8192], P('h', 'f')
- w_down: bfloat16 [8192, 2048], P('f', 'h')
- o: bfloat16 [4096, 2048], P(None, 'f')
- w_o: bfloat16 [2048, 2048], P('f', 'h')
- w_qkv: bfloat16 [2048, 3072], P('h', 'f')
Outputs:
- output 1: bfloat16 [4096, 2048], P(None, 'h')
- output 2: bfloat16 [4096, 3072], P(None, 'f')
All inputs are finite; a program needn't handle non-finite values.
Results may differ from the reference program's by a relative error of at most 0.00413217.
Values are sent between devices in bfloat16 or wider.
A program may use at most 1 GiB of HBM per device.

```python
import jax
import jax.numpy as jnp
from jax import lax

T = 4096
D = 2048
FF = 8192
HEADS = 32
KV_HEADS = 8
HEAD = 64
HD = HEADS * HEAD
Q = (HEADS + 2 * KV_HEADS) * HEAD
EPS = 1e-6


def _w(key, shape):
    return (jax.random.normal(key, shape, jnp.float32) * shape[0] ** -0.5).astype(jnp.bfloat16)


def setup_inputs(seed: int = 0) -> dict:
    ks = jax.random.split(jax.random.PRNGKey(seed), 11)
    z = jax.random.normal(ks[0], (T, D), jnp.float32)
    row = jnp.exp(jax.random.uniform(ks[1], (T, 1), jnp.float32, -1.0, 1.0))
    tilt = jax.random.uniform(ks[2], (T, 1), jnp.float32, -1.0, 1.0)
    pos = jnp.arange(D, dtype=jnp.float32)[None, :] * (2.0 / D) - 1.0
    x = (z * row * jnp.exp(tilt * pos)).astype(jnp.bfloat16)
    o = (0.7 * jax.random.normal(ks[8], (T, HD), jnp.float32)).astype(jnp.bfloat16)
    return {
        'x': x,
        'g1': jax.random.uniform(ks[3], (D,), jnp.float32, 0.5, 1.5),
        'g2': jax.random.uniform(ks[4], (D,), jnp.float32, 0.5, 1.5),
        'w_gate': _w(ks[5], (D, FF)),
        'w_up': _w(ks[6], (D, FF)),
        'w_down': _w(ks[7], (FF, D)),
        'o': o,
        'w_o': _w(ks[9], (HD, D)),
        'w_qkv': _w(ks[10], (D, Q)),
    }


def _norm(x, g):
    xf = x.astype(jnp.float32)
    r = lax.rsqrt(jnp.mean(xf * xf, axis=-1, keepdims=True) + EPS)
    return (xf * r * g).astype(jnp.bfloat16)


def reference(x, g1, g2, w_gate, w_up, w_down, o, w_o, w_qkv):
    n = _norm(x, g1)
    gt = jnp.dot(n, w_gate, preferred_element_type=jnp.float32)
    up = jnp.dot(n, w_up, preferred_element_type=jnp.float32)
    a = (jax.nn.silu(gt) * up).astype(jnp.bfloat16)
    y = jnp.dot(a, w_down, preferred_element_type=jnp.float32) + jnp.dot(o, w_o, preferred_element_type=jnp.float32)
    x_next = (x.astype(jnp.float32) + y).astype(jnp.bfloat16)
    n1 = _norm(x_next, g2)
    qkv = jnp.dot(n1, w_qkv, preferred_element_type=jnp.float32).astype(jnp.bfloat16)
    return (x_next, qkv)
```

```python
import jax
import jax.numpy as jnp
from jax import lax
from jax.sharding import PartitionSpec as P

EPS = 1e-6


def _dot(a, b):
    return jnp.dot(a, b, preferred_element_type=jnp.float32)


def _norm(x, g):
    xf = x.astype(jnp.float32)
    r = lax.rsqrt(jnp.mean(xf * xf, axis=-1, keepdims=True) + EPS)
    return (xf * r * g).astype(jnp.bfloat16)


def solution(mesh):
    nh, nf = mesh.shape['h'], mesh.shape['f']

    def body(x, g1, g2, w_gate, w_up, w_down, o, w_o, w_qkv):
        h = lax.axis_index('h')
        f = lax.axis_index('f')
        t = x.shape[0] // nh
        ts = t // nf
        xt = lax.all_to_all(x, 'h', split_axis=0, concat_axis=1, tiled=True)
        g1, g2 = lax.all_gather((g1, g2), 'h', axis=0, tiled=True)
        wg, wu = (lax.all_gather(w, 'h', axis=0, tiled=True) for w in (w_gate, w_up))
        wd, wo = (lax.all_gather(w, 'h', axis=1, tiled=True) for w in (w_down, w_o))
        wq = lax.all_gather(w_qkv, 'h', axis=0, tiled=True)
        n = _norm(xt, g1)
        a = (jax.nn.silu(_dot(n, wg)) * _dot(n, wu)).astype(jnp.bfloat16)
        ot = lax.dynamic_slice_in_dim(o, h * t, t, axis=0)
        y = lax.psum_scatter(_dot(a, wd) + _dot(ot, wo), 'f', scatter_dimension=0, tiled=True)
        xs = lax.dynamic_slice_in_dim(xt, f * ts, ts, axis=0)
        xn = (xs.astype(jnp.float32) + y).astype(jnp.bfloat16)
        xg = lax.all_gather(xn, 'f', axis=0, tiled=True)
        n1 = _norm(xg, g2)
        q = _dot(n1, wq).astype(jnp.bfloat16)
        x_next = lax.all_to_all(xg, 'h', split_axis=1, concat_axis=0, tiled=True)
        qkv = lax.all_gather(q, 'h', axis=0, tiled=True)
        return x_next, qkv

    in_specs = (P(None, 'h'), P('h'), P('h'), P('h', 'f'), P('h', 'f'), P('f', 'h'),
                P(None, 'f'), P('f', 'h'), P('h', 'f'))
    return jax.shard_map(body, mesh=mesh, in_specs=in_specs,
                         out_specs=(P(None, 'h'), P(None, 'f')), check_vma=False)
```

```python
import functools

import jax
import jax.numpy as jnp
from jax import lax
from jax.experimental import pallas as pl
from jax.experimental.pallas import tpu as pltpu
from jax.sharding import PartitionSpec as P

EPS = 1e-6
BF, F32 = jnp.bfloat16, jnp.float32
MESH = pl.DeviceIdType.MESH

NS = 4
NU = 16
NJ = 4
STAGES = 7


def _dot(a, b):
    return jnp.dot(a, b, preferred_element_type=F32)


def _kernel(d_model, x_ref, g1_ref, g2_ref, wg_ref, wu_ref, wd_ref, o_ref, wo_ref, wq_ref,
            outx_ref, outq_ref,
            xt, n, g1b, g2b, wg, wu, wd, wo, wq, ot, a, yb, yr, z0r, z1r, xg, nq, qb,
            loc, gs, gr, xs, xr, ws, wr, bs, br, ps, pr, qs, qr):
    f, h = lax.axis_index('f'), lax.axis_index('h')
    z, y = f // 2, f % 2
    z1, z0 = z // 2, z % 2
    xx, c = h // 2, h % 2
    pos = y * 4 + z0 * 2 + z1

    def hx(k):
        return 2 * ((xx + k // 2) % 2) + (c + k % 2) % 2

    def dev(ff, hh):
        return (ff, hh)

    ypeer = dev(z * 2 + (1 - y), h)
    z0peer = dev((z1 * 2 + (1 - z0)) * 2 + y, h)
    z1peer = dev(((1 - z1) * 2 + z0) * 2 + y, h)
    core, across = dev(f, hx(1)), dev(f, hx(2))

    def remote(src, dst, ssem, rsem, to):
        return pltpu.make_async_remote_copy(src_ref=src, dst_ref=dst, send_sem=ssem, recv_sem=rsem,
                                            device_id=to, device_id_type=MESH)

    bar = pltpu.get_barrier_semaphore()
    for k in range(1, 4):
        pl.semaphore_signal(bar, inc=1, device_id=dev(f, hx(k)), device_id_type=MESH)
    for i in range(1, 8):
        pl.semaphore_signal(bar, inc=1, device_id=dev((f + i) % 8, h), device_id_type=MESH)
    pl.semaphore_wait(bar, 10)

    jw = wg.shape[-1]

    def wcols(ref, j):
        return ref.at[:, pl.ds(j * jw, jw)]

    crows = pl.ds((f % 2) * 4, 4)

    def x_cross(k):
        return remote(x_ref.at[hx(k), f // 2, crows], xt.at[h, f // 2, crows],
                      xs.at[k], xr.at[k], dev(f, hx(k)))

    x_core = remote(x_ref.at[hx(1)], xt.at[h], xs.at[1], xr.at[1], core)
    x_cross(2).start()
    x_cross(3).start()
    gcopies = []
    for k in range(1, 4):
        gcopies.append(remote(g1_ref, g1b.at[h], gs.at[0, k], gr.at[0, k], dev(f, hx(k))))
        gcopies.append(remote(g2_ref, g2b.at[h], gs.at[1, k], gr.at[1, k], dev(f, hx(k))))
    for cp in gcopies:
        cp.start()
    x_core.start()

    def w_send(i, j, to, lane):
        src, dst = ((wg_ref, wg), (wu_ref, wu))[i]
        return remote(wcols(src, j), dst.at[j, h], ws.at[lane, i, j], wr.at[lane, i, j], to)

    def w_fwd(i, j):
        dst = (wg, wu)[i]
        return remote(dst.at[j, hx(2)], dst.at[j, hx(2)], ws.at[2, i, j], wr.at[2, i, j], core)

    big = ((wo_ref, wo), (wd_ref, wd), (wq_ref, wq))

    def b_send(i, to, lane):
        return remote(big[i][0], big[i][1].at[h], bs.at[lane, i], br.at[lane, i], to)

    def b_fwd(i):
        dst = big[i][1]
        return remote(dst.at[hx(2)], dst.at[hx(2)], bs.at[2, i], br.at[2, i], core)

    for j in range(NJ):
        for i in range(2):
            w_send(i, j, across, 0).start()
    for i in range(3):
        b_send(i, across, 0).start()

    lcopies = [pltpu.make_async_copy(x_ref.at[h], xt.at[h], loc.at[0]),
               pltpu.make_async_copy(g1_ref, g1b.at[h], loc.at[1]),
               pltpu.make_async_copy(g2_ref, g2b.at[h], loc.at[2]),
               pltpu.make_async_copy(o_ref.at[h], ot, loc.at[3])]
    for i in range(3):
        lcopies.append(pltpu.make_async_copy(big[i][0], big[i][1].at[h], loc.at[4 + i]))
    for j in range(NJ):
        lcopies.append(pltpu.make_async_copy(wcols(wg_ref, j), wg.at[j, h], loc.at[7 + 2 * j]))
        lcopies.append(pltpu.make_async_copy(wcols(wu_ref, j), wu.at[j, h], loc.at[8 + 2 * j]))
    for cp in lcopies:
        cp.start()
    for j in range(NJ):
        for i in range(2):
            w_send(i, j, core, 1).start()
    for i in range(3):
        b_send(i, core, 1).start()

    x_cross(2).wait_recv()
    x_cross(3).wait_recv()
    oth = pl.ds(2 * (1 - xx), 2)

    def x_bcast(i):
        view = xt.at[oth, f // 2, crows]
        return remote(view, view, xs.at[3 + i], xr.at[3 + i], dev((f + i) % 8, h))

    for i in range(1, 8):
        x_bcast(i).start()

    for i in range(2):
        w_send(i, 0, across, 0).wait_recv()
        w_fwd(i, 0).start()

    for cp in lcopies:
        cp.wait()
    for cp in gcopies:
        cp.wait_recv()
    x_core.wait_recv()
    for i in range(1, 8):
        x_bcast(i).wait_recv()

    dh = xt.shape[-1]
    urows = 8 * xt.shape[3]

    @pl.loop(0, NS)
    def _(s):
        blocks = [xt[b, s].reshape(urows, dh).astype(F32) for b in range(4)]
        ss = functools.reduce(jnp.add, [jnp.sum(v * v, axis=-1, keepdims=True) for v in blocks])
        r = lax.rsqrt(ss / d_model + EPS)
        for b in range(4):
            n[s, :, b * dh:(b + 1) * dh] = (blocks[b] * r * g1b[b]).astype(BF)

    for j in range(NJ):
        for i in range(2):
            if j > 0:
                w_send(i, j, across, 0).wait_recv()
                w_fwd(i, j).start()
        for i in range(2):
            w_send(i, j, core, 1).wait_recv()
            w_fwd(i, j).wait_recv()
        wgj = wg.at[j]
        wuj = wu.at[j]

        @pl.loop(0, NS)
        def _(s):
            ns = n[s]
            gt = _dot(ns, wgj[...].reshape(4 * dh, jw))
            up = _dot(ns, wuj[...].reshape(4 * dh, jw))
            a[s, :, j * jw:(j + 1) * jw] = (jax.nn.silu(gt) * up).astype(BF)

    for i in range(3):
        b_send(i, core, 1).wait_recv()

    def st_y(u):
        return remote(yb.at[u, pl.ds((1 - y) * 4, 4)], yr.at[u], ps.at[0, u], pr.at[0, u], ypeer)

    def st_z0(u):
        return remote(yb.at[u, pl.ds(y * 4 + (1 - z0) * 2, 2)], z0r.at[u], ps.at[1, u], pr.at[1, u], z0peer)

    def st_z1(u):
        return remote(yb.at[u, y * 4 + z0 * 2 + (1 - z1)], z1r.at[u], ps.at[2, u], pr.at[2, u], z1peer)

    def ag_z1(u):
        v = xg.at[u, y, pl.ds(z0 * 2 + z1, 1)]
        return remote(v, v, ps.at[3, u], pr.at[3, u], z1peer)

    def ag_y(u):
        v = xg.at[u, y, pl.ds(z0 * 2, 2)]
        return remote(v, v, ps.at[4, u], pr.at[4, u], ypeer)

    def ag_z0(u):
        v = xg.at[u, :, pl.ds(z0 * 2, 2)]
        return remote(v, v, ps.at[5, u], pr.at[5, u], z0peer)

    def out_x(u, to_h):
        return remote(xg.at[u], outx_ref.at[h * NS + u // 4], ps.at[6, u], pr.at[6, u], dev(f, to_h))

    def out_x_local(u):
        return pltpu.make_async_copy(xg.at[u], outx_ref.at[h * NS + u // 4], ps.at[6, u])

    def out_q(s, k):
        return remote(qb.at[s], outq_ref.at[h * NS + s], qs.at[k, s], qr.at[k, s], dev(f, hx(k)))

    def out_q_local(s):
        return pltpu.make_async_copy(qb.at[s], outq_ref.at[h * NS + s], qs.at[0, s])

    def at(t, lag, fn):
        u = t - lag

        @pl.when((u >= 0) & (u < NU))
        def _():
            fn(u)

    def p_compute(u):
        s, b = u // 4, hx(u % 4)

        @pl.when(u == 2)
        def _():
            for i in range(3):
                b_send(i, across, 0).wait_recv()
                b_fwd(i).start()

        @pl.when(u == 3)
        def _():
            for i in range(3):
                b_fwd(i).wait_recv()

        v = _dot(a[s], wd[b]) + _dot(ot[s], wo[b])
        yb[u] = v.reshape(yb.shape[1:])
        st_y(u).start()

    def p_y(u):
        st_y(u).wait_recv()
        rows = pl.ds(y * 4, 4)
        yb[u, rows] = yb[u, rows] + yr[u]
        st_z0(u).start()

    def p_z0(u):
        st_z0(u).wait_recv()
        rows = pl.ds(y * 4 + z0 * 2, 2)
        yb[u, rows] = yb[u, rows] + z0r[u]
        st_z1(u).start()

    def p_z1(u):
        st_z1(u).wait_recv()
        s, b = u // 4, hx(u % 4)
        v = yb[u, pos] + z1r[u]
        xg[u, y, z0 * 2 + z1] = (xt[b, s, pos].astype(F32) + v).astype(BF)
        ag_z1(u).start()

    def p_ag_z1(u):
        ag_z1(u).wait_recv()
        ag_y(u).start()

    def p_ag_y(u):
        ag_y(u).wait_recv()
        ag_z0(u).start()

    def p_out(u):
        ag_z0(u).wait_recv()

        @pl.when(u % 4 == 0)
        def _():
            out_x_local(u).start()

        @pl.when(u % 4 != 0)
        def _():
            out_x(u, hx(u % 4)).start()

        @pl.when(u % 4 == 3)
        def _():
            s = u // 4
            blocks = [xg[4 * s + k].reshape(urows, dh).astype(F32) for k in range(4)]
            ss = functools.reduce(jnp.add, [jnp.sum(v * v, axis=-1, keepdims=True) for v in blocks])
            r = lax.rsqrt(ss / d_model + EPS)
            for k in range(4):
                nq[k] = (blocks[k] * r * g2b[hx(k)]).astype(BF)
            acc = functools.reduce(jnp.add, [_dot(nq[k], wq[hx(k)]) for k in range(4)])
            qb[s] = acc.astype(BF)
            for k in (2, 3, 1):
                out_q(s, k).start()
            out_q_local(s).start()

    @pl.loop(0, NU + 8)
    def _(t):
        at(t, 0, p_compute)
        at(t, 2, p_y)
        at(t, 3, p_z0)
        at(t, 4, p_z1)
        at(t, 5, p_ag_z1)
        at(t, 6, p_ag_y)
        at(t, 7, p_out)

    for cp in gcopies:
        cp.wait_send()
    x_core.wait_send()
    x_cross(2).wait_send()
    x_cross(3).wait_send()
    for i in range(1, 8):
        x_bcast(i).wait_send()
    for j in range(NJ):
        for i in range(2):
            w_send(i, j, across, 0).wait_send()
            w_send(i, j, core, 1).wait_send()
            w_fwd(i, j).wait_send()
    for i in range(3):
        b_send(i, across, 0).wait_send()
        b_send(i, core, 1).wait_send()
        b_fwd(i).wait_send()

    @pl.loop(0, NU)
    def _(u):
        st_y(u).wait_send()
        st_z0(u).wait_send()
        st_z1(u).wait_send()
        ag_z1(u).wait_send()
        ag_y(u).wait_send()
        ag_z0(u).wait_send()

        @pl.when(u % 4 == 0)
        def _():
            out_x_local(u).wait()

        @pl.when(u % 4 != 0)
        def _():
            k = u % 4
            rows = outx_ref.at[hx(k) * NS + u // 4]
            remote(xg.at[u], rows, ps.at[6, u], pr.at[6, u], dev(f, hx(k))).wait()

    @pl.loop(0, NS)
    def _(s):
        out_q_local(s).wait()
        for k in range(1, 4):
            remote(qb.at[s], outq_ref.at[hx(k) * NS + s], qs.at[k, s], qr.at[k, s], dev(f, hx(k))).wait()


def _block(x, g1, g2, w_gate, w_up, w_down, o, w_o, w_qkv):
    tokens, dh = x.shape
    tq = tokens // 4
    ur = tq // NS
    ch = ur // 8
    ff, ko, nqk = w_gate.shape[1], o.shape[1], w_qkv.shape[1]
    jw = ff // NJ
    any_ = pl.BlockSpec(memory_space=pl.ANY)
    dma = pltpu.SemaphoreType.DMA
    scratch = [
        pltpu.VMEM((4, NS, 8, ch, dh), BF),
        pltpu.VMEM((NS, ur, 4 * dh), BF),
        pltpu.VMEM((4, 1, dh), F32),
        pltpu.VMEM((4, 1, dh), F32),
        pltpu.VMEM((NJ, 4, dh, jw), BF),
        pltpu.VMEM((NJ, 4, dh, jw), BF),
        pltpu.VMEM((4, ff, dh), BF),
        pltpu.VMEM((4, ko, dh), BF),
        pltpu.VMEM((4, dh, nqk), BF),
        pltpu.VMEM((NS, ur, ko), BF),
        pltpu.VMEM((NS, ur, ff), BF),
        pltpu.VMEM((NU, 8, ch, dh), F32),
        pltpu.VMEM((NU, 4, ch, dh), F32),
        pltpu.VMEM((NU, 2, ch, dh), F32),
        pltpu.VMEM((NU, ch, dh), F32),
        pltpu.VMEM((NU, 2, 4, ch, dh), BF),
        pltpu.VMEM((4, ur, dh), BF),
        pltpu.VMEM((NS, ur, nqk), BF),
        dma((15,)),
        dma((2, 4)), dma((2, 4)),
        dma((11,)), dma((11,)),
        dma((3, 2, NJ)), dma((3, 2, NJ)),
        dma((3, 3)), dma((3, 3)),
        dma((STAGES, NU)), dma((STAGES, NU)),
        dma((4, NS)), dma((4, NS)),
    ]
    outx, outq = pl.pallas_call(
        functools.partial(_kernel, 4 * dh),
        name="block",
        out_shape=(jax.ShapeDtypeStruct((4 * NS, 2, 4, ch, dh), BF),
                   jax.ShapeDtypeStruct((4 * NS, ur, nqk), BF)),
        in_specs=[any_] * 9,
        out_specs=(any_, any_),
        scratch_shapes=scratch,
        compiler_params=pltpu.CompilerParams(collective_id=0, has_side_effects=True,
                                             vmem_limit_bytes=67043328),
    )(x.reshape(4, NS, 8, ch, dh), g1.reshape(1, dh), g2.reshape(1, dh), w_gate, w_up, w_down,
      o.reshape(4, NS, ur, ko), w_o, w_qkv)
    return outx.reshape(tokens, dh), outq.reshape(tokens, nqk)


def solution(mesh):
    in_specs = (P(None, 'h'), P('h'), P('h'), P('h', 'f'), P('h', 'f'), P('f', 'h'),
                P(None, 'f'), P('f', 'h'), P('h', 'f'))
    return jax.shard_map(_block, mesh=mesh, in_specs=in_specs,
                         out_specs=(P(None, 'h'), P(None, 'f')), check_vma=False)
```

```python
import functools

import jax
import jax.numpy as jnp
from jax import lax
from jax.experimental import pallas as pl
from jax.experimental.pallas import tpu as pltpu
from jax.sharding import PartitionSpec as P

EPS = 1e-6
BF, F32 = jnp.bfloat16, jnp.float32
MESH = pl.DeviceIdType.MESH

NS = 4
NU = 16
NJ = 4
STAGES = 5


def _dot(a, b):
    return jnp.dot(a, b, preferred_element_type=F32)


def _kernel(d_model, x_ref, g1_ref, g2_ref, wg_ref, wu_ref, wd_ref, o_ref, wo_ref, wq_ref,
            outx_ref, outq_ref,
            xt, n, g1b, g2b, wg, wu, wd, wo, wq, ot, a, yb, yr, upr, dnr, xg, nq, qb,
            loc, gs, gr, xs, xr, ws, wr, bs, br, ps, pr, zs, zr, qs, qr):
    f, h = lax.axis_index('f'), lax.axis_index('h')
    z, y = f // 2, f % 2
    xx, c = h // 2, h % 2

    def hx(k):
        return 2 * ((xx + k // 2) % 2) + (c + k % 2) % 2

    def dev(ff, hh):
        return (ff, hh)

    ypeer = dev(z * 2 + (1 - y), h)
    above, below = dev((f + 2) % 8, h), dev((f + 6) % 8, h)
    core, across = dev(f, hx(1)), dev(f, hx(2))

    def remote(src, dst, ssem, rsem, to):
        return pltpu.make_async_remote_copy(src_ref=src, dst_ref=dst, send_sem=ssem, recv_sem=rsem,
                                            device_id=to, device_id_type=MESH)

    bar = pltpu.get_barrier_semaphore()
    for k in range(1, 4):
        pl.semaphore_signal(bar, inc=1, device_id=dev(f, hx(k)), device_id_type=MESH)
    for i in range(1, 8):
        pl.semaphore_signal(bar, inc=1, device_id=dev((f + i) % 8, h), device_id_type=MESH)
    pl.semaphore_wait(bar, 10)

    jw = wg.shape[-1]

    def wcols(ref, j):
        return ref.at[:, pl.ds(j * jw, jw)]

    crows = pl.ds((f % 2) * 4, 4)

    def x_cross(k):
        return remote(x_ref.at[hx(k), f // 2, crows], xt.at[h, f // 2, crows],
                      xs.at[k], xr.at[k], dev(f, hx(k)))

    x_core = remote(x_ref.at[hx(1)], xt.at[h], xs.at[1], xr.at[1], core)
    x_cross(2).start()
    x_cross(3).start()
    gcopies = []
    for k in range(1, 4):
        gcopies.append(remote(g1_ref, g1b.at[h], gs.at[0, k], gr.at[0, k], dev(f, hx(k))))
        gcopies.append(remote(g2_ref, g2b.at[h], gs.at[1, k], gr.at[1, k], dev(f, hx(k))))
    for cp in gcopies:
        cp.start()
    x_core.start()

    def w_send(i, j, to, lane):
        src, dst = ((wg_ref, wg), (wu_ref, wu))[i]
        return remote(wcols(src, j), dst.at[j, h], ws.at[lane, i, j], wr.at[lane, i, j], to)

    def w_fwd(i, j):
        dst = (wg, wu)[i]
        return remote(dst.at[j, hx(2)], dst.at[j, hx(2)], ws.at[2, i, j], wr.at[2, i, j], core)

    big = ((wo_ref, wo), (wd_ref, wd), (wq_ref, wq))

    def b_send(i, to, lane):
        return remote(big[i][0], big[i][1].at[h], bs.at[lane, i], br.at[lane, i], to)

    def b_fwd(i):
        dst = big[i][1]
        return remote(dst.at[hx(2)], dst.at[hx(2)], bs.at[2, i], br.at[2, i], core)

    for j in range(NJ):
        for i in range(2):
            w_send(i, j, across, 0).start()
    for i in range(3):
        b_send(i, across, 0).start()

    lcopies = [pltpu.make_async_copy(x_ref.at[h], xt.at[h], loc.at[0]),
               pltpu.make_async_copy(g1_ref, g1b.at[h], loc.at[1]),
               pltpu.make_async_copy(g2_ref, g2b.at[h], loc.at[2]),
               pltpu.make_async_copy(o_ref.at[h], ot, loc.at[3])]
    for i in range(3):
        lcopies.append(pltpu.make_async_copy(big[i][0], big[i][1].at[h], loc.at[4 + i]))
    for j in range(NJ):
        lcopies.append(pltpu.make_async_copy(wcols(wg_ref, j), wg.at[j, h], loc.at[7 + 2 * j]))
        lcopies.append(pltpu.make_async_copy(wcols(wu_ref, j), wu.at[j, h], loc.at[8 + 2 * j]))
    for cp in lcopies:
        cp.start()
    for j in range(NJ):
        for i in range(2):
            w_send(i, j, core, 1).start()
    for i in range(3):
        b_send(i, core, 1).start()

    x_cross(2).wait_recv()
    x_cross(3).wait_recv()
    oth = pl.ds(2 * (1 - xx), 2)

    def x_z(i):
        view = xt.at[oth, f // 2, crows]
        return remote(view, view, xs.at[3 + i], xr.at[3 + i], dev((f + 2 * i) % 8, h))

    def x_y(i):
        src = (f + 8 - 2 * i) % 8
        view = xt.at[oth, src // 2, pl.ds((src % 2) * 4, 4)]
        return remote(view, view, xs.at[7 + i], xr.at[7 + i], ypeer)

    for i in (1, 3, 2):
        x_z(i).start()
    x_y(0).start()
    for i in (1, 3, 2):
        x_z(i).wait_recv()
        x_y(i).start()

    for i in range(2):
        w_send(i, 0, across, 0).wait_recv()
        w_fwd(i, 0).start()

    for cp in lcopies:
        cp.wait()
    for cp in gcopies:
        cp.wait_recv()
    x_core.wait_recv()
    for i in range(4):
        x_y(i).wait_recv()

    dh = xt.shape[-1]
    urows = 8 * xt.shape[3]

    @pl.loop(0, NS)
    def _(s):
        blocks = [xt[b, s].reshape(urows, dh).astype(F32) for b in range(4)]
        ss = functools.reduce(jnp.add, [jnp.sum(v * v, axis=-1, keepdims=True) for v in blocks])
        r = lax.rsqrt(ss / d_model + EPS)
        for b in range(4):
            n[s, :, b * dh:(b + 1) * dh] = (blocks[b] * r * g1b[b]).astype(BF)

    for j in range(NJ):
        for i in range(2):
            if j > 0:
                w_send(i, j, across, 0).wait_recv()
                w_fwd(i, j).start()
        for i in range(2):
            w_send(i, j, core, 1).wait_recv()
            w_fwd(i, j).wait_recv()
        wgj = wg.at[j]
        wuj = wu.at[j]

        @pl.loop(0, NS)
        def _(s):
            ns = n[s]
            gt = _dot(ns, wgj[...].reshape(4 * dh, jw))
            up = _dot(ns, wuj[...].reshape(4 * dh, jw))
            a[s, :, j * jw:(j + 1) * jw] = (jax.nn.silu(gt) * up).astype(BF)

    for i in range(3):
        b_send(i, core, 1).wait_recv()

    def st_y(u):
        return remote(yb.at[u, pl.ds((1 - y) * 4, 4)], yr.at[u], ps.at[0, u], pr.at[0, u], ypeer)

    def st_up(u, zz):
        return remote(yb.at[u, pl.ds(y * 4 + zz + 1, 3 - zz)], upr.at[u, pl.ds(zz, 3 - zz)],
                      ps.at[1, u], pr.at[1, u], above)

    def st_dn(u, zz):
        return remote(yb.at[u, pl.ds(y * 4, zz)], dnr.at[u, pl.ds(0, zz)],
                      ps.at[2, u], pr.at[2, u], below)

    def ag_y(u):
        v = xg.at[u, y, pl.ds(z, 1)]
        return remote(v, v, ps.at[3, u], pr.at[3, u], ypeer)

    def ag_z(u, src, way):
        v = xg.at[u, :, pl.ds(src, 1)]
        return remote(v, v, zs.at[way, u, src], zr.at[u, src], (above, below)[way])

    def out_x(u, to_h):
        return remote(xg.at[u], outx_ref.at[h * NS + u // 4], ps.at[4, u], pr.at[4, u], dev(f, to_h))

    def out_x_local(u):
        return pltpu.make_async_copy(xg.at[u], outx_ref.at[h * NS + u // 4], ps.at[4, u])

    def out_q(s, k):
        return remote(qb.at[s], outq_ref.at[h * NS + s], qs.at[k, s], qr.at[k, s], dev(f, hx(k)))

    def out_q_local(s):
        return pltpu.make_async_copy(qb.at[s], outq_ref.at[h * NS + s], qs.at[0, s])

    def at(t, lag, fn):
        u = t - lag

        @pl.when((u >= 0) & (u < NU))
        def _():
            fn(u)

    def p_compute(u):
        s, b = u // 4, hx(u % 4)

        @pl.when(u == 2)
        def _():
            for i in range(3):
                b_send(i, across, 0).wait_recv()
                b_fwd(i).start()

        @pl.when(u == 3)
        def _():
            for i in range(3):
                b_fwd(i).wait_recv()

        v = _dot(a[s], wd[b]) + _dot(ot[s], wo[b])
        yb[u] = v.reshape(yb.shape[1:])
        st_y(u).start()

    def send_up(u, zz):
        @pl.when(z == zz)
        def _():
            if zz > 0:
                st_up(u, zz - 1).wait_recv()
                for q in range(zz + 1, 4):
                    yb[u, y * 4 + q] = yb[u, y * 4 + q] + upr[u, q - 1]
            st_up(u, zz).start()

    def send_dn(u, zz):
        @pl.when(z == zz)
        def _():
            if zz < 3:
                st_dn(u, zz + 1).wait_recv()
                for q in range(zz):
                    yb[u, y * 4 + q] = yb[u, y * 4 + q] + dnr[u, q]
            st_dn(u, zz).start()

    def p_y(u):
        st_y(u).wait_recv()
        rows = pl.ds(y * 4, 4)
        yb[u, rows] = yb[u, rows] + yr[u]
        send_up(u, 0)
        send_dn(u, 3)

    def p_h2(u):
        send_up(u, 1)
        send_dn(u, 2)

    def p_h3(u):
        send_up(u, 2)
        send_dn(u, 1)

    def p_fin(u):
        s, b = u // 4, hx(u % 4)
        own = xt[b, s, y * 4 + z].astype(F32)

        @pl.when(z == 0)
        def _():
            st_dn(u, 1).wait_recv()
            xg[u, y, 0] = (own + (yb[u, y * 4] + dnr[u, 0])).astype(BF)

        @pl.when(z == 3)
        def _():
            st_up(u, 2).wait_recv()
            xg[u, y, 3] = (own + (yb[u, y * 4 + 3] + upr[u, 2])).astype(BF)

        @pl.when((z == 1) | (z == 2))
        def _():
            v = yb[u, y * 4 + z] + upr[u, z - 1] + dnr[u, z]
            xg[u, y, z] = (own + v).astype(BF)

        ag_y(u).start()

    def p_g1(u):
        ag_y(u).wait_recv()

        @pl.when(z < 3)
        def _():
            ag_z(u, z, 0).start()

        @pl.when(z > 0)
        def _():
            ag_z(u, z, 1).start()

    def p_fwd(u, d):
        @pl.when(z >= d)
        def _():
            ag_z(u, z - d, 0).wait_recv()

        @pl.when((z >= d) & (z < 3))
        def _():
            ag_z(u, z - d, 0).start()

        @pl.when(z + d <= 3)
        def _():
            ag_z(u, z + d, 1).wait_recv()

        @pl.when((z + d <= 3) & (z > 0))
        def _():
            ag_z(u, z + d, 1).start()

    def p_g2(u):
        p_fwd(u, 1)

    def p_g3(u):
        p_fwd(u, 2)

    def p_out(u):
        p_fwd(u, 3)

        @pl.when(u % 4 == 0)
        def _():
            out_x_local(u).start()

        @pl.when(u % 4 != 0)
        def _():
            out_x(u, hx(u % 4)).start()

        @pl.when(u % 4 == 3)
        def _():
            s = u // 4
            blocks = [xg[4 * s + k].reshape(urows, dh).astype(F32) for k in range(4)]
            ss = functools.reduce(jnp.add, [jnp.sum(v * v, axis=-1, keepdims=True) for v in blocks])
            r = lax.rsqrt(ss / d_model + EPS)
            for k in range(4):
                nq[k] = (blocks[k] * r * g2b[hx(k)]).astype(BF)
            acc = functools.reduce(jnp.add, [_dot(nq[k], wq[hx(k)]) for k in range(4)])
            qb[s] = acc.astype(BF)
            for k in (2, 1):
                out_q(s, k).start()
            out_q_local(s).start()

    def out_q_from(s, k):
        rows = outq_ref.at[hx(k) * NS + s]
        return remote(qb.at[s], rows, qs.at[k, s], qr.at[k, s], dev(f, hx(k)))

    def q_fwd(s):
        rows = outq_ref.at[hx(2) * NS + s]
        return remote(rows, rows, qs.at[3, s], qr.at[3, s], core)

    def p_q(u):
        @pl.when(u % 4 == 3)
        def _():
            out_q_from(u // 4, 2).wait_recv()
            q_fwd(u // 4).start()

    @pl.loop(0, NU + 10)
    def _(t):
        for lag, fn in ((0, p_compute), (2, p_y), (3, p_h2), (4, p_h3), (5, p_fin), (6, p_g1),
                        (7, p_g2), (8, p_g3), (9, p_out), (10, p_q)):
            at(t, lag, fn)

    for cp in gcopies:
        cp.wait_send()
    x_core.wait_send()
    x_cross(2).wait_send()
    x_cross(3).wait_send()
    for i in range(4):
        x_y(i).wait_send()
    for i in range(1, 4):
        x_z(i).wait_send()
    for j in range(NJ):
        for i in range(2):
            w_send(i, j, across, 0).wait_send()
            w_send(i, j, core, 1).wait_send()
            w_fwd(i, j).wait_send()
    for i in range(3):
        b_send(i, across, 0).wait_send()
        b_send(i, core, 1).wait_send()
        b_fwd(i).wait_send()

    @pl.loop(0, NU)
    def _(u):
        st_y(u).wait_send()
        for zz in range(3):
            @pl.when(z == zz)
            def _():
                st_up(u, zz).wait_send()

            @pl.when(z == zz + 1)
            def _():
                st_dn(u, zz + 1).wait_send()

        ag_y(u).wait_send()
        for d in range(3):
            @pl.when((z >= d) & (z < 3))
            def _():
                ag_z(u, z - d, 0).wait_send()

            @pl.when((z + d <= 3) & (z > 0))
            def _():
                ag_z(u, z + d, 1).wait_send()

        @pl.when(u % 4 == 0)
        def _():
            out_x_local(u).wait()

        @pl.when(u % 4 != 0)
        def _():
            k = u % 4
            rows = outx_ref.at[hx(k) * NS + u // 4]
            remote(xg.at[u], rows, ps.at[4, u], pr.at[4, u], dev(f, hx(k))).wait()

    @pl.loop(0, NS)
    def _(s):
        out_q_local(s).wait()
        out_q_from(s, 1).wait()
        out_q_from(s, 2).wait_send()
        q_fwd(s).wait_send()
        out_q_from(s, 3).wait_recv()


def _block(x, g1, g2, w_gate, w_up, w_down, o, w_o, w_qkv):
    tokens, dh = x.shape
    tq = tokens // 4
    ur = tq // NS
    ch = ur // 8
    ff, ko, nqk = w_gate.shape[1], o.shape[1], w_qkv.shape[1]
    jw = ff // NJ
    any_ = pl.BlockSpec(memory_space=pl.ANY)
    dma = pltpu.SemaphoreType.DMA
    scratch = [
        pltpu.VMEM((4, NS, 8, ch, dh), BF),
        pltpu.VMEM((NS, ur, 4 * dh), BF),
        pltpu.VMEM((4, 1, dh), F32),
        pltpu.VMEM((4, 1, dh), F32),
        pltpu.VMEM((NJ, 4, dh, jw), BF),
        pltpu.VMEM((NJ, 4, dh, jw), BF),
        pltpu.VMEM((4, ff, dh), BF),
        pltpu.VMEM((4, ko, dh), BF),
        pltpu.VMEM((4, dh, nqk), BF),
        pltpu.VMEM((NS, ur, ko), BF),
        pltpu.VMEM((NS, ur, ff), BF),
        pltpu.VMEM((NU, 8, ch, dh), F32),
        pltpu.VMEM((NU, 4, ch, dh), F32),
        pltpu.VMEM((NU, 3, ch, dh), F32),
        pltpu.VMEM((NU, 3, ch, dh), F32),
        pltpu.VMEM((NU, 2, 4, ch, dh), BF),
        pltpu.VMEM((4, ur, dh), BF),
        pltpu.VMEM((NS, ur, nqk), BF),
        dma((15,)),
        dma((2, 4)), dma((2, 4)),
        dma((11,)), dma((11,)),
        dma((3, 2, NJ)), dma((3, 2, NJ)),
        dma((3, 3)), dma((3, 3)),
        dma((STAGES, NU)), dma((STAGES, NU)),
        dma((2, NU, 4)), dma((NU, 4)),
        dma((4, NS)), dma((4, NS)),
    ]
    outx, outq = pl.pallas_call(
        functools.partial(_kernel, 4 * dh),
        name="block",
        out_shape=(jax.ShapeDtypeStruct((4 * NS, 2, 4, ch, dh), BF),
                   jax.ShapeDtypeStruct((4 * NS, ur, nqk), BF)),
        in_specs=[any_] * 9,
        out_specs=(any_, any_),
        scratch_shapes=scratch,
        compiler_params=pltpu.CompilerParams(collective_id=0, has_side_effects=True,
                                             vmem_limit_bytes=67043328),
    )(x.reshape(4, NS, 8, ch, dh), g1.reshape(1, dh), g2.reshape(1, dh), w_gate, w_up, w_down,
      o.reshape(4, NS, ur, ko), w_o, w_qkv)
    return outx.reshape(tokens, dh), outq.reshape(tokens, nqk)


def solution(mesh):
    in_specs = (P(None, 'h'), P('h'), P('h'), P('h', 'f'), P('h', 'f'), P('f', 'h'),
                P(None, 'f'), P('f', 'h'), P('h', 'f'))
    return jax.shard_map(_block, mesh=mesh, in_specs=in_specs,
                         out_specs=(P(None, 'h'), P(None, 'f')), check_vma=False)
```

```python
import functools

import jax
import jax.numpy as jnp
from jax import lax
from jax.experimental import pallas as pl
from jax.experimental.pallas import tpu as pltpu
from jax.sharding import PartitionSpec as P

EPS = 1e-6
BF, F32 = jnp.bfloat16, jnp.float32
MESH = pl.DeviceIdType.MESH

NS = 8
NU = 32
NE = 6
NJ = 4
STAGES = 5


def _dot(a, b):
    return jnp.dot(a, b, preferred_element_type=F32)


def _kernel(d_model, x_ref, g1_ref, g2_ref, wg_ref, wu_ref, wd_ref, o_ref, wo_ref, wq_ref,
            outx_ref, outq_ref,
            xt, n, g1b, g2b, wg, wu, wd, wo, wq, ot, a, yb, yr, upr, dnr, xg, nq, qb,
            loc, gs, gr, xs, xr, ws, wr, bs, br, ps, pr, zs, zr, qs, qr):
    f, h = lax.axis_index('f'), lax.axis_index('h')
    z, y = f // 2, f % 2
    xx, c = h // 2, h % 2

    def hx(k):
        return 2 * ((xx + k // 2) % 2) + (c + k % 2) % 2

    def dev(ff, hh):
        return (ff, hh)

    ypeer = dev(z * 2 + (1 - y), h)
    above, below = dev((f + 2) % 8, h), dev((f + 6) % 8, h)
    core, across = dev(f, hx(1)), dev(f, hx(2))

    def remote(src, dst, ssem, rsem, to):
        return pltpu.make_async_remote_copy(src_ref=src, dst_ref=dst, send_sem=ssem, recv_sem=rsem,
                                            device_id=to, device_id_type=MESH)

    bar = pltpu.get_barrier_semaphore()
    for k in range(1, 4):
        pl.semaphore_signal(bar, inc=1, device_id=dev(f, hx(k)), device_id_type=MESH)
    for i in range(1, 8):
        pl.semaphore_signal(bar, inc=1, device_id=dev((f + i) % 8, h), device_id_type=MESH)
    pl.semaphore_wait(bar, 10)

    jw = wg.shape[-1]

    def wcols(ref, j):
        return ref.at[:, pl.ds(j * jw, jw)]


    def x_cross(k):
        return remote(x_ref.at[hx(k), f], xt.at[h, f],
                      xs.at[k], xr.at[k], dev(f, hx(k)))

    x_core = remote(x_ref.at[hx(1)], xt.at[h], xs.at[1], xr.at[1], core)
    x_cross(2).start()
    x_cross(3).start()
    gcopies = []
    for k in range(1, 4):
        gcopies.append(remote(g1_ref, g1b.at[h], gs.at[0, k], gr.at[0, k], dev(f, hx(k))))
        gcopies.append(remote(g2_ref, g2b.at[h], gs.at[1, k], gr.at[1, k], dev(f, hx(k))))
    for cp in gcopies:
        cp.start()
    x_core.start()

    def w_send(i, j, to, lane):
        src, dst = ((wg_ref, wg), (wu_ref, wu))[i]
        return remote(wcols(src, j), dst.at[j, h], ws.at[lane, i, j], wr.at[lane, i, j], to)

    def w_fwd(i, j):
        dst = (wg, wu)[i]
        return remote(dst.at[j, hx(2)], dst.at[j, hx(2)], ws.at[2, i, j], wr.at[2, i, j], core)

    big = ((wo_ref, wo), (wd_ref, wd), (wq_ref, wq))

    def b_send(i, to, lane):
        return remote(big[i][0], big[i][1].at[h], bs.at[lane, i], br.at[lane, i], to)

    def b_fwd(i):
        dst = big[i][1]
        return remote(dst.at[hx(2)], dst.at[hx(2)], bs.at[2, i], br.at[2, i], core)

    for j in range(NJ):
        for i in range(2):
            w_send(i, j, across, 0).start()
    for i in range(3):
        b_send(i, across, 0).start()

    lcopies = [pltpu.make_async_copy(x_ref.at[h], xt.at[h], loc.at[0]),
               pltpu.make_async_copy(g1_ref, g1b.at[h], loc.at[1]),
               pltpu.make_async_copy(g2_ref, g2b.at[h], loc.at[2]),
               pltpu.make_async_copy(o_ref.at[h], ot, loc.at[3])]
    for i in range(3):
        lcopies.append(pltpu.make_async_copy(big[i][0], big[i][1].at[h], loc.at[4 + i]))
    for j in range(NJ):
        lcopies.append(pltpu.make_async_copy(wcols(wg_ref, j), wg.at[j, h], loc.at[7 + 2 * j]))
        lcopies.append(pltpu.make_async_copy(wcols(wu_ref, j), wu.at[j, h], loc.at[8 + 2 * j]))
    for cp in lcopies:
        cp.start()
    for j in range(NJ):
        for i in range(2):
            w_send(i, j, core, 1).start()
    for i in range(3):
        b_send(i, core, 1).start()

    x_cross(2).wait_recv()
    x_cross(3).wait_recv()
    oth = pl.ds(2 * (1 - xx), 2)

    def x_z(i):
        view = xt.at[oth, f]
        return remote(view, view, xs.at[3 + i], xr.at[3 + i], dev((f + 2 * i) % 8, h))

    def x_y(i):
        src = (f + 8 - 2 * i) % 8
        view = xt.at[oth, src]
        return remote(view, view, xs.at[7 + i], xr.at[7 + i], ypeer)

    for i in (1, 3, 2):
        x_z(i).start()
    x_y(0).start()
    for i in (1, 3, 2):
        x_z(i).wait_recv()
        x_y(i).start()

    for i in range(2):
        w_send(i, 0, across, 0).wait_recv()
        w_fwd(i, 0).start()

    for cp in lcopies:
        cp.wait()
    for cp in gcopies:
        cp.wait_recv()
    x_core.wait_recv()
    for i in range(4):
        x_y(i).wait_recv()

    dh = xt.shape[-1]
    urows = 8 * xt.shape[3]

    @pl.loop(0, NS)
    def _(s):
        blocks = [xt[b, s].reshape(urows, dh).astype(F32) for b in range(4)]
        ss = functools.reduce(jnp.add, [jnp.sum(v * v, axis=-1, keepdims=True) for v in blocks])
        r = lax.rsqrt(ss / d_model + EPS)
        for b in range(4):
            n[s, :, b * dh:(b + 1) * dh] = (blocks[b] * r * g1b[b]).astype(BF)

    for j in range(NJ):
        for i in range(2):
            if j > 0:
                w_send(i, j, across, 0).wait_recv()
                w_fwd(i, j).start()
        for i in range(2):
            w_send(i, j, core, 1).wait_recv()
            w_fwd(i, j).wait_recv()
        wgj = wg.at[j]
        wuj = wu.at[j]

        @pl.loop(0, NS // 2)
        def _(i):
            ns = n[pl.ds(2 * i, 2)].reshape(2 * urows, 4 * dh)
            gt = _dot(ns, wgj[...].reshape(4 * dh, jw))
            up = _dot(ns, wuj[...].reshape(4 * dh, jw))
            v = (jax.nn.silu(gt) * up).astype(BF)
            a[pl.ds(2 * i, 2), :, j * jw:(j + 1) * jw] = v.reshape(2, urows, jw)

    for i in range(3):
        b_send(i, core, 1).wait_recv()

    def st_y(u):
        return remote(yb.at[u, pl.ds((1 - y) * 4, 4)], yr.at[u], ps.at[0, u], pr.at[0, u], ypeer)

    def st_up(u, zz):
        return remote(yb.at[u, pl.ds(y * 4 + zz + 1, 3 - zz)], upr.at[u, pl.ds(zz, 3 - zz)],
                      ps.at[1, u], pr.at[1, u], above)

    def st_dn(u, zz):
        return remote(yb.at[u, pl.ds(y * 4, zz)], dnr.at[u, pl.ds(0, zz)],
                      ps.at[2, u], pr.at[2, u], below)

    def ag_y(u):
        v = xg.at[u, y, pl.ds(z, 1)]
        return remote(v, v, ps.at[3, u], pr.at[3, u], ypeer)

    def ag_z(u, src, way):
        v = xg.at[u, :, pl.ds(src, 1)]
        return remote(v, v, zs.at[way, u, src], zr.at[u, src], (above, below)[way])

    def out_x(u, to_h):
        return remote(xg.at[u], outx_ref.at[h * NS + u // 4], ps.at[4, u], pr.at[4, u], dev(f, to_h))

    def out_x_local(u):
        return pltpu.make_async_copy(xg.at[u], outx_ref.at[h * NS + u // 4], ps.at[4, u])

    def out_q(s, k):
        return remote(qb.at[s], outq_ref.at[h * NS + s], qs.at[k, s], qr.at[k, s], dev(f, hx(k)))

    def out_q_local(s):
        return pltpu.make_async_copy(qb.at[s], outq_ref.at[h * NS + s], qs.at[0, s])

    def at(t, lag, fn):
        i = t - lag

        @pl.when((i >= 0) & (i < NU))
        def _():
            late = i // (4 * NE)
            s = (1 - late) * ((i % (2 * NE)) // 2) + late * (i // 4)
            k = (1 - late) * (2 * (i // (2 * NE)) + i % 2) + late * ((i + 2) % 4)
            fn(4 * s + k)

    def p_compute(u):
        s, b = u // 4, hx(u % 4)

        @pl.when(u == 2)
        def _():
            for i in range(2):
                b_send(i, across, 0).wait_recv()
                b_fwd(i).start()

        @pl.when(u == 3)
        def _():
            for i in range(2):
                b_fwd(i).wait_recv()

        v = _dot(a[s], wd[b]) + _dot(ot[s], wo[b])
        yb[u] = v.reshape(yb.shape[1:])
        st_y(u).start()

    def send_up(u, zz):
        @pl.when(z == zz)
        def _():
            if zz > 0:
                st_up(u, zz - 1).wait_recv()
                for q in range(zz + 1, 4):
                    yb[u, y * 4 + q] = yb[u, y * 4 + q] + upr[u, q - 1]
            st_up(u, zz).start()

    def send_dn(u, zz):
        @pl.when(z == zz)
        def _():
            if zz < 3:
                st_dn(u, zz + 1).wait_recv()
                for q in range(zz):
                    yb[u, y * 4 + q] = yb[u, y * 4 + q] + dnr[u, q]
            st_dn(u, zz).start()

    def p_y(u):
        st_y(u).wait_recv()
        rows = pl.ds(y * 4, 4)
        yb[u, rows] = yb[u, rows] + yr[u]
        send_up(u, 0)
        send_dn(u, 3)

    def p_h2(u):
        send_up(u, 1)
        send_dn(u, 2)

    def p_h3(u):
        send_up(u, 2)
        send_dn(u, 1)

    def p_fin(u):
        s, b = u // 4, hx(u % 4)
        own = xt[b, s, y * 4 + z].astype(F32)

        @pl.when(z == 0)
        def _():
            st_dn(u, 1).wait_recv()
            xg[u, y, 0] = (own + (yb[u, y * 4] + dnr[u, 0])).astype(BF)

        @pl.when(z == 3)
        def _():
            st_up(u, 2).wait_recv()
            xg[u, y, 3] = (own + (yb[u, y * 4 + 3] + upr[u, 2])).astype(BF)

        @pl.when((z == 1) | (z == 2))
        def _():
            v = yb[u, y * 4 + z] + upr[u, z - 1] + dnr[u, z]
            xg[u, y, z] = (own + v).astype(BF)

        ag_y(u).start()

    def p_g1(u):
        @pl.when(u == 3)
        def _():
            b_send(2, across, 0).wait_recv()
            b_fwd(2).start()

        ag_y(u).wait_recv()

        @pl.when(z < 3)
        def _():
            ag_z(u, z, 0).start()

        @pl.when(z > 0)
        def _():
            ag_z(u, z, 1).start()

    def p_fwd(u, d):
        @pl.when(z >= d)
        def _():
            ag_z(u, z - d, 0).wait_recv()

        @pl.when((z >= d) & (z < 3))
        def _():
            ag_z(u, z - d, 0).start()

        @pl.when(z + d <= 3)
        def _():
            ag_z(u, z + d, 1).wait_recv()

        @pl.when((z + d <= 3) & (z > 0))
        def _():
            ag_z(u, z + d, 1).start()

    def p_g2(u):
        p_fwd(u, 1)

    def p_g3(u):
        p_fwd(u, 2)

    def done(u):
        return ((u % 4 == 3) & (u < 4 * NE)) | ((u % 4 == 1) & (u >= 4 * NE))

    def p_out(u):
        p_fwd(u, 3)

        @pl.when(u == 3)
        def _():
            b_fwd(2).wait_recv()

        @pl.when(u % 4 == 0)
        def _():
            out_x_local(u).start()

        @pl.when(u % 4 != 0)
        def _():
            out_x(u, hx(u % 4)).start()

        @pl.when(done(u))
        def _():
            s = u // 4
            blocks = [xg[4 * s + k].reshape(urows, dh).astype(F32) for k in range(4)]
            ss = functools.reduce(jnp.add, [jnp.sum(v * v, axis=-1, keepdims=True) for v in blocks])
            r = lax.rsqrt(ss / d_model + EPS)
            for k in range(4):
                nq[k] = (blocks[k] * r * g2b[hx(k)]).astype(BF)
            acc = functools.reduce(jnp.add, [_dot(nq[k], wq[hx(k)]) for k in range(4)])
            qb[s] = acc.astype(BF)
            for k in (2, 1):
                out_q(s, k).start()
            out_q_local(s).start()

    def out_q_from(s, k):
        rows = outq_ref.at[hx(k) * NS + s]
        return remote(qb.at[s], rows, qs.at[k, s], qr.at[k, s], dev(f, hx(k)))

    def q_fwd(s):
        rows = outq_ref.at[hx(2) * NS + s]
        return remote(rows, rows, qs.at[3, s], qr.at[3, s], core)

    def p_q(u):
        @pl.when(done(u))
        def _():
            out_q_from(u // 4, 2).wait_recv()
            q_fwd(u // 4).start()

    @pl.loop(0, NU + 10)
    def _(t):
        for lag, fn in ((0, p_compute), (2, p_y), (3, p_h2), (4, p_h3), (5, p_fin), (6, p_g1),
                        (7, p_g2), (8, p_g3), (9, p_out), (10, p_q)):
            at(t, lag, fn)

    for cp in gcopies:
        cp.wait_send()
    x_core.wait_send()
    x_cross(2).wait_send()
    x_cross(3).wait_send()
    for i in range(4):
        x_y(i).wait_send()
    for i in range(1, 4):
        x_z(i).wait_send()
    for j in range(NJ):
        for i in range(2):
            w_send(i, j, across, 0).wait_send()
            w_send(i, j, core, 1).wait_send()
            w_fwd(i, j).wait_send()
    for i in range(3):
        b_send(i, across, 0).wait_send()
        b_send(i, core, 1).wait_send()
        b_fwd(i).wait_send()

    @pl.loop(0, NU)
    def _(u):
        st_y(u).wait_send()
        for zz in range(3):
            @pl.when(z == zz)
            def _():
                st_up(u, zz).wait_send()

            @pl.when(z == zz + 1)
            def _():
                st_dn(u, zz + 1).wait_send()

        ag_y(u).wait_send()
        for d in range(3):
            @pl.when((z >= d) & (z < 3))
            def _():
                ag_z(u, z - d, 0).wait_send()

            @pl.when((z + d <= 3) & (z > 0))
            def _():
                ag_z(u, z + d, 1).wait_send()

        @pl.when(u % 4 == 0)
        def _():
            out_x_local(u).wait()

        @pl.when(u % 4 != 0)
        def _():
            k = u % 4
            rows = outx_ref.at[hx(k) * NS + u // 4]
            remote(xg.at[u], rows, ps.at[4, u], pr.at[4, u], dev(f, hx(k))).wait()

    @pl.loop(0, NS)
    def _(s):
        out_q_local(s).wait()
        out_q_from(s, 1).wait()
        out_q_from(s, 2).wait_send()
        q_fwd(s).wait_send()
        out_q_from(s, 3).wait_recv()


def _block(x, g1, g2, w_gate, w_up, w_down, o, w_o, w_qkv):
    tokens, dh = x.shape
    tq = tokens // 4
    ur = tq // NS
    ch = ur // 8
    ff, ko, nqk = w_gate.shape[1], o.shape[1], w_qkv.shape[1]
    jw = ff // NJ
    any_ = pl.BlockSpec(memory_space=pl.ANY)
    dma = pltpu.SemaphoreType.DMA
    scratch = [
        pltpu.VMEM((4, NS, 8, ch, dh), BF),
        pltpu.VMEM((NS, ur, 4 * dh), BF),
        pltpu.VMEM((4, 1, dh), F32),
        pltpu.VMEM((4, 1, dh), F32),
        pltpu.VMEM((NJ, 4, dh, jw), BF),
        pltpu.VMEM((NJ, 4, dh, jw), BF),
        pltpu.VMEM((4, ff, dh), BF),
        pltpu.VMEM((4, ko, dh), BF),
        pltpu.VMEM((4, dh, nqk), BF),
        pltpu.VMEM((NS, ur, ko), BF),
        pltpu.VMEM((NS, ur, ff), BF),
        pltpu.VMEM((NU, 8, ch, dh), F32),
        pltpu.VMEM((NU, 4, ch, dh), F32),
        pltpu.VMEM((NU, 3, ch, dh), F32),
        pltpu.VMEM((NU, 3, ch, dh), F32),
        pltpu.VMEM((NU, 2, 4, ch, dh), BF),
        pltpu.VMEM((4, ur, dh), BF),
        pltpu.VMEM((NS, ur, nqk), BF),
        dma((15,)),
        dma((2, 4)), dma((2, 4)),
        dma((11,)), dma((11,)),
        dma((3, 2, NJ)), dma((3, 2, NJ)),
        dma((3, 3)), dma((3, 3)),
        dma((STAGES, NU)), dma((STAGES, NU)),
        dma((2, NU, 4)), dma((NU, 4)),
        dma((4, NS)), dma((4, NS)),
    ]
    outx, outq = pl.pallas_call(
        functools.partial(_kernel, 4 * dh),
        name="block",
        out_shape=(pltpu.VMEM((4 * NS, 2, 4, ch, dh), BF),
                   pltpu.VMEM((4 * NS, ur, nqk), BF)),
        in_specs=[any_] * 9,
        out_specs=(any_, any_),
        scratch_shapes=scratch,
        compiler_params=pltpu.CompilerParams(collective_id=0, has_side_effects=True,
                                             vmem_limit_bytes=56 * 2**20),
    )(x.reshape(4, NS, 8, ch, dh), g1.reshape(1, dh), g2.reshape(1, dh), w_gate, w_up, w_down,
      o.reshape(4, NS, ur, ko), w_o, w_qkv)
    return outx.reshape(tokens, dh), outq.reshape(tokens, nqk)


def solution(mesh):
    in_specs = (P(None, 'h'), P('h'), P('h'), P('h', 'f'), P('h', 'f'), P('f', 'h'),
                P(None, 'f'), P('f', 'h'), P('h', 'f'))
    return jax.shard_map(_block, mesh=mesh, in_specs=in_specs,
                         out_specs=(P(None, 'h'), P(None, 'f')), check_vma=False)
```

```python
import functools

import jax
import jax.numpy as jnp
from jax import lax
from jax.experimental import pallas as pl
from jax.experimental.pallas import tpu as pltpu
from jax.sharding import PartitionSpec as P

EPS = 1e-6
BF, F32 = jnp.bfloat16, jnp.float32
MESH = pl.DeviceIdType.MESH

NS = 8
NU = 32
NE = 6
NJ = 4
STAGES = 5


def _dot(a, b):
    return jnp.dot(a, b, preferred_element_type=F32)


def _kernel(d_model, x_ref, g1_ref, g2_ref, wg_ref, wu_ref, wd_ref, o_ref, wo_ref, wq_ref,
            outx_ref, outq_ref,
            xt, n, g1b, g2b, wg, wu, wd, wo, wq, ot, a, yb, yr, upr, dnr, xg, nq, qb,
            loc, gs, gr, xs, xr, ws, wr, bs, br, ps, pr, zs, zr, qs, qr):
    f, h = lax.axis_index('f'), lax.axis_index('h')
    z, y = f // 2, f % 2
    xx, c = h // 2, h % 2

    def hx(k):
        return 2 * ((xx + k // 2) % 2) + (c + k % 2) % 2

    def dev(ff, hh):
        return (ff, hh)

    ypeer = dev(z * 2 + (1 - y), h)
    above, below = dev((f + 2) % 8, h), dev((f + 6) % 8, h)
    core, across = dev(f, hx(1)), dev(f, hx(2))

    def remote(src, dst, ssem, rsem, to):
        return pltpu.make_async_remote_copy(src_ref=src, dst_ref=dst, send_sem=ssem, recv_sem=rsem,
                                            device_id=to, device_id_type=MESH)

    bar = pltpu.get_barrier_semaphore()
    for k in range(1, 4):
        pl.semaphore_signal(bar, inc=1, device_id=dev(f, hx(k)), device_id_type=MESH)
    for i in range(1, 8):
        pl.semaphore_signal(bar, inc=1, device_id=dev((f + i) % 8, h), device_id_type=MESH)
    pl.semaphore_wait(bar, 10)

    jw = wg.shape[-1]

    def wcols(ref, j):
        return ref.at[:, pl.ds(j * jw, jw)]


    def x_cross(k):
        return remote(x_ref.at[hx(k), f], xt.at[h, f],
                      xs.at[k], xr.at[k], dev(f, hx(k)))

    x_core = remote(x_ref.at[hx(1)], xt.at[h], xs.at[1], xr.at[1], core)
    x_cross(2).start()
    x_cross(3).start()
    gcopies = []
    for k in range(1, 4):
        gcopies.append(remote(g1_ref, g1b.at[h], gs.at[0, k], gr.at[0, k], dev(f, hx(k))))
        gcopies.append(remote(g2_ref, g2b.at[h], gs.at[1, k], gr.at[1, k], dev(f, hx(k))))
    for cp in gcopies:
        cp.start()
    x_core.start()

    def w_send(i, j, to, lane):
        src, dst = ((wg_ref, wg), (wu_ref, wu))[i]
        return remote(wcols(src, j), dst.at[j, h], ws.at[lane, i, j], wr.at[lane, i, j], to)

    def w_fwd(i, j):
        dst = (wg, wu)[i]
        return remote(dst.at[j, hx(2)], dst.at[j, hx(2)], ws.at[2, i, j], wr.at[2, i, j], core)

    big = ((wo_ref, wo), (wd_ref, wd), (wq_ref, wq))

    def b_send(i, to, lane):
        return remote(big[i][0], big[i][1].at[h], bs.at[lane, i], br.at[lane, i], to)

    def b_fwd(i):
        dst = big[i][1]
        return remote(dst.at[hx(2)], dst.at[hx(2)], bs.at[2, i], br.at[2, i], core)

    for j in range(NJ):
        for i in range(2):
            w_send(i, j, across, 0).start()
    for i in range(3):
        b_send(i, across, 0).start()

    lcopies = [pltpu.make_async_copy(x_ref.at[h], xt.at[h], loc.at[0]),
               pltpu.make_async_copy(g1_ref, g1b.at[h], loc.at[1]),
               pltpu.make_async_copy(g2_ref, g2b.at[h], loc.at[2]),
               pltpu.make_async_copy(o_ref.at[h], ot, loc.at[3])]
    for i in range(3):
        lcopies.append(pltpu.make_async_copy(big[i][0], big[i][1].at[h], loc.at[4 + i]))
    for j in range(NJ):
        lcopies.append(pltpu.make_async_copy(wcols(wg_ref, j), wg.at[j, h], loc.at[7 + 2 * j]))
        lcopies.append(pltpu.make_async_copy(wcols(wu_ref, j), wu.at[j, h], loc.at[8 + 2 * j]))
    for cp in lcopies:
        cp.start()
    for j in range(NJ):
        for i in range(2):
            w_send(i, j, core, 1).start()
    for i in range(3):
        b_send(i, core, 1).start()

    x_cross(2).wait_recv()
    x_cross(3).wait_recv()
    oth = pl.ds(2 * (1 - xx), 2)

    def x_z(i):
        view = xt.at[oth, f]
        return remote(view, view, xs.at[3 + i], xr.at[3 + i], dev((f + 2 * i) % 8, h))

    def x_y(i):
        src = (f + 8 - 2 * i) % 8
        view = xt.at[oth, src]
        return remote(view, view, xs.at[7 + i], xr.at[7 + i], ypeer)

    for i in (1, 3, 2):
        x_z(i).start()
    x_y(0).start()
    for i in (1, 3, 2):
        x_z(i).wait_recv()
        x_y(i).start()

    for i in range(2):
        w_send(i, 0, across, 0).wait_recv()
        w_fwd(i, 0).start()

    for cp in lcopies:
        cp.wait()
    for cp in gcopies:
        cp.wait_recv()
    x_core.wait_recv()
    for i in range(4):
        x_y(i).wait_recv()

    dh = xt.shape[-1]
    urows = 8 * xt.shape[3]

    @pl.loop(0, NS)
    def _(s):
        blocks = [xt[b, s].reshape(urows, dh).astype(F32) for b in range(4)]
        ss = functools.reduce(jnp.add, [jnp.sum(v * v, axis=-1, keepdims=True) for v in blocks])
        r = lax.rsqrt(ss / d_model + EPS)
        for b in range(4):
            n[s, :, b * dh:(b + 1) * dh] = (blocks[b] * r * g1b[b]).astype(BF)

    for j in range(NJ):
        for i in range(2):
            if j > 0:
                w_send(i, j, across, 0).wait_recv()
                w_fwd(i, j).start()
        for i in range(2):
            w_send(i, j, core, 1).wait_recv()
            w_fwd(i, j).wait_recv()
        wgj = wg.at[j]
        wuj = wu.at[j]

        @pl.loop(0, NS // 2)
        def _(i):
            ns = n[pl.ds(2 * i, 2)].reshape(2 * urows, 4 * dh)
            gt = _dot(ns, wgj[...].reshape(4 * dh, jw))
            up = _dot(ns, wuj[...].reshape(4 * dh, jw))
            v = (jax.nn.silu(gt) * up).astype(BF)
            a[pl.ds(2 * i, 2), :, j * jw:(j + 1) * jw] = v.reshape(2, urows, jw)

    for i in range(3):
        b_send(i, core, 1).wait_recv()

    def st_y(u):
        return remote(yb.at[u, pl.ds((1 - y) * 4, 4)], yr.at[u], ps.at[0, u], pr.at[0, u], ypeer)

    def st_up(u, zz):
        return remote(yb.at[u, pl.ds(y * 4 + zz + 1, 3 - zz)], upr.at[u, pl.ds(zz, 3 - zz)],
                      ps.at[1, u], pr.at[1, u], above)

    def st_dn(u, zz):
        return remote(yb.at[u, pl.ds(y * 4, zz)], dnr.at[u, pl.ds(0, zz)],
                      ps.at[2, u], pr.at[2, u], below)

    def ag_y(u):
        v = xg.at[u, y, pl.ds(z, 1)]
        return remote(v, v, ps.at[3, u], pr.at[3, u], ypeer)

    def ag_z(u, src, way):
        v = xg.at[u, :, pl.ds(src, 1)]
        return remote(v, v, zs.at[way, u, src], zr.at[u, src], (above, below)[way])

    def out_x(u, to_h):
        return remote(xg.at[u], outx_ref.at[h * NS + u // 4], ps.at[4, u], pr.at[4, u], dev(f, to_h))

    def out_x_local(u):
        return pltpu.make_async_copy(xg.at[u], outx_ref.at[h * NS + u // 4], ps.at[4, u])

    def out_q(s, k):
        return remote(qb.at[s], outq_ref.at[h * NS + s], qs.at[k, s], qr.at[k, s], dev(f, hx(k)))

    def out_q_local(s):
        return pltpu.make_async_copy(qb.at[s], outq_ref.at[h * NS + s], qs.at[0, s])

    def at(t, lag, fn):
        i = t - lag

        @pl.when((i >= 0) & (i < NU))
        def _():
            late = i // (4 * NE)
            s = (1 - late) * ((i % (2 * NE)) // 2) + late * (i // 4)
            k = (1 - late) * (2 * (i // (2 * NE)) + i % 2) + late * ((i + 2) % 4)
            fn(4 * s + k)

    def p_compute(u):
        s, b = u // 4, hx(u % 4)

        @pl.when(u == 2)
        def _():
            for i in range(2):
                b_send(i, across, 0).wait_recv()
                b_fwd(i).start()

        @pl.when(u == 3)
        def _():
            for i in range(2):
                b_fwd(i).wait_recv()

        v = _dot(a[s], wd[b]) + _dot(ot[s], wo[b])
        yb[u] = v.reshape(yb.shape[1:])
        st_y(u).start()

    def send_up(u, zz):
        @pl.when(z == zz)
        def _():
            if zz > 0:
                st_up(u, zz - 1).wait_recv()
                for q in range(zz + 1, 4):
                    yb[u, y * 4 + q] = yb[u, y * 4 + q] + upr[u, q - 1]
            st_up(u, zz).start()

    def send_dn(u, zz):
        @pl.when(z == zz)
        def _():
            if zz < 3:
                st_dn(u, zz + 1).wait_recv()
                for q in range(zz):
                    yb[u, y * 4 + q] = yb[u, y * 4 + q] + dnr[u, q]
            st_dn(u, zz).start()

    def p_y(u):
        st_y(u).wait_recv()
        rows = pl.ds(y * 4, 4)
        yb[u, rows] = yb[u, rows] + yr[u]
        send_up(u, 0)
        send_dn(u, 3)

    def p_h2(u):
        send_up(u, 1)
        send_dn(u, 2)

    def p_h3(u):
        send_up(u, 2)
        send_dn(u, 1)

    def p_fin(u):
        s, b = u // 4, hx(u % 4)
        own = xt[b, s, y * 4 + z].astype(F32)

        @pl.when(z == 0)
        def _():
            st_dn(u, 1).wait_recv()
            xg[u, y, 0] = (own + (yb[u, y * 4] + dnr[u, 0])).astype(BF)

        @pl.when(z == 3)
        def _():
            st_up(u, 2).wait_recv()
            xg[u, y, 3] = (own + (yb[u, y * 4 + 3] + upr[u, 2])).astype(BF)

        @pl.when((z == 1) | (z == 2))
        def _():
            v = yb[u, y * 4 + z] + upr[u, z - 1] + dnr[u, z]
            xg[u, y, z] = (own + v).astype(BF)

        ag_y(u).start()

    def p_g1(u):
        @pl.when(u == 3)
        def _():
            b_send(2, across, 0).wait_recv()
            b_fwd(2).start()

        ag_y(u).wait_recv()

        @pl.when(z < 3)
        def _():
            ag_z(u, z, 0).start()

        @pl.when(z > 0)
        def _():
            ag_z(u, z, 1).start()

    def p_fwd(u, d):
        @pl.when(z >= d)
        def _():
            ag_z(u, z - d, 0).wait_recv()

        @pl.when((z >= d) & (z < 3))
        def _():
            ag_z(u, z - d, 0).start()

        @pl.when(z + d <= 3)
        def _():
            ag_z(u, z + d, 1).wait_recv()

        @pl.when((z + d <= 3) & (z > 0))
        def _():
            ag_z(u, z + d, 1).start()

    def p_g2(u):
        p_fwd(u, 1)

    def p_g3(u):
        p_fwd(u, 2)

    def done(u):
        return ((u % 4 == 3) & (u < 4 * NE)) | ((u % 4 == 1) & (u >= 4 * NE))

    def p_out(u):
        p_fwd(u, 3)

        @pl.when(u == 3)
        def _():
            b_fwd(2).wait_recv()

        @pl.when(u % 4 == 0)
        def _():
            out_x_local(u).start()

        @pl.when(u % 4 != 0)
        def _():
            out_x(u, hx(u % 4)).start()

        @pl.when(done(u))
        def _():
            s = u // 4
            blocks = [xg[4 * s + k].reshape(urows, dh).astype(F32) for k in range(4)]
            ss = functools.reduce(jnp.add, [jnp.sum(v * v, axis=-1, keepdims=True) for v in blocks])
            r = lax.rsqrt(ss / d_model + EPS)
            for k in range(4):
                nq[k] = (blocks[k] * r * g2b[hx(k)]).astype(BF)
            acc = functools.reduce(jnp.add, [_dot(nq[k], wq[hx(k)]) for k in range(4)])
            qb[s] = acc.astype(BF)
            for k in (2, 1):
                out_q(s, k).start()
            out_q_local(s).start()

    def out_q_from(s, k):
        rows = outq_ref.at[hx(k) * NS + s]
        return remote(qb.at[s], rows, qs.at[k, s], qr.at[k, s], dev(f, hx(k)))

    def q_fwd(s):
        rows = outq_ref.at[hx(2) * NS + s]
        return remote(rows, rows, qs.at[3, s], qr.at[3, s], core)

    def p_q(u):
        @pl.when(done(u))
        def _():
            out_q_from(u // 4, 2).wait_recv()
            q_fwd(u // 4).start()

    @pl.loop(0, NU + 19)
    def _(t):
        for lag, fn in ((0, p_compute), (3, p_y), (5, p_h2), (7, p_h3), (9, p_fin), (11, p_g1),
                        (13, p_g2), (15, p_g3), (17, p_out), (19, p_q)):
            at(t, lag, fn)

    for cp in gcopies:
        cp.wait_send()
    x_core.wait_send()
    x_cross(2).wait_send()
    x_cross(3).wait_send()
    for i in range(4):
        x_y(i).wait_send()
    for i in range(1, 4):
        x_z(i).wait_send()
    for j in range(NJ):
        for i in range(2):
            w_send(i, j, across, 0).wait_send()
            w_send(i, j, core, 1).wait_send()
            w_fwd(i, j).wait_send()
    for i in range(3):
        b_send(i, across, 0).wait_send()
        b_send(i, core, 1).wait_send()
        b_fwd(i).wait_send()

    @pl.loop(0, NU)
    def _(u):
        st_y(u).wait_send()
        for zz in range(3):
            @pl.when(z == zz)
            def _():
                st_up(u, zz).wait_send()

            @pl.when(z == zz + 1)
            def _():
                st_dn(u, zz + 1).wait_send()

        ag_y(u).wait_send()
        for d in range(3):
            @pl.when((z >= d) & (z < 3))
            def _():
                ag_z(u, z - d, 0).wait_send()

            @pl.when((z + d <= 3) & (z > 0))
            def _():
                ag_z(u, z + d, 1).wait_send()

        @pl.when(u % 4 == 0)
        def _():
            out_x_local(u).wait()

        @pl.when(u % 4 != 0)
        def _():
            k = u % 4
            rows = outx_ref.at[hx(k) * NS + u // 4]
            remote(xg.at[u], rows, ps.at[4, u], pr.at[4, u], dev(f, hx(k))).wait()

    @pl.loop(0, NS)
    def _(s):
        out_q_local(s).wait()
        out_q_from(s, 1).wait()
        out_q_from(s, 2).wait_send()
        q_fwd(s).wait_send()
        out_q_from(s, 3).wait_recv()


def _block(x, g1, g2, w_gate, w_up, w_down, o, w_o, w_qkv):
    tokens, dh = x.shape
    tq = tokens // 4
    ur = tq // NS
    ch = ur // 8
    ff, ko, nqk = w_gate.shape[1], o.shape[1], w_qkv.shape[1]
    jw = ff // NJ
    any_ = pl.BlockSpec(memory_space=pl.ANY)
    dma = pltpu.SemaphoreType.DMA
    scratch = [
        pltpu.VMEM((4, NS, 8, ch, dh), BF),
        pltpu.VMEM((NS, ur, 4 * dh), BF),
        pltpu.VMEM((4, 1, dh), F32),
        pltpu.VMEM((4, 1, dh), F32),
        pltpu.VMEM((NJ, 4, dh, jw), BF),
        pltpu.VMEM((NJ, 4, dh, jw), BF),
        pltpu.VMEM((4, ff, dh), BF),
        pltpu.VMEM((4, ko, dh), BF),
        pltpu.VMEM((4, dh, nqk), BF),
        pltpu.VMEM((NS, ur, ko), BF),
        pltpu.VMEM((NS, ur, ff), BF),
        pltpu.VMEM((NU, 8, ch, dh), F32),
        pltpu.VMEM((NU, 4, ch, dh), F32),
        pltpu.VMEM((NU, 3, ch, dh), F32),
        pltpu.VMEM((NU, 3, ch, dh), F32),
        pltpu.VMEM((NU, 2, 4, ch, dh), BF),
        pltpu.VMEM((4, ur, dh), BF),
        pltpu.VMEM((NS, ur, nqk), BF),
        dma((15,)),
        dma((2, 4)), dma((2, 4)),
        dma((11,)), dma((11,)),
        dma((3, 2, NJ)), dma((3, 2, NJ)),
        dma((3, 3)), dma((3, 3)),
        dma((STAGES, NU)), dma((STAGES, NU)),
        dma((2, NU, 4)), dma((NU, 4)),
        dma((4, NS)), dma((4, NS)),
    ]
    outx, outq = pl.pallas_call(
        functools.partial(_kernel, 4 * dh),
        name="block",
        out_shape=(pltpu.VMEM((4 * NS, 2, 4, ch, dh), BF),
                   pltpu.VMEM((4 * NS, ur, nqk), BF)),
        in_specs=[any_] * 9,
        out_specs=(any_, any_),
        scratch_shapes=scratch,
        compiler_params=pltpu.CompilerParams(collective_id=0, has_side_effects=True,
                                             vmem_limit_bytes=56 * 2**20),
    )(x.reshape(4, NS, 8, ch, dh), g1.reshape(1, dh), g2.reshape(1, dh), w_gate, w_up, w_down,
      o.reshape(4, NS, ur, ko), w_o, w_qkv)
    return outx.reshape(tokens, dh), outq.reshape(tokens, nqk)


def solution(mesh):
    in_specs = (P(None, 'h'), P('h'), P('h'), P('h', 'f'), P('h', 'f'), P('f', 'h'),
                P(None, 'f'), P('f', 'h'), P('h', 'f'))
    return jax.shard_map(_block, mesh=mesh, in_specs=in_specs,
                         out_specs=(P(None, 'h'), P(None, 'f')), check_vma=False)
```

```python
import functools

import jax
import jax.numpy as jnp
from jax import lax
from jax.experimental import pallas as pl
from jax.experimental.pallas import tpu as pltpu
from jax.sharding import PartitionSpec as P

EPS = 1e-6
BF, F32 = jnp.bfloat16, jnp.float32
MESH = pl.DeviceIdType.MESH

NS = 8
NU = 32
NE = 5
ND = 4
NJ = 4
STAGES = 5


def _dot(a, b):
    return jnp.dot(a, b, preferred_element_type=F32)


def _kernel(d_model, x_ref, g1_ref, g2_ref, wg_ref, wu_ref, wd_ref, o_ref, wo_ref, wq_ref,
            outx_ref, outq_ref,
            xt, n, g1b, g2b, wg, wu, wd, wo, wq, ot, a, yb, yr, upr, dnr, dbuf, xg, nq, qb,
            loc, gs, gr, xs, xr, ws, wr, bs, br, ps, pr, zs, zr, ds, dr, qs, qr):
    f, h = lax.axis_index('f'), lax.axis_index('h')
    z, y = f // 2, f % 2
    xx, c = h // 2, h % 2

    def hx(k):
        return 2 * ((xx + k // 2) % 2) + (c + k % 2) % 2

    def dev(ff, hh):
        return (ff, hh)

    ypeer = dev(z * 2 + (1 - y), h)
    above, below = dev((f + 2) % 8, h), dev((f + 6) % 8, h)
    core, across = dev(f, hx(1)), dev(f, hx(2))

    def remote(src, dst, ssem, rsem, to):
        return pltpu.make_async_remote_copy(src_ref=src, dst_ref=dst, send_sem=ssem, recv_sem=rsem,
                                            device_id=to, device_id_type=MESH)

    bar = pltpu.get_barrier_semaphore()
    for k in range(1, 4):
        pl.semaphore_signal(bar, inc=1, device_id=dev(f, hx(k)), device_id_type=MESH)
    for i in range(1, 8):
        pl.semaphore_signal(bar, inc=1, device_id=dev((f + i) % 8, h), device_id_type=MESH)
    pl.semaphore_wait(bar, 10)

    jw = wg.shape[-1]

    def wcols(ref, j):
        return ref.at[:, pl.ds(j * jw, jw)]


    def x_cross(k):
        return remote(x_ref.at[hx(k), f], xt.at[h, f],
                      xs.at[k], xr.at[k], dev(f, hx(k)))

    x_core = remote(x_ref.at[hx(1)], xt.at[h], xs.at[1], xr.at[1], core)
    x_cross(2).start()
    x_cross(3).start()
    gcopies = []
    for k in range(1, 4):
        gcopies.append(remote(g1_ref, g1b.at[h], gs.at[0, k], gr.at[0, k], dev(f, hx(k))))
        gcopies.append(remote(g2_ref, g2b.at[h], gs.at[1, k], gr.at[1, k], dev(f, hx(k))))
    for cp in gcopies:
        cp.start()
    x_core.start()

    def w_send(i, j, to, lane):
        src, dst = ((wg_ref, wg), (wu_ref, wu))[i]
        return remote(wcols(src, j), dst.at[j, h], ws.at[lane, i, j], wr.at[lane, i, j], to)

    def w_fwd(i, j):
        dst = (wg, wu)[i]
        return remote(dst.at[j, hx(2)], dst.at[j, hx(2)], ws.at[2, i, j], wr.at[2, i, j], core)

    big = ((wo_ref, wo), (wd_ref, wd), (wq_ref, wq))

    def b_send(i, to, lane):
        return remote(big[i][0], big[i][1].at[h], bs.at[lane, i], br.at[lane, i], to)

    def b_fwd(i):
        dst = big[i][1]
        return remote(dst.at[hx(2)], dst.at[hx(2)], bs.at[2, i], br.at[2, i], core)

    for j in range(NJ):
        for i in range(2):
            w_send(i, j, across, 0).start()
    for i in range(3):
        b_send(i, across, 0).start()

    lcopies = [pltpu.make_async_copy(x_ref.at[h], xt.at[h], loc.at[0]),
               pltpu.make_async_copy(g1_ref, g1b.at[h], loc.at[1]),
               pltpu.make_async_copy(g2_ref, g2b.at[h], loc.at[2]),
               pltpu.make_async_copy(o_ref.at[h], ot, loc.at[3])]
    for i in range(3):
        lcopies.append(pltpu.make_async_copy(big[i][0], big[i][1].at[h], loc.at[4 + i]))
    for j in range(NJ):
        lcopies.append(pltpu.make_async_copy(wcols(wg_ref, j), wg.at[j, h], loc.at[7 + 2 * j]))
        lcopies.append(pltpu.make_async_copy(wcols(wu_ref, j), wu.at[j, h], loc.at[8 + 2 * j]))
    for cp in lcopies:
        cp.start()
    for j in range(NJ):
        for i in range(2):
            w_send(i, j, core, 1).start()
    for i in range(3):
        b_send(i, core, 1).start()

    x_cross(2).wait_recv()
    x_cross(3).wait_recv()
    oth = pl.ds(2 * (1 - xx), 2)

    def x_z(i):
        view = xt.at[oth, f]
        return remote(view, view, xs.at[3 + i], xr.at[3 + i], dev((f + 2 * i) % 8, h))

    def x_y(i):
        src = (f + 8 - 2 * i) % 8
        view = xt.at[oth, src]
        return remote(view, view, xs.at[7 + i], xr.at[7 + i], ypeer)

    for i in (1, 3, 2):
        x_z(i).start()
    x_y(0).start()
    for i in (1, 3, 2):
        x_z(i).wait_recv()
        x_y(i).start()

    for i in range(2):
        w_send(i, 0, across, 0).wait_recv()
        w_fwd(i, 0).start()

    for cp in lcopies:
        cp.wait()
    for cp in gcopies:
        cp.wait_recv()
    x_core.wait_recv()
    for i in range(4):
        x_y(i).wait_recv()

    dh = xt.shape[-1]
    urows = 8 * xt.shape[3]

    @pl.loop(0, NS)
    def _(s):
        blocks = [xt[b, s].reshape(urows, dh).astype(F32) for b in range(4)]
        ss = functools.reduce(jnp.add, [jnp.sum(v * v, axis=-1, keepdims=True) for v in blocks])
        r = lax.rsqrt(ss / d_model + EPS)
        for b in range(4):
            n[s, :, b * dh:(b + 1) * dh] = (blocks[b] * r * g1b[b]).astype(BF)

    for j in range(NJ):
        for i in range(2):
            if j > 0:
                w_send(i, j, across, 0).wait_recv()
                w_fwd(i, j).start()
        for i in range(2):
            w_send(i, j, core, 1).wait_recv()
            w_fwd(i, j).wait_recv()
        wgj = wg.at[j]
        wuj = wu.at[j]

        @pl.loop(0, NS // 2)
        def _(i):
            ns = n[pl.ds(2 * i, 2)].reshape(2 * urows, 4 * dh)
            gt = _dot(ns, wgj[...].reshape(4 * dh, jw))
            up = _dot(ns, wuj[...].reshape(4 * dh, jw))
            v = (jax.nn.silu(gt) * up).astype(BF)
            a[pl.ds(2 * i, 2), :, j * jw:(j + 1) * jw] = v.reshape(2, urows, jw)

    for i in range(3):
        b_send(i, core, 1).wait_recv()

    def st_y(u):
        return remote(yb.at[u, pl.ds((1 - y) * 4, 4)], yr.at[u], ps.at[0, u], pr.at[0, u], ypeer)

    def st_up(u, zz):
        return remote(yb.at[u, pl.ds(y * 4 + zz + 1, 3 - zz)], upr.at[u, pl.ds(zz, 3 - zz)],
                      ps.at[1, u], pr.at[1, u], above)

    def st_dn(u, zz):
        return remote(yb.at[u, pl.ds(y * 4, zz)], dnr.at[u, pl.ds(0, zz)],
                      ps.at[2, u], pr.at[2, u], below)

    def ag_y(u):
        v = xg.at[u, y, pl.ds(z, 1)]
        return remote(v, v, ps.at[3, u], pr.at[3, u], ypeer)

    def ag_z(u, src, way):
        v = xg.at[u, :, pl.ds(src, 1)]
        return remote(v, v, zs.at[way, u, src], zr.at[u, src], (above, below)[way])

    def out_x(u, to_h):
        return remote(xg.at[u], outx_ref.at[h * NS + u // 4], ps.at[4, u], pr.at[4, u], dev(f, to_h))

    def out_x_local(u):
        return pltpu.make_async_copy(xg.at[u], outx_ref.at[h * NS + u // 4], ps.at[4, u])

    def out_q(s, k):
        return remote(qb.at[s], outq_ref.at[h * NS + s], qs.at[k, s], qr.at[k, s], dev(f, hx(k)))

    def out_q_local(s):
        return pltpu.make_async_copy(qb.at[s], outq_ref.at[h * NS + s], qs.at[0, s])

    def at(t, lag, fn, lo=0, hi=NU):
        i = t - lag

        @pl.when((i >= lo) & (i < hi))
        def _():
            p = i // 2 - NE
            early = 1 - (p + NE) // NE + (p + NE) // (2 * NE) + (p + NE) // (3 * NE)
            near_a, near_b = (p % 3) // 2, p // 10
            s_a = (1 - near_a) * (2 * (p // 3) + p % 3) + near_a * (NE + p // 3)
            s_b = (1 - near_b) * (p - 2) + near_b * (NS - 1)
            last = p // 6
            s = early * (p + NE) + (1 - early) * ((1 - last) * s_a + last * s_b)
            near = early + (1 - early) * ((1 - last) * near_a + last * near_b)
            fn(4 * s + 2 * (1 - near) + i % 2)

    def p_compute(u):
        s, b = u // 4, hx(u % 4)

        @pl.when(u == 2)
        def _():
            for i in range(2):
                b_send(i, across, 0).wait_recv()
                b_fwd(i).start()

        @pl.when(u == 3)
        def _():
            for i in range(2):
                b_fwd(i).wait_recv()

        v = _dot(a[s], wd[b]) + _dot(ot[s], wo[b])
        yb[u] = v.reshape(yb.shape[1:])
        st_y(u).start()

    def send_up(u, zz):
        @pl.when(z == zz)
        def _():
            if zz > 0:
                st_up(u, zz - 1).wait_recv()
                for q in range(zz + 1, 4):
                    yb[u, y * 4 + q] = yb[u, y * 4 + q] + upr[u, q - 1]
            st_up(u, zz).start()

    def send_dn(u, zz):
        @pl.when(z == zz)
        def _():
            if zz < 3:
                st_dn(u, zz + 1).wait_recv()
                for q in range(zz):
                    yb[u, y * 4 + q] = yb[u, y * 4 + q] + dnr[u, q]
            st_dn(u, zz).start()

    def p_y(u):
        st_y(u).wait_recv()
        rows = pl.ds(y * 4, 4)
        yb[u, rows] = yb[u, rows] + yr[u]
        send_up(u, 0)
        send_dn(u, 3)

    def p_h2(u):
        send_up(u, 1)
        send_dn(u, 2)

    def p_h3(u):
        send_up(u, 2)
        send_dn(u, 1)

    def p_fin(u):
        s, b = u // 4, hx(u % 4)
        own = xt[b, s, y * 4 + z].astype(F32)

        @pl.when(z == 0)
        def _():
            st_dn(u, 1).wait_recv()
            xg[u, y, 0] = (own + (yb[u, y * 4] + dnr[u, 0])).astype(BF)

        @pl.when(z == 3)
        def _():
            st_up(u, 2).wait_recv()
            xg[u, y, 3] = (own + (yb[u, y * 4 + 3] + upr[u, 2])).astype(BF)

        @pl.when((z == 1) | (z == 2))
        def _():
            v = yb[u, y * 4 + z] + upr[u, z - 1] + dnr[u, z]
            xg[u, y, z] = (own + v).astype(BF)

        ag_y(u).start()

    def p_g1(u):
        @pl.when(u == 3)
        def _():
            b_send(2, across, 0).wait_recv()
            b_fwd(2).start()

        ag_y(u).wait_recv()

        @pl.when(z < 3)
        def _():
            ag_z(u, z, 0).start()

        @pl.when(z > 0)
        def _():
            ag_z(u, z, 1).start()

    def p_fwd(u, d):
        @pl.when(z >= d)
        def _():
            ag_z(u, z - d, 0).wait_recv()

        @pl.when((z >= d) & (z < 3))
        def _():
            ag_z(u, z - d, 0).start()

        @pl.when(z + d <= 3)
        def _():
            ag_z(u, z + d, 1).wait_recv()

        @pl.when((z + d <= 3) & (z > 0))
        def _():
            ag_z(u, z + d, 1).start()

    def p_g2(u):
        p_fwd(u, 1)

    def p_g3(u):
        p_fwd(u, 2)

    def done(u):
        return ((u % 4 == 3) & (u != NU - 1)) | (u == NU - 3)

    def p_out(u):
        p_fwd(u, 3)

        @pl.when(u == 3)
        def _():
            b_fwd(2).wait_recv()

        finish(u)

    def d_rs(u, i):
        e = u - (NU - ND)
        return remote(yb.at[u, y * 4 + (z + i) % 4], dbuf.at[e, i - 1], ds.at[0, e, i], dr.at[0, e, i],
                      dev((f + 2 * i) % 8, h))

    def d_ag(u, i):
        e = u - (NU - ND)
        v = xg.at[u, y, z]
        return remote(v, v, ds.at[1, e, i], dr.at[1, e, i], dev((f + 2 * i) % 8, h))

    def d_agy(u):
        return remote(xg.at[u, y], xg.at[u, y], ps.at[3, u], pr.at[3, u], ypeer)

    def d_y(u):
        st_y(u).wait_recv()
        rows = pl.ds(y * 4, 4)
        yb[u, rows] = yb[u, rows] + yr[u]
        for i in (2, 1, 3):
            d_rs(u, i).start()

    def d_fin(u):
        s, b, e = u // 4, hx(u % 4), u - (NU - ND)
        for i in range(1, 4):
            d_rs(u, i).wait_recv()
        v = (yb[u, y * 4 + z] + dbuf[e, 0]) + (dbuf[e, 1] + dbuf[e, 2])
        xg[u, y, z] = (xt[b, s, y * 4 + z].astype(F32) + v).astype(BF)
        for i in (2, 1, 3):
            d_ag(u, i).start()

    def d_g(u):
        for i in range(1, 4):
            d_ag(u, i).wait_recv()
        d_agy(u).start()

    def d_out(u):
        d_agy(u).wait_recv()
        finish(u)

    def finish(u):
        @pl.when(u % 4 == 0)
        def _():
            out_x_local(u).start()

        @pl.when(u % 4 != 0)
        def _():
            out_x(u, hx(u % 4)).start()

        @pl.when(done(u))
        def _():
            s = u // 4
            blocks = [xg[4 * s + k].reshape(urows, dh).astype(F32) for k in range(4)]
            ss = functools.reduce(jnp.add, [jnp.sum(v * v, axis=-1, keepdims=True) for v in blocks])
            r = lax.rsqrt(ss / d_model + EPS)
            for k in range(4):
                nq[k] = (blocks[k] * r * g2b[hx(k)]).astype(BF)
            acc = functools.reduce(jnp.add, [_dot(nq[k], wq[hx(k)]) for k in range(4)])
            qb[s] = acc.astype(BF)
            for k in (2, 1):
                out_q(s, k).start()
            out_q_local(s).start()

    def out_q_from(s, k):
        rows = outq_ref.at[hx(k) * NS + s]
        return remote(qb.at[s], rows, qs.at[k, s], qr.at[k, s], dev(f, hx(k)))

    def q_fwd(s):
        rows = outq_ref.at[hx(2) * NS + s]
        return remote(rows, rows, qs.at[3, s], qr.at[3, s], core)

    def p_q(u):
        @pl.when(done(u))
        def _():
            out_q_from(u // 4, 2).wait_recv()
            q_fwd(u // 4).start()

    @pl.loop(0, NU + 8)
    def _(t):
        at(t, 0, p_compute)
        for lag, fn in ((2, p_y), (3, p_h2), (4, p_h3), (5, p_fin), (6, p_g1), (7, p_g2), (8, p_g3),
                        (9, p_out), (10, p_q)):
            at(t, lag, fn, hi=NU - ND)
        for lag, fn in ((2, d_y), (4, d_fin), (5, d_g), (6, d_out), (8, p_q)):
            at(t, lag, fn, lo=NU - ND)

    for cp in gcopies:
        cp.wait_send()
    x_core.wait_send()
    x_cross(2).wait_send()
    x_cross(3).wait_send()
    for i in range(4):
        x_y(i).wait_send()
    for i in range(1, 4):
        x_z(i).wait_send()
    for j in range(NJ):
        for i in range(2):
            w_send(i, j, across, 0).wait_send()
            w_send(i, j, core, 1).wait_send()
            w_fwd(i, j).wait_send()
    for i in range(3):
        b_send(i, across, 0).wait_send()
        b_send(i, core, 1).wait_send()
        b_fwd(i).wait_send()

    @pl.loop(0, NU - ND)
    def _(u):
        for zz in range(3):
            @pl.when(z == zz)
            def _():
                st_up(u, zz).wait_send()

            @pl.when(z == zz + 1)
            def _():
                st_dn(u, zz + 1).wait_send()

        ag_y(u).wait_send()
        for d in range(3):
            @pl.when((z >= d) & (z < 3))
            def _():
                ag_z(u, z - d, 0).wait_send()

            @pl.when((z + d <= 3) & (z > 0))
            def _():
                ag_z(u, z + d, 1).wait_send()

    @pl.loop(NU - ND, NU)
    def _(u):
        for i in range(1, 4):
            d_rs(u, i).wait_send()
            d_ag(u, i).wait_send()
        d_agy(u).wait_send()

    @pl.loop(0, NU)
    def _(u):
        st_y(u).wait_send()

        @pl.when(u % 4 == 0)
        def _():
            out_x_local(u).wait()

        @pl.when(u % 4 != 0)
        def _():
            k = u % 4
            rows = outx_ref.at[hx(k) * NS + u // 4]
            remote(xg.at[u], rows, ps.at[4, u], pr.at[4, u], dev(f, hx(k))).wait()

    @pl.loop(0, NS)
    def _(s):
        out_q_local(s).wait()
        out_q_from(s, 1).wait()
        out_q_from(s, 2).wait_send()
        q_fwd(s).wait_send()
        out_q_from(s, 3).wait_recv()


def _block(x, g1, g2, w_gate, w_up, w_down, o, w_o, w_qkv):
    tokens, dh = x.shape
    tq = tokens // 4
    ur = tq // NS
    ch = ur // 8
    ff, ko, nqk = w_gate.shape[1], o.shape[1], w_qkv.shape[1]
    jw = ff // NJ
    any_ = pl.BlockSpec(memory_space=pl.ANY)
    dma = pltpu.SemaphoreType.DMA
    scratch = [
        pltpu.VMEM((4, NS, 8, ch, dh), BF),
        pltpu.VMEM((NS, ur, 4 * dh), BF),
        pltpu.VMEM((4, 1, dh), F32),
        pltpu.VMEM((4, 1, dh), F32),
        pltpu.VMEM((NJ, 4, dh, jw), BF),
        pltpu.VMEM((NJ, 4, dh, jw), BF),
        pltpu.VMEM((4, ff, dh), BF),
        pltpu.VMEM((4, ko, dh), BF),
        pltpu.VMEM((4, dh, nqk), BF),
        pltpu.VMEM((NS, ur, ko), BF),
        pltpu.VMEM((NS, ur, ff), BF),
        pltpu.VMEM((NU, 8, ch, dh), F32),
        pltpu.VMEM((NU, 4, ch, dh), F32),
        pltpu.VMEM((NU, 3, ch, dh), F32),
        pltpu.VMEM((NU, 3, ch, dh), F32),
        pltpu.VMEM((ND, 3, ch, dh), F32),
        pltpu.VMEM((NU, 2, 4, ch, dh), BF),
        pltpu.VMEM((4, ur, dh), BF),
        pltpu.VMEM((NS, ur, nqk), BF),
        dma((15,)),
        dma((2, 4)), dma((2, 4)),
        dma((11,)), dma((11,)),
        dma((3, 2, NJ)), dma((3, 2, NJ)),
        dma((3, 3)), dma((3, 3)),
        dma((STAGES, NU)), dma((STAGES, NU)),
        dma((2, NU, 4)), dma((NU, 4)),
        dma((2, ND, 4)), dma((2, ND, 4)),
        dma((4, NS)), dma((4, NS)),
    ]
    outx, outq = pl.pallas_call(
        functools.partial(_kernel, 4 * dh),
        name="block",
        out_shape=(pltpu.VMEM((4 * NS, 2, 4, ch, dh), BF),
                   pltpu.VMEM((4 * NS, ur, nqk), BF)),
        in_specs=[any_] * 9,
        out_specs=(any_, any_),
        scratch_shapes=scratch,
        compiler_params=pltpu.CompilerParams(collective_id=0, has_side_effects=True,
                                             vmem_limit_bytes=56 * 2**20),
    )(x.reshape(4, NS, 8, ch, dh), g1.reshape(1, dh), g2.reshape(1, dh), w_gate, w_up, w_down,
      o.reshape(4, NS, ur, ko), w_o, w_qkv)
    return outx.reshape(tokens, dh), outq.reshape(tokens, nqk)


def solution(mesh):
    in_specs = (P(None, 'h'), P('h'), P('h'), P('h', 'f'), P('h', 'f'), P('f', 'h'),
                P(None, 'f'), P('f', 'h'), P('h', 'f'))
    return jax.shard_map(_block, mesh=mesh, in_specs=in_specs,
                         out_specs=(P(None, 'h'), P(None, 'f')), check_vma=False)
```

```python
import functools

import jax
import jax.numpy as jnp
from jax import lax
from jax.experimental import pallas as pl
from jax.experimental.pallas import tpu as pltpu
from jax.sharding import PartitionSpec as P

EPS = 1e-6
BF, F32 = jnp.bfloat16, jnp.float32
MESH = pl.DeviceIdType.MESH

NS = 8
NU = 32
NE = 4
ND = 4
NJ = 4
STAGES = 5


def _dot(a, b):
    return jnp.dot(a, b, preferred_element_type=F32)


def _kernel(d_model, x_ref, g1_ref, g2_ref, wg_ref, wu_ref, wd_ref, o_ref, wo_ref, wq_ref,
            outx_ref, outq_ref,
            xt, n, g1b, g2b, wg, wu, wd, wo, wq, ot, a, yb, yr, upr, dnr, dbuf, xg, nq, qb,
            loc, gs, gr, xs, xr, ws, wr, bs, br, ps, pr, zs, zr, ds, dr, qs, qr):
    f, h = lax.axis_index('f'), lax.axis_index('h')
    z, y = f // 2, f % 2
    xx, c = h // 2, h % 2

    def hx(k):
        return 2 * ((xx + k // 2) % 2) + (c + k % 2) % 2

    def dev(ff, hh):
        return (ff, hh)

    ypeer = dev(z * 2 + (1 - y), h)
    above, below = dev((f + 2) % 8, h), dev((f + 6) % 8, h)
    core, across = dev(f, hx(1)), dev(f, hx(2))

    def remote(src, dst, ssem, rsem, to):
        return pltpu.make_async_remote_copy(src_ref=src, dst_ref=dst, send_sem=ssem, recv_sem=rsem,
                                            device_id=to, device_id_type=MESH)

    bar = pltpu.get_barrier_semaphore()
    for k in range(1, 4):
        pl.semaphore_signal(bar, inc=1, device_id=dev(f, hx(k)), device_id_type=MESH)
    for i in range(1, 8):
        pl.semaphore_signal(bar, inc=1, device_id=dev((f + i) % 8, h), device_id_type=MESH)
    pl.semaphore_wait(bar, 10)

    jw = wg.shape[-1]

    def wcols(ref, j):
        return ref.at[:, pl.ds(j * jw, jw)]


    def x_cross(k):
        return remote(x_ref.at[hx(k), f], xt.at[h, f],
                      xs.at[k], xr.at[k], dev(f, hx(k)))

    x_core = remote(x_ref.at[hx(1)], xt.at[h], xs.at[1], xr.at[1], core)
    x_cross(2).start()
    x_cross(3).start()
    gcopies = []
    for k in range(1, 4):
        gcopies.append(remote(g1_ref, g1b.at[h], gs.at[0, k], gr.at[0, k], dev(f, hx(k))))
        gcopies.append(remote(g2_ref, g2b.at[h], gs.at[1, k], gr.at[1, k], dev(f, hx(k))))
    for cp in gcopies:
        cp.start()
    x_core.start()

    def w_send(i, j, to, lane):
        src, dst = ((wg_ref, wg), (wu_ref, wu))[i]
        return remote(wcols(src, j), dst.at[j, h], ws.at[lane, i, j], wr.at[lane, i, j], to)

    def w_fwd(i, j):
        dst = (wg, wu)[i]
        return remote(dst.at[j, hx(2)], dst.at[j, hx(2)], ws.at[2, i, j], wr.at[2, i, j], core)

    big = ((wo_ref, wo), (wd_ref, wd), (wq_ref, wq))

    def b_send(i, to, lane):
        return remote(big[i][0], big[i][1].at[h], bs.at[lane, i], br.at[lane, i], to)

    def b_fwd(i):
        dst = big[i][1]
        return remote(dst.at[hx(2)], dst.at[hx(2)], bs.at[2, i], br.at[2, i], core)

    for j in range(NJ):
        for i in range(2):
            w_send(i, j, across, 0).start()
    for i in range(3):
        b_send(i, across, 0).start()

    lcopies = [pltpu.make_async_copy(x_ref.at[h], xt.at[h], loc.at[0]),
               pltpu.make_async_copy(g1_ref, g1b.at[h], loc.at[1]),
               pltpu.make_async_copy(g2_ref, g2b.at[h], loc.at[2]),
               pltpu.make_async_copy(o_ref.at[h], ot, loc.at[3])]
    for i in range(3):
        lcopies.append(pltpu.make_async_copy(big[i][0], big[i][1].at[h], loc.at[4 + i]))
    for j in range(NJ):
        lcopies.append(pltpu.make_async_copy(wcols(wg_ref, j), wg.at[j, h], loc.at[7 + 2 * j]))
        lcopies.append(pltpu.make_async_copy(wcols(wu_ref, j), wu.at[j, h], loc.at[8 + 2 * j]))
    for cp in lcopies:
        cp.start()
    for j in range(NJ):
        for i in range(2):
            w_send(i, j, core, 1).start()
    for i in range(3):
        b_send(i, core, 1).start()

    x_cross(2).wait_recv()
    x_cross(3).wait_recv()
    oth = pl.ds(2 * (1 - xx), 2)

    def x_z(i):
        view = xt.at[oth, f]
        return remote(view, view, xs.at[3 + i], xr.at[3 + i], dev((f + 2 * i) % 8, h))

    def x_y(i):
        src = (f + 8 - 2 * i) % 8
        view = xt.at[oth, src]
        return remote(view, view, xs.at[7 + i], xr.at[7 + i], ypeer)

    for i in (1, 3, 2):
        x_z(i).start()
    x_y(0).start()
    for i in (1, 3, 2):
        x_z(i).wait_recv()
        x_y(i).start()

    for i in range(2):
        w_send(i, 0, across, 0).wait_recv()
        w_fwd(i, 0).start()

    for cp in lcopies:
        cp.wait()
    for cp in gcopies:
        cp.wait_recv()
    x_core.wait_recv()
    for i in range(4):
        x_y(i).wait_recv()

    dh = xt.shape[-1]
    urows = 8 * xt.shape[3]

    @pl.loop(0, NS)
    def _(s):
        blocks = [xt[b, s].reshape(urows, dh).astype(F32) for b in range(4)]
        ss = functools.reduce(jnp.add, [jnp.sum(v * v, axis=-1, keepdims=True) for v in blocks])
        r = lax.rsqrt(ss / d_model + EPS)
        for b in range(4):
            n[s, :, b * dh:(b + 1) * dh] = (blocks[b] * r * g1b[b]).astype(BF)

    for j in range(NJ):
        for i in range(2):
            if j > 0:
                w_send(i, j, across, 0).wait_recv()
                w_fwd(i, j).start()
        for i in range(2):
            w_send(i, j, core, 1).wait_recv()
            w_fwd(i, j).wait_recv()
        wgj = wg.at[j]
        wuj = wu.at[j]

        @pl.loop(0, NS // 2)
        def _(i):
            ns = n[pl.ds(2 * i, 2)].reshape(2 * urows, 4 * dh)
            gt = _dot(ns, wgj[...].reshape(4 * dh, jw))
            up = _dot(ns, wuj[...].reshape(4 * dh, jw))
            v = (jax.nn.silu(gt) * up).astype(BF)
            a[pl.ds(2 * i, 2), :, j * jw:(j + 1) * jw] = v.reshape(2, urows, jw)

    for i in range(3):
        b_send(i, core, 1).wait_recv()

    def st_y(u):
        return remote(yb.at[u, pl.ds((1 - y) * 4, 4)], yr.at[u], ps.at[0, u], pr.at[0, u], ypeer)

    def st_up(u, zz):
        return remote(yb.at[u, pl.ds(y * 4 + zz + 1, 3 - zz)], upr.at[u, pl.ds(zz, 3 - zz)],
                      ps.at[1, u], pr.at[1, u], above)

    def st_dn(u, zz):
        return remote(yb.at[u, pl.ds(y * 4, zz)], dnr.at[u, pl.ds(0, zz)],
                      ps.at[2, u], pr.at[2, u], below)

    def ag_y(u):
        v = xg.at[u, y, pl.ds(z, 1)]
        return remote(v, v, ps.at[3, u], pr.at[3, u], ypeer)

    def ag_z(u, src, way):
        v = xg.at[u, :, pl.ds(src, 1)]
        return remote(v, v, zs.at[way, u, src], zr.at[u, src], (above, below)[way])

    def out_x(u, to_h):
        return remote(xg.at[u], outx_ref.at[h * NS + u // 4], ps.at[4, u], pr.at[4, u], dev(f, to_h))

    def out_x_local(u):
        return pltpu.make_async_copy(xg.at[u], outx_ref.at[h * NS + u // 4], ps.at[4, u])

    def out_q(s, k):
        return remote(qb.at[s], outq_ref.at[h * NS + s], qs.at[k, s], qr.at[k, s], dev(f, hx(k)))

    def out_q_local(s):
        return pltpu.make_async_copy(qb.at[s], outq_ref.at[h * NS + s], qs.at[0, s])

    def at(t, lag, fn, lo=0, hi=NU):
        i = t - lag

        @pl.when((i >= lo) & (i < hi))
        def _():
            p = i // 2 - NE
            early = 1 - (p + NE) // NE + (p + NE) // (2 * NE) + (p + NE) // (3 * NE)
            n_mix = (p % 3) // 2
            s_mix = (1 - n_mix) * (2 * (p // 3) + p % 3) + n_mix * (NE + p // 3)
            s = early * (p + NE) + (1 - early) * s_mix
            near = early + (1 - early) * n_mix
            fn(4 * s + 2 * (1 - near) + i % 2)

    def p_compute(u):
        s, b = u // 4, hx(u % 4)

        @pl.when(u == 2)
        def _():
            for i in range(2):
                b_send(i, across, 0).wait_recv()
                b_fwd(i).start()

        @pl.when(u == 3)
        def _():
            for i in range(2):
                b_fwd(i).wait_recv()

        v = _dot(a[s], wd[b]) + _dot(ot[s], wo[b])
        yb[u] = v.reshape(yb.shape[1:])
        st_y(u).start()

    def send_up(u, zz):
        @pl.when(z == zz)
        def _():
            if zz > 0:
                st_up(u, zz - 1).wait_recv()
                for q in range(zz + 1, 4):
                    yb[u, y * 4 + q] = yb[u, y * 4 + q] + upr[u, q - 1]
            st_up(u, zz).start()

    def send_dn(u, zz):
        @pl.when(z == zz)
        def _():
            if zz < 3:
                st_dn(u, zz + 1).wait_recv()
                for q in range(zz):
                    yb[u, y * 4 + q] = yb[u, y * 4 + q] + dnr[u, q]
            st_dn(u, zz).start()

    def p_y(u):
        st_y(u).wait_recv()
        rows = pl.ds(y * 4, 4)
        yb[u, rows] = yb[u, rows] + yr[u]
        send_up(u, 0)
        send_dn(u, 3)

    def p_h2(u):
        send_up(u, 1)
        send_dn(u, 2)

    def p_h3(u):
        send_up(u, 2)
        send_dn(u, 1)

    def p_fin(u):
        s, b = u // 4, hx(u % 4)
        own = xt[b, s, y * 4 + z].astype(F32)

        @pl.when(z == 0)
        def _():
            st_dn(u, 1).wait_recv()
            xg[u, y, 0] = (own + (yb[u, y * 4] + dnr[u, 0])).astype(BF)

        @pl.when(z == 3)
        def _():
            st_up(u, 2).wait_recv()
            xg[u, y, 3] = (own + (yb[u, y * 4 + 3] + upr[u, 2])).astype(BF)

        @pl.when((z == 1) | (z == 2))
        def _():
            v = yb[u, y * 4 + z] + upr[u, z - 1] + dnr[u, z]
            xg[u, y, z] = (own + v).astype(BF)

        ag_y(u).start()

    def p_g1(u):
        @pl.when(u == 3)
        def _():
            b_send(2, across, 0).wait_recv()
            b_fwd(2).start()

        ag_y(u).wait_recv()

        @pl.when(z < 3)
        def _():
            ag_z(u, z, 0).start()

        @pl.when(z > 0)
        def _():
            ag_z(u, z, 1).start()

    def p_fwd(u, d):
        @pl.when(z >= d)
        def _():
            ag_z(u, z - d, 0).wait_recv()

        @pl.when((z >= d) & (z < 3))
        def _():
            ag_z(u, z - d, 0).start()

        @pl.when(z + d <= 3)
        def _():
            ag_z(u, z + d, 1).wait_recv()

        @pl.when((z + d <= 3) & (z > 0))
        def _():
            ag_z(u, z + d, 1).start()

    def p_g2(u):
        p_fwd(u, 1)

    def p_g3(u):
        p_fwd(u, 2)

    def done(u):
        return ((u % 4 == 3) & (u != NU - 1)) | (u == NU - 3)

    def p_out(u):
        p_fwd(u, 3)

        @pl.when(u == 3)
        def _():
            b_fwd(2).wait_recv()

        finish(u)

    def d_rs(u, i):
        e = u - (NU - ND)
        return remote(yb.at[u, y * 4 + (z + i) % 4], dbuf.at[e, i - 1], ds.at[0, e, i], dr.at[0, e, i],
                      dev((f + 2 * i) % 8, h))

    def d_ag(u, i):
        e = u - (NU - ND)
        v = xg.at[u, y, z]
        return remote(v, v, ds.at[1, e, i], dr.at[1, e, i], dev((f + 2 * i) % 8, h))

    def d_agy(u):
        return remote(xg.at[u, y], xg.at[u, y], ps.at[3, u], pr.at[3, u], ypeer)

    def d_y(u):
        st_y(u).wait_recv()
        rows = pl.ds(y * 4, 4)
        yb[u, rows] = yb[u, rows] + yr[u]
        for i in (2, 1, 3):
            d_rs(u, i).start()

    def d_fin(u):
        s, b, e = u // 4, hx(u % 4), u - (NU - ND)
        for i in range(1, 4):
            d_rs(u, i).wait_recv()
        v = (yb[u, y * 4 + z] + dbuf[e, 0]) + (dbuf[e, 1] + dbuf[e, 2])
        xg[u, y, z] = (xt[b, s, y * 4 + z].astype(F32) + v).astype(BF)
        for i in (2, 1, 3):
            d_ag(u, i).start()

    def d_g(u):
        for i in range(1, 4):
            d_ag(u, i).wait_recv()
        d_agy(u).start()

    def d_out(u):
        d_agy(u).wait_recv()
        finish(u)

    def finish(u):
        @pl.when(u % 4 == 0)
        def _():
            out_x_local(u).start()

        @pl.when(u % 4 != 0)
        def _():
            out_x(u, hx(u % 4)).start()

        @pl.when(done(u))
        def _():
            s = u // 4
            blocks = [xg[4 * s + k].reshape(urows, dh).astype(F32) for k in range(4)]
            ss = functools.reduce(jnp.add, [jnp.sum(v * v, axis=-1, keepdims=True) for v in blocks])
            r = lax.rsqrt(ss / d_model + EPS)
            for k in range(4):
                nq[k] = (blocks[k] * r * g2b[hx(k)]).astype(BF)
            acc = functools.reduce(jnp.add, [_dot(nq[k], wq[hx(k)]) for k in range(4)])
            qb[s] = acc.astype(BF)
            for k in (2, 1):
                out_q(s, k).start()
            out_q_local(s).start()

    def out_q_from(s, k):
        rows = outq_ref.at[hx(k) * NS + s]
        return remote(qb.at[s], rows, qs.at[k, s], qr.at[k, s], dev(f, hx(k)))

    def q_fwd(s):
        rows = outq_ref.at[hx(2) * NS + s]
        return remote(rows, rows, qs.at[3, s], qr.at[3, s], core)

    def p_q(u):
        @pl.when(done(u))
        def _():
            out_q_from(u // 4, 2).wait_recv()
            q_fwd(u // 4).start()

    @pl.loop(0, NU + 10)
    def _(t):
        at(t, 0, p_compute)
        for lag, fn in ((2, p_y), (4, p_h2), (6, p_h3), (7, p_fin), (9, p_g1), (10, p_g2), (12, p_g3),
                        (13, p_out), (14, p_q)):
            at(t, lag, fn, hi=NU - ND)
        for lag, fn in ((2, d_y), (4, d_fin), (6, d_g), (8, d_out), (10, p_q)):
            at(t, lag, fn, lo=NU - ND)

    for cp in gcopies:
        cp.wait_send()
    x_core.wait_send()
    x_cross(2).wait_send()
    x_cross(3).wait_send()
    for i in range(4):
        x_y(i).wait_send()
    for i in range(1, 4):
        x_z(i).wait_send()
    for j in range(NJ):
        for i in range(2):
            w_send(i, j, across, 0).wait_send()
            w_send(i, j, core, 1).wait_send()
            w_fwd(i, j).wait_send()
    for i in range(3):
        b_send(i, across, 0).wait_send()
        b_send(i, core, 1).wait_send()
        b_fwd(i).wait_send()

    @pl.loop(0, NU - ND)
    def _(u):
        for zz in range(3):
            @pl.when(z == zz)
            def _():
                st_up(u, zz).wait_send()

            @pl.when(z == zz + 1)
            def _():
                st_dn(u, zz + 1).wait_send()

        ag_y(u).wait_send()
        for d in range(3):
            @pl.when((z >= d) & (z < 3))
            def _():
                ag_z(u, z - d, 0).wait_send()

            @pl.when((z + d <= 3) & (z > 0))
            def _():
                ag_z(u, z + d, 1).wait_send()

    @pl.loop(NU - ND, NU)
    def _(u):
        for i in range(1, 4):
            d_rs(u, i).wait_send()
            d_ag(u, i).wait_send()
        d_agy(u).wait_send()

    @pl.loop(0, NU)
    def _(u):
        st_y(u).wait_send()

        @pl.when(u % 4 == 0)
        def _():
            out_x_local(u).wait()

        @pl.when(u % 4 != 0)
        def _():
            k = u % 4
            rows = outx_ref.at[hx(k) * NS + u // 4]
            remote(xg.at[u], rows, ps.at[4, u], pr.at[4, u], dev(f, hx(k))).wait()

    @pl.loop(0, NS)
    def _(s):
        out_q_local(s).wait()
        out_q_from(s, 1).wait()
        out_q_from(s, 2).wait_send()
        q_fwd(s).wait_send()
        out_q_from(s, 3).wait_recv()


def _block(x, g1, g2, w_gate, w_up, w_down, o, w_o, w_qkv):
    tokens, dh = x.shape
    tq = tokens // 4
    ur = tq // NS
    ch = ur // 8
    ff, ko, nqk = w_gate.shape[1], o.shape[1], w_qkv.shape[1]
    jw = ff // NJ
    any_ = pl.BlockSpec(memory_space=pl.ANY)
    dma = pltpu.SemaphoreType.DMA
    scratch = [
        pltpu.VMEM((4, NS, 8, ch, dh), BF),
        pltpu.VMEM((NS, ur, 4 * dh), BF),
        pltpu.VMEM((4, 1, dh), F32),
        pltpu.VMEM((4, 1, dh), F32),
        pltpu.VMEM((NJ, 4, dh, jw), BF),
        pltpu.VMEM((NJ, 4, dh, jw), BF),
        pltpu.VMEM((4, ff, dh), BF),
        pltpu.VMEM((4, ko, dh), BF),
        pltpu.VMEM((4, dh, nqk), BF),
        pltpu.VMEM((NS, ur, ko), BF),
        pltpu.VMEM((NS, ur, ff), BF),
        pltpu.VMEM((NU, 8, ch, dh), F32),
        pltpu.VMEM((NU, 4, ch, dh), F32),
        pltpu.VMEM((NU, 3, ch, dh), F32),
        pltpu.VMEM((NU, 3, ch, dh), F32),
        pltpu.VMEM((ND, 3, ch, dh), F32),
        pltpu.VMEM((NU, 2, 4, ch, dh), BF),
        pltpu.VMEM((4, ur, dh), BF),
        pltpu.VMEM((NS, ur, nqk), BF),
        dma((15,)),
        dma((2, 4)), dma((2, 4)),
        dma((11,)), dma((11,)),
        dma((3, 2, NJ)), dma((3, 2, NJ)),
        dma((3, 3)), dma((3, 3)),
        dma((STAGES, NU)), dma((STAGES, NU)),
        dma((2, NU, 4)), dma((NU, 4)),
        dma((2, ND, 4)), dma((2, ND, 4)),
        dma((4, NS)), dma((4, NS)),
    ]
    outx, outq = pl.pallas_call(
        functools.partial(_kernel, 4 * dh),
        name="block",
        out_shape=(pltpu.VMEM((4 * NS, 2, 4, ch, dh), BF),
                   pltpu.VMEM((4 * NS, ur, nqk), BF)),
        in_specs=[any_] * 9,
        out_specs=(any_, any_),
        scratch_shapes=scratch,
        compiler_params=pltpu.CompilerParams(collective_id=0, has_side_effects=True,
                                             vmem_limit_bytes=56 * 2**20),
    )(x.reshape(4, NS, 8, ch, dh), g1.reshape(1, dh), g2.reshape(1, dh), w_gate, w_up, w_down,
      o.reshape(4, NS, ur, ko), w_o, w_qkv)
    return outx.reshape(tokens, dh), outq.reshape(tokens, nqk)


def solution(mesh):
    in_specs = (P(None, 'h'), P('h'), P('h'), P('h', 'f'), P('h', 'f'), P('f', 'h'),
                P(None, 'f'), P('f', 'h'), P('h', 'f'))
    return jax.shard_map(_block, mesh=mesh, in_specs=in_specs,
                         out_specs=(P(None, 'h'), P(None, 'f')), check_vma=False)
```

```python
import functools

import jax
import jax.numpy as jnp
from jax import lax
from jax.experimental import pallas as pl
from jax.experimental.pallas import tpu as pltpu
from jax.sharding import PartitionSpec as P

EPS = 1e-6
BF, F32 = jnp.bfloat16, jnp.float32
MESH = pl.DeviceIdType.MESH

NS = 8
NU = 32
ND = 4
NJ = 4
STAGES = 5


def _dot(a, b):
    return jnp.dot(a, b, preferred_element_type=F32)


def _kernel(d_model, x_ref, g1_ref, g2_ref, wg_ref, wu_ref, wd_ref, o_ref, wo_ref, wq_ref,
            outx_ref, outq_ref,
            xt, n, g1b, g2b, wg, wu, wd, wo, wq, ot, a, yb, yr, upr, dnr, dbuf, xg, nq, qb,
            loc, gs, gr, xs, xr, ws, wr, bs, br, ps, pr, zs, zr, ds, dr, qs, qr):
    f, h = lax.axis_index('f'), lax.axis_index('h')
    z, y = f // 2, f % 2
    xx, c = h // 2, h % 2

    def hx(k):
        return 2 * ((xx + k // 2) % 2) + (c + k % 2) % 2

    def dev(ff, hh):
        return (ff, hh)

    ypeer = dev(z * 2 + (1 - y), h)
    above, below = dev((f + 2) % 8, h), dev((f + 6) % 8, h)
    core, across = dev(f, hx(1)), dev(f, hx(2))

    def remote(src, dst, ssem, rsem, to):
        return pltpu.make_async_remote_copy(src_ref=src, dst_ref=dst, send_sem=ssem, recv_sem=rsem,
                                            device_id=to, device_id_type=MESH)

    bar = pltpu.get_barrier_semaphore()
    for k in range(1, 4):
        pl.semaphore_signal(bar, inc=1, device_id=dev(f, hx(k)), device_id_type=MESH)
    for i in range(1, 8):
        pl.semaphore_signal(bar, inc=1, device_id=dev((f + i) % 8, h), device_id_type=MESH)
    pl.semaphore_wait(bar, 10)

    jw = wg.shape[-1]

    def wcols(ref, j):
        return ref.at[:, pl.ds(j * jw, jw)]


    def x_cross(k):
        return remote(x_ref.at[hx(k), f], xt.at[h, f],
                      xs.at[k], xr.at[k], dev(f, hx(k)))

    x_core = remote(x_ref.at[hx(1)], xt.at[h], xs.at[1], xr.at[1], core)
    x_cross(2).start()
    x_cross(3).start()
    gcopies = []
    for k in range(1, 4):
        gcopies.append(remote(g1_ref, g1b.at[h], gs.at[0, k], gr.at[0, k], dev(f, hx(k))))
        gcopies.append(remote(g2_ref, g2b.at[h], gs.at[1, k], gr.at[1, k], dev(f, hx(k))))
    for cp in gcopies:
        cp.start()
    x_core.start()

    def w_send(i, j, to, lane):
        src, dst = ((wg_ref, wg), (wu_ref, wu))[i]
        return remote(wcols(src, j), dst.at[j, h], ws.at[lane, i, j], wr.at[lane, i, j], to)

    def w_fwd(i, j):
        dst = (wg, wu)[i]
        return remote(dst.at[j, hx(2)], dst.at[j, hx(2)], ws.at[2, i, j], wr.at[2, i, j], core)

    big = ((wo_ref, wo), (wd_ref, wd), (wq_ref, wq))

    def b_send(i, to, lane):
        return remote(big[i][0], big[i][1].at[h], bs.at[lane, i], br.at[lane, i], to)

    def b_fwd(i):
        dst = big[i][1]
        return remote(dst.at[hx(2)], dst.at[hx(2)], bs.at[2, i], br.at[2, i], core)

    for j in range(NJ):
        for i in range(2):
            w_send(i, j, across, 0).start()
    for i in range(3):
        b_send(i, across, 0).start()

    lcopies = [pltpu.make_async_copy(x_ref.at[h], xt.at[h], loc.at[0]),
               pltpu.make_async_copy(g1_ref, g1b.at[h], loc.at[1]),
               pltpu.make_async_copy(g2_ref, g2b.at[h], loc.at[2]),
               pltpu.make_async_copy(o_ref.at[h], ot, loc.at[3])]
    for i in range(3):
        lcopies.append(pltpu.make_async_copy(big[i][0], big[i][1].at[h], loc.at[4 + i]))
    for j in range(NJ):
        lcopies.append(pltpu.make_async_copy(wcols(wg_ref, j), wg.at[j, h], loc.at[7 + 2 * j]))
        lcopies.append(pltpu.make_async_copy(wcols(wu_ref, j), wu.at[j, h], loc.at[8 + 2 * j]))
    for cp in lcopies:
        cp.start()
    for j in range(NJ):
        for i in range(2):
            w_send(i, j, core, 1).start()
    for i in range(3):
        b_send(i, core, 1).start()

    x_cross(2).wait_recv()
    x_cross(3).wait_recv()
    oth = pl.ds(2 * (1 - xx), 2)

    def x_z(i):
        view = xt.at[oth, f]
        return remote(view, view, xs.at[3 + i], xr.at[3 + i], dev((f + 2 * i) % 8, h))

    def x_y(i):
        src = (f + 8 - 2 * i) % 8
        view = xt.at[oth, src]
        return remote(view, view, xs.at[7 + i], xr.at[7 + i], ypeer)

    for i in (1, 3, 2):
        x_z(i).start()
    x_y(0).start()
    for i in (1, 3, 2):
        x_z(i).wait_recv()
        x_y(i).start()

    for i in range(2):
        w_send(i, 0, across, 0).wait_recv()
        w_fwd(i, 0).start()

    for cp in lcopies:
        cp.wait()
    for cp in gcopies:
        cp.wait_recv()
    x_core.wait_recv()
    for i in range(4):
        x_y(i).wait_recv()

    dh = xt.shape[-1]
    urows = 8 * xt.shape[3]

    @pl.loop(0, NS)
    def _(s):
        blocks = [xt[b, s].reshape(urows, dh).astype(F32) for b in range(4)]
        ss = functools.reduce(jnp.add, [jnp.sum(v * v, axis=-1, keepdims=True) for v in blocks])
        r = lax.rsqrt(ss / d_model + EPS)
        for b in range(4):
            n[s, :, b * dh:(b + 1) * dh] = (blocks[b] * r * g1b[b]).astype(BF)

    for j in range(NJ):
        for i in range(2):
            if j > 0:
                w_send(i, j, across, 0).wait_recv()
                w_fwd(i, j).start()
        for i in range(2):
            w_send(i, j, core, 1).wait_recv()
            w_fwd(i, j).wait_recv()
        wgj = wg.at[j]
        wuj = wu.at[j]

        @pl.loop(0, NS // 2)
        def _(i):
            ns = n[pl.ds(2 * i, 2)].reshape(2 * urows, 4 * dh)
            gt = _dot(ns, wgj[...].reshape(4 * dh, jw))
            up = _dot(ns, wuj[...].reshape(4 * dh, jw))
            v = (jax.nn.silu(gt) * up).astype(BF)
            a[pl.ds(2 * i, 2), :, j * jw:(j + 1) * jw] = v.reshape(2, urows, jw)

    for i in range(3):
        b_send(i, core, 1).wait_recv()

    def st_y(u):
        return remote(yb.at[u, pl.ds((1 - y) * 4, 4)], yr.at[u], ps.at[0, u], pr.at[0, u], ypeer)

    def st_up(u, zz):
        return remote(yb.at[u, pl.ds(y * 4 + zz + 1, 3 - zz)], upr.at[u, pl.ds(zz, 3 - zz)],
                      ps.at[1, u], pr.at[1, u], above)

    def st_dn(u, zz):
        return remote(yb.at[u, pl.ds(y * 4, zz)], dnr.at[u, pl.ds(0, zz)],
                      ps.at[2, u], pr.at[2, u], below)

    def ag_y(u):
        v = xg.at[u, y, pl.ds(z, 1)]
        return remote(v, v, ps.at[3, u], pr.at[3, u], ypeer)

    def ag_z(u, src, way):
        v = xg.at[u, :, pl.ds(src, 1)]
        return remote(v, v, zs.at[way, u, src], zr.at[u, src], (above, below)[way])

    def out_x(u, to_h):
        return remote(xg.at[u], outx_ref.at[h * NS + u // 4], ps.at[4, u], pr.at[4, u], dev(f, to_h))

    def out_x_local(u):
        return pltpu.make_async_copy(xg.at[u], outx_ref.at[h * NS + u // 4], ps.at[4, u])

    def out_q(s, k):
        return remote(qb.at[s], outq_ref.at[h * NS + s], qs.at[k, s], qr.at[k, s], dev(f, hx(k)))

    def out_q_local(s):
        return pltpu.make_async_copy(qb.at[s], outq_ref.at[h * NS + s], qs.at[0, s])

    def at(t, lag, fn, lo=0, hi=NU):
        i = t - lag

        @pl.when((i >= lo) & (i < hi))
        def _():
            p = i // 2
            q = (2 * p) // NS
            far = (q + 2) // 3 - q // 3
            s = p - (NS // 2) * ((q + 2) // 3 + q // 3)
            fn(4 * s + 2 * far + i % 2)

    def p_compute(u):
        s, b = u // 4, hx(u % 4)

        @pl.when(u == 2)
        def _():
            for i in range(2):
                b_send(i, across, 0).wait_recv()
                b_fwd(i).start()

        @pl.when(u == 3)
        def _():
            for i in range(2):
                b_fwd(i).wait_recv()

        v = _dot(a[s], wd[b]) + _dot(ot[s], wo[b])
        yb[u] = v.reshape(yb.shape[1:])
        st_y(u).start()

    def send_up(u, zz):
        @pl.when(z == zz)
        def _():
            if zz > 0:
                st_up(u, zz - 1).wait_recv()
                for q in range(zz + 1, 4):
                    yb[u, y * 4 + q] = yb[u, y * 4 + q] + upr[u, q - 1]
            st_up(u, zz).start()

    def send_dn(u, zz):
        @pl.when(z == zz)
        def _():
            if zz < 3:
                st_dn(u, zz + 1).wait_recv()
                for q in range(zz):
                    yb[u, y * 4 + q] = yb[u, y * 4 + q] + dnr[u, q]
            st_dn(u, zz).start()

    def p_y(u):
        st_y(u).wait_recv()
        rows = pl.ds(y * 4, 4)
        yb[u, rows] = yb[u, rows] + yr[u]
        send_up(u, 0)
        send_dn(u, 3)

    def p_h2(u):
        send_up(u, 1)
        send_dn(u, 2)

    def p_h3(u):
        send_up(u, 2)
        send_dn(u, 1)

    def p_fin(u):
        s, b = u // 4, hx(u % 4)
        own = xt[b, s, y * 4 + z].astype(F32)

        @pl.when(z == 0)
        def _():
            st_dn(u, 1).wait_recv()
            xg[u, y, 0] = (own + (yb[u, y * 4] + dnr[u, 0])).astype(BF)

        @pl.when(z == 3)
        def _():
            st_up(u, 2).wait_recv()
            xg[u, y, 3] = (own + (yb[u, y * 4 + 3] + upr[u, 2])).astype(BF)

        @pl.when((z == 1) | (z == 2))
        def _():
            v = yb[u, y * 4 + z] + upr[u, z - 1] + dnr[u, z]
            xg[u, y, z] = (own + v).astype(BF)

        ag_y(u).start()

    def p_g1(u):
        @pl.when(u == 3)
        def _():
            b_send(2, across, 0).wait_recv()
            b_fwd(2).start()

        ag_y(u).wait_recv()

        @pl.when(z < 3)
        def _():
            ag_z(u, z, 0).start()

        @pl.when(z > 0)
        def _():
            ag_z(u, z, 1).start()

    def p_fwd(u, d):
        @pl.when(z >= d)
        def _():
            ag_z(u, z - d, 0).wait_recv()

        @pl.when((z >= d) & (z < 3))
        def _():
            ag_z(u, z - d, 0).start()

        @pl.when(z + d <= 3)
        def _():
            ag_z(u, z + d, 1).wait_recv()

        @pl.when((z + d <= 3) & (z > 0))
        def _():
            ag_z(u, z + d, 1).start()

    def p_g2(u):
        p_fwd(u, 1)

    def p_g3(u):
        p_fwd(u, 2)

    def done(u):
        return ((u % 4 == 3) & (u < NU // 2)) | ((u % 4 == 1) & (u >= NU // 2))

    def straight(u):
        return (u >= NU - 2 * ND) & (u % 4 < 2)

    def p_out(u):
        p_fwd(u, 3)

        @pl.when(u == 3)
        def _():
            b_fwd(2).wait_recv()

        finish(u)

    def nth(u):
        return (u - (NU - 2 * ND)) // 4 * 2 + u % 4

    def d_rs(u, i):
        e = nth(u)
        return remote(yb.at[u, y * 4 + (z + i) % 4], dbuf.at[e, i - 1], ds.at[0, e, i], dr.at[0, e, i],
                      dev((f + 2 * i) % 8, h))

    def d_ag(u, i):
        e = nth(u)
        v = xg.at[u, y, z]
        return remote(v, v, ds.at[1, e, i], dr.at[1, e, i], dev((f + 2 * i) % 8, h))

    def d_agy(u):
        return remote(xg.at[u, y], xg.at[u, y], ps.at[3, u], pr.at[3, u], ypeer)

    def d_y(u):
        st_y(u).wait_recv()
        rows = pl.ds(y * 4, 4)
        yb[u, rows] = yb[u, rows] + yr[u]
        for i in (2, 1, 3):
            d_rs(u, i).start()

    def d_fin(u):
        s, b, e = u // 4, hx(u % 4), nth(u)
        for i in range(1, 4):
            d_rs(u, i).wait_recv()
        v = (yb[u, y * 4 + z] + dbuf[e, 0]) + (dbuf[e, 1] + dbuf[e, 2])
        xg[u, y, z] = (xt[b, s, y * 4 + z].astype(F32) + v).astype(BF)
        for i in (2, 1, 3):
            d_ag(u, i).start()

    def d_g(u):
        for i in range(1, 4):
            d_ag(u, i).wait_recv()
        d_agy(u).start()

    def d_out(u):
        d_agy(u).wait_recv()
        finish(u)

    def finish(u):
        @pl.when(u % 4 == 0)
        def _():
            out_x_local(u).start()

        @pl.when(u % 4 != 0)
        def _():
            out_x(u, hx(u % 4)).start()

        @pl.when(done(u))
        def _():
            s = u // 4
            blocks = [xg[4 * s + k].reshape(urows, dh).astype(F32) for k in range(4)]
            ss = functools.reduce(jnp.add, [jnp.sum(v * v, axis=-1, keepdims=True) for v in blocks])
            r = lax.rsqrt(ss / d_model + EPS)
            for k in range(4):
                nq[k] = (blocks[k] * r * g2b[hx(k)]).astype(BF)
            acc = functools.reduce(jnp.add, [_dot(nq[k], wq[hx(k)]) for k in range(4)])
            qb[s] = acc.astype(BF)
            for k in (2, 1):
                out_q(s, k).start()
            out_q_local(s).start()

    def out_q_from(s, k):
        rows = outq_ref.at[hx(k) * NS + s]
        return remote(qb.at[s], rows, qs.at[k, s], qr.at[k, s], dev(f, hx(k)))

    def q_fwd(s):
        rows = outq_ref.at[hx(2) * NS + s]
        return remote(rows, rows, qs.at[3, s], qr.at[3, s], core)

    def p_q(u):
        @pl.when(done(u))
        def _():
            out_q_from(u // 4, 2).wait_recv()
            q_fwd(u // 4).start()

    @pl.loop(0, NU + 10)
    def _(t):
        at(t, 0, p_compute)
        for lag, fn in ((2, p_y), (4, p_h2), (6, p_h3), (7, p_fin), (9, p_g1), (10, p_g2), (12, p_g3),
                        (13, p_out), (14, p_q)):
            at(t, lag, fn, hi=NU - ND)
        for lag, fn in ((2, d_y), (4, d_fin), (6, d_g), (8, d_out), (10, p_q)):
            at(t, lag, fn, lo=NU - ND)

    for cp in gcopies:
        cp.wait_send()
    x_core.wait_send()
    x_cross(2).wait_send()
    x_cross(3).wait_send()
    for i in range(4):
        x_y(i).wait_send()
    for i in range(1, 4):
        x_z(i).wait_send()
    for j in range(NJ):
        for i in range(2):
            w_send(i, j, across, 0).wait_send()
            w_send(i, j, core, 1).wait_send()
            w_fwd(i, j).wait_send()
    for i in range(3):
        b_send(i, across, 0).wait_send()
        b_send(i, core, 1).wait_send()
        b_fwd(i).wait_send()

    def line_sent(u):
        for zz in range(3):
            @pl.when(z == zz)
            def _():
                st_up(u, zz).wait_send()

            @pl.when(z == zz + 1)
            def _():
                st_dn(u, zz + 1).wait_send()

        ag_y(u).wait_send()
        for d in range(3):
            @pl.when((z >= d) & (z < 3))
            def _():
                ag_z(u, z - d, 0).wait_send()

            @pl.when((z + d <= 3) & (z > 0))
            def _():
                ag_z(u, z + d, 1).wait_send()

    def straight_sent(u):
        for i in range(1, 4):
            d_rs(u, i).wait_send()
            d_ag(u, i).wait_send()
        d_agy(u).wait_send()

    @pl.loop(0, NU)
    def _(u):
        st_y(u).wait_send()

        @pl.when(straight(u))
        def _():
            straight_sent(u)

        @pl.when(jnp.logical_not(straight(u)))
        def _():
            line_sent(u)

        @pl.when(u % 4 == 0)
        def _():
            out_x_local(u).wait()

        @pl.when(u % 4 != 0)
        def _():
            k = u % 4
            rows = outx_ref.at[hx(k) * NS + u // 4]
            remote(xg.at[u], rows, ps.at[4, u], pr.at[4, u], dev(f, hx(k))).wait()

    @pl.loop(0, NS)
    def _(s):
        out_q_local(s).wait()
        out_q_from(s, 1).wait()
        out_q_from(s, 2).wait_send()
        q_fwd(s).wait_send()
        out_q_from(s, 3).wait_recv()


def _block(x, g1, g2, w_gate, w_up, w_down, o, w_o, w_qkv):
    tokens, dh = x.shape
    tq = tokens // 4
    ur = tq // NS
    ch = ur // 8
    ff, ko, nqk = w_gate.shape[1], o.shape[1], w_qkv.shape[1]
    jw = ff // NJ
    any_ = pl.BlockSpec(memory_space=pl.ANY)
    dma = pltpu.SemaphoreType.DMA
    scratch = [
        pltpu.VMEM((4, NS, 8, ch, dh), BF),
        pltpu.VMEM((NS, ur, 4 * dh), BF),
        pltpu.VMEM((4, 1, dh), F32),
        pltpu.VMEM((4, 1, dh), F32),
        pltpu.VMEM((NJ, 4, dh, jw), BF),
        pltpu.VMEM((NJ, 4, dh, jw), BF),
        pltpu.VMEM((4, ff, dh), BF),
        pltpu.VMEM((4, ko, dh), BF),
        pltpu.VMEM((4, dh, nqk), BF),
        pltpu.VMEM((NS, ur, ko), BF),
        pltpu.VMEM((NS, ur, ff), BF),
        pltpu.VMEM((NU, 8, ch, dh), F32),
        pltpu.VMEM((NU, 4, ch, dh), F32),
        pltpu.VMEM((NU, 3, ch, dh), F32),
        pltpu.VMEM((NU, 3, ch, dh), F32),
        pltpu.VMEM((ND, 3, ch, dh), F32),
        pltpu.VMEM((NU, 2, 4, ch, dh), BF),
        pltpu.VMEM((4, ur, dh), BF),
        pltpu.VMEM((NS, ur, nqk), BF),
        dma((15,)),
        dma((2, 4)), dma((2, 4)),
        dma((11,)), dma((11,)),
        dma((3, 2, NJ)), dma((3, 2, NJ)),
        dma((3, 3)), dma((3, 3)),
        dma((STAGES, NU)), dma((STAGES, NU)),
        dma((2, NU, 4)), dma((NU, 4)),
        dma((2, ND, 4)), dma((2, ND, 4)),
        dma((4, NS)), dma((4, NS)),
    ]
    outx, outq = pl.pallas_call(
        functools.partial(_kernel, 4 * dh),
        name="block",
        out_shape=(pltpu.VMEM((4 * NS, 2, 4, ch, dh), BF),
                   pltpu.VMEM((4 * NS, ur, nqk), BF)),
        in_specs=[any_] * 9,
        out_specs=(any_, any_),
        scratch_shapes=scratch,
        compiler_params=pltpu.CompilerParams(collective_id=0, has_side_effects=True,
                                             vmem_limit_bytes=56 * 2**20),
    )(x.reshape(4, NS, 8, ch, dh), g1.reshape(1, dh), g2.reshape(1, dh), w_gate, w_up, w_down,
      o.reshape(4, NS, ur, ko), w_o, w_qkv)
    return outx.reshape(tokens, dh), outq.reshape(tokens, nqk)


def solution(mesh):
    in_specs = (P(None, 'h'), P('h'), P('h'), P('h', 'f'), P('h', 'f'), P('f', 'h'),
                P(None, 'f'), P('f', 'h'), P('h', 'f'))
    return jax.shard_map(_block, mesh=mesh, in_specs=in_specs,
                         out_specs=(P(None, 'h'), P(None, 'f')), check_vma=False)
```

```python
import functools

import jax
import jax.numpy as jnp
from jax import lax
from jax.experimental import pallas as pl
from jax.experimental.pallas import tpu as pltpu
from jax.sharding import PartitionSpec as P

EPS = 1e-6
BF, F32 = jnp.bfloat16, jnp.float32
MESH = pl.DeviceIdType.MESH

NS = 8
NU = 32
ND = 4
NJ = 4
STAGES = 5


def _dot(a, b):
    return jnp.dot(a, b, preferred_element_type=F32)


def _kernel(d_model, x_ref, g1_ref, g2_ref, wg_ref, wu_ref, wd_ref, o_ref, wo_ref, wq_ref,
            outx_ref, outq_ref,
            xt, n, g1b, g2b, wg, wu, wd, wo, wq, ot, a, yb, yr, upr, dnr, dbuf, xg, nq, qb,
            loc, gs, gr, xs, xr, ws, wr, bs, br, ps, pr, zs, zr, ds, dr, qs, qr):
    f, h = lax.axis_index('f'), lax.axis_index('h')
    z, y = f // 2, f % 2
    xx, c = h // 2, h % 2

    def hx(k):
        return 2 * ((xx + k // 2) % 2) + (c + k % 2) % 2

    def dev(ff, hh):
        return (ff, hh)

    ypeer = dev(z * 2 + (1 - y), h)
    above, below = dev((f + 2) % 8, h), dev((f + 6) % 8, h)
    core, across = dev(f, hx(1)), dev(f, hx(2))

    def remote(src, dst, ssem, rsem, to):
        return pltpu.make_async_remote_copy(src_ref=src, dst_ref=dst, send_sem=ssem, recv_sem=rsem,
                                            device_id=to, device_id_type=MESH)

    bar = pltpu.get_barrier_semaphore()
    for k in range(1, 4):
        pl.semaphore_signal(bar, inc=1, device_id=dev(f, hx(k)), device_id_type=MESH)
    for i in range(1, 8):
        pl.semaphore_signal(bar, inc=1, device_id=dev((f + i) % 8, h), device_id_type=MESH)
    pl.semaphore_wait(bar, 10)

    jw = wg.shape[-1]

    def wcols(ref, j):
        return ref.at[:, pl.ds(j * jw, jw)]


    def x_cross(k):
        return remote(x_ref.at[hx(k), f], xt.at[h, f],
                      xs.at[k], xr.at[k], dev(f, hx(k)))

    x_core = remote(x_ref.at[hx(1)], xt.at[h], xs.at[1], xr.at[1], core)
    x_cross(2).start()
    x_cross(3).start()
    gcopies = []
    for k in range(1, 4):
        gcopies.append(remote(g1_ref, g1b.at[h], gs.at[0, k], gr.at[0, k], dev(f, hx(k))))
        gcopies.append(remote(g2_ref, g2b.at[h], gs.at[1, k], gr.at[1, k], dev(f, hx(k))))
    for cp in gcopies:
        cp.start()
    x_core.start()

    def w_send(i, j, to, lane):
        src, dst = ((wg_ref, wg), (wu_ref, wu))[i]
        return remote(wcols(src, j), dst.at[j, h], ws.at[lane, i, j], wr.at[lane, i, j], to)

    def w_fwd(i, j):
        dst = (wg, wu)[i]
        return remote(dst.at[j, hx(2)], dst.at[j, hx(2)], ws.at[2, i, j], wr.at[2, i, j], core)

    big = ((wo_ref, wo), (wd_ref, wd), (wq_ref, wq))

    def b_send(i, to, lane):
        return remote(big[i][0], big[i][1].at[h], bs.at[lane, i], br.at[lane, i], to)

    def b_fwd(i):
        dst = big[i][1]
        return remote(dst.at[hx(2)], dst.at[hx(2)], bs.at[2, i], br.at[2, i], core)

    for j in range(NJ):
        for i in range(2):
            w_send(i, j, across, 0).start()
    for i in range(3):
        b_send(i, across, 0).start()

    lcopies = [pltpu.make_async_copy(x_ref.at[h], xt.at[h], loc.at[0]),
               pltpu.make_async_copy(g1_ref, g1b.at[h], loc.at[1]),
               pltpu.make_async_copy(g2_ref, g2b.at[h], loc.at[2]),
               pltpu.make_async_copy(o_ref.at[h], ot, loc.at[3])]
    for i in range(3):
        lcopies.append(pltpu.make_async_copy(big[i][0], big[i][1].at[h], loc.at[4 + i]))
    for j in range(NJ):
        lcopies.append(pltpu.make_async_copy(wcols(wg_ref, j), wg.at[j, h], loc.at[7 + 2 * j]))
        lcopies.append(pltpu.make_async_copy(wcols(wu_ref, j), wu.at[j, h], loc.at[8 + 2 * j]))
    for cp in lcopies:
        cp.start()
    for j in range(NJ):
        for i in range(2):
            w_send(i, j, core, 1).start()
    for i in range(3):
        b_send(i, core, 1).start()

    x_cross(2).wait_recv()
    x_cross(3).wait_recv()
    oth = pl.ds(2 * (1 - xx), 2)

    def x_z(i):
        view = xt.at[oth, f]
        return remote(view, view, xs.at[3 + i], xr.at[3 + i], dev((f + 2 * i) % 8, h))

    def x_y(i):
        src = (f + 8 - 2 * i) % 8
        view = xt.at[oth, src]
        return remote(view, view, xs.at[7 + i], xr.at[7 + i], ypeer)

    for i in (1, 3, 2):
        x_z(i).start()
    x_y(0).start()
    for i in (1, 3, 2):
        x_z(i).wait_recv()
        x_y(i).start()

    for i in range(2):
        w_send(i, 0, across, 0).wait_recv()
        w_fwd(i, 0).start()

    for cp in lcopies:
        cp.wait()
    for cp in gcopies:
        cp.wait_recv()
    x_core.wait_recv()
    for i in range(4):
        x_y(i).wait_recv()

    dh = xt.shape[-1]
    urows = 8 * xt.shape[3]

    @pl.loop(0, NS)
    def _(s):
        blocks = [xt[b, s].reshape(urows, dh).astype(F32) for b in range(4)]
        ss = functools.reduce(jnp.add, [jnp.sum(v * v, axis=-1, keepdims=True) for v in blocks])
        r = lax.rsqrt(ss / d_model + EPS)
        for b in range(4):
            n[s, :, b * dh:(b + 1) * dh] = (blocks[b] * r * g1b[b]).astype(BF)

    for j in range(NJ):
        for i in range(2):
            if j > 0:
                w_send(i, j, across, 0).wait_recv()
                w_fwd(i, j).start()
        for i in range(2):
            w_send(i, j, core, 1).wait_recv()
            w_fwd(i, j).wait_recv()
        wgj = wg.at[j]
        wuj = wu.at[j]

        @pl.loop(0, NS // 2)
        def _(i):
            ns = n[pl.ds(2 * i, 2)].reshape(2 * urows, 4 * dh)
            gt = _dot(ns, wgj[...].reshape(4 * dh, jw))
            up = _dot(ns, wuj[...].reshape(4 * dh, jw))
            v = (jax.nn.silu(gt) * up).astype(BF)
            a[pl.ds(2 * i, 2), :, j * jw:(j + 1) * jw] = v.reshape(2, urows, jw)

    for i in range(3):
        b_send(i, core, 1).wait_recv()

    def st_y(u):
        return remote(yb.at[u, pl.ds((1 - y) * 4, 4)], yr.at[u], ps.at[0, u], pr.at[0, u], ypeer)

    def st_up(u, zz):
        return remote(yb.at[u, pl.ds(y * 4 + zz + 1, 3 - zz)], upr.at[u, pl.ds(zz, 3 - zz)],
                      ps.at[1, u], pr.at[1, u], above)

    def st_dn(u, zz):
        return remote(yb.at[u, pl.ds(y * 4, zz)], dnr.at[u, pl.ds(0, zz)],
                      ps.at[2, u], pr.at[2, u], below)

    def ag_y(u):
        v = xg.at[u, y, pl.ds(z, 1)]
        return remote(v, v, ps.at[3, u], pr.at[3, u], ypeer)

    def ag_z(u, src, way):
        v = xg.at[u, :, pl.ds(src, 1)]
        return remote(v, v, zs.at[way, u, src], zr.at[u, src], (above, below)[way])

    def out_x(u, to_h):
        return remote(xg.at[u], outx_ref.at[h * NS + u // 4], ps.at[4, u], pr.at[4, u], dev(f, to_h))

    def out_x_local(u):
        return pltpu.make_async_copy(xg.at[u], outx_ref.at[h * NS + u // 4], ps.at[4, u])

    def out_q(s, k):
        return remote(qb.at[s], outq_ref.at[h * NS + s], qs.at[k, s], qr.at[k, s], dev(f, hx(k)))

    def out_q_local(s):
        return pltpu.make_async_copy(qb.at[s], outq_ref.at[h * NS + s], qs.at[0, s])

    def at(t, lag, fn, lo=0, hi=NU):
        i = t - lag

        @pl.when((i >= lo) & (i < hi))
        def _():
            p = i // 2
            q = (2 * p) // NS
            far = (q + 2) // 3 - q // 3
            s = p - (NS // 2) * ((q + 2) // 3 + q // 3)
            fn(4 * s + 2 * far + i % 2)

    def p_compute(u):
        s, b = u // 4, hx(u % 4)

        @pl.when(u == 2)
        def _():
            for i in range(2):
                b_send(i, across, 0).wait_recv()
                b_fwd(i).start()

        @pl.when(u == 3)
        def _():
            for i in range(2):
                b_fwd(i).wait_recv()

        v = _dot(a[s], wd[b]) + _dot(ot[s], wo[b])
        yb[u] = v.reshape(yb.shape[1:])
        st_y(u).start()

    def send_up(u, zz):
        @pl.when(z == zz)
        def _():
            if zz > 0:
                st_up(u, zz - 1).wait_recv()
                for q in range(zz + 1, 4):
                    yb[u, y * 4 + q] = yb[u, y * 4 + q] + upr[u, q - 1]
            st_up(u, zz).start()

    def send_dn(u, zz):
        @pl.when(z == zz)
        def _():
            if zz < 3:
                st_dn(u, zz + 1).wait_recv()
                for q in range(zz):
                    yb[u, y * 4 + q] = yb[u, y * 4 + q] + dnr[u, q]
            st_dn(u, zz).start()

    def p_y(u):
        st_y(u).wait_recv()
        rows = pl.ds(y * 4, 4)
        yb[u, rows] = yb[u, rows] + yr[u]
        send_up(u, 0)
        send_dn(u, 3)

    def p_h2(u):
        send_up(u, 1)
        send_dn(u, 2)

    def p_h3(u):
        send_up(u, 2)
        send_dn(u, 1)

    def p_fin(u):
        s, b = u // 4, hx(u % 4)
        own = xt[b, s, y * 4 + z].astype(F32)

        @pl.when(z == 0)
        def _():
            st_dn(u, 1).wait_recv()
            xg[u, y, 0] = (own + (yb[u, y * 4] + dnr[u, 0])).astype(BF)

        @pl.when(z == 3)
        def _():
            st_up(u, 2).wait_recv()
            xg[u, y, 3] = (own + (yb[u, y * 4 + 3] + upr[u, 2])).astype(BF)

        @pl.when((z == 1) | (z == 2))
        def _():
            v = yb[u, y * 4 + z] + upr[u, z - 1] + dnr[u, z]
            xg[u, y, z] = (own + v).astype(BF)

        ag_y(u).start()

    def p_g1(u):
        @pl.when(u == 3)
        def _():
            b_send(2, across, 0).wait_recv()
            b_fwd(2).start()

        ag_y(u).wait_recv()

        @pl.when(z < 3)
        def _():
            ag_z(u, z, 0).start()

        @pl.when(z > 0)
        def _():
            ag_z(u, z, 1).start()

    def p_fwd(u, d):
        @pl.when(z >= d)
        def _():
            ag_z(u, z - d, 0).wait_recv()

        @pl.when((z >= d) & (z < 3))
        def _():
            ag_z(u, z - d, 0).start()

        @pl.when(z + d <= 3)
        def _():
            ag_z(u, z + d, 1).wait_recv()

        @pl.when((z + d <= 3) & (z > 0))
        def _():
            ag_z(u, z + d, 1).start()

    def p_g2(u):
        p_fwd(u, 1)

    def p_g3(u):
        p_fwd(u, 2)

    def done(u):
        return ((u % 4 == 3) & (u < NU // 2)) | ((u % 4 == 1) & (u >= NU // 2))

    def straight(u):
        return (u >= NU - 2 * ND) & (u % 4 < 2)

    def p_out(u):
        p_fwd(u, 3)

        @pl.when(u == 3)
        def _():
            b_fwd(2).wait_recv()

        finish(u)

    def nth(u):
        return (u - (NU - 2 * ND)) // 4 * 2 + u % 4

    def d_rs(u, i):
        e = nth(u)
        return remote(yb.at[u, y * 4 + (z + i) % 4], dbuf.at[e, i - 1], ds.at[0, e, i], dr.at[0, e, i],
                      dev((f + 2 * i) % 8, h))

    def d_ag(u, i):
        e = nth(u)
        v = xg.at[u, y, z]
        return remote(v, v, ds.at[1, e, i], dr.at[1, e, i], dev((f + 2 * i) % 8, h))

    def d_agy(u):
        return remote(xg.at[u, y], xg.at[u, y], ps.at[3, u], pr.at[3, u], ypeer)

    def d_y(u):
        st_y(u).wait_recv()
        rows = pl.ds(y * 4, 4)
        yb[u, rows] = yb[u, rows] + yr[u]
        for i in (2, 1, 3):
            d_rs(u, i).start()

    def d_fin(u):
        s, b, e = u // 4, hx(u % 4), nth(u)
        for i in range(1, 4):
            d_rs(u, i).wait_recv()
        v = (yb[u, y * 4 + z] + dbuf[e, 0]) + (dbuf[e, 1] + dbuf[e, 2])
        xg[u, y, z] = (xt[b, s, y * 4 + z].astype(F32) + v).astype(BF)
        for i in (2, 1, 3):
            d_ag(u, i).start()

    def d_g(u):
        for i in range(1, 4):
            d_ag(u, i).wait_recv()
        d_agy(u).start()

    def d_out(u):
        d_agy(u).wait_recv()
        finish(u)

    def finish(u):
        @pl.when(u % 4 == 0)
        def _():
            out_x_local(u).start()

        @pl.when(u % 4 != 0)
        def _():
            out_x(u, hx(u % 4)).start()

        @pl.when(done(u))
        def _():
            s = u // 4
            blocks = [xg[4 * s + k].reshape(urows, dh).astype(F32) for k in range(4)]
            ss = functools.reduce(jnp.add, [jnp.sum(v * v, axis=-1, keepdims=True) for v in blocks])
            r = lax.rsqrt(ss / d_model + EPS)
            for k in range(4):
                nq[k] = (blocks[k] * r * g2b[hx(k)]).astype(BF)
            acc = functools.reduce(jnp.add, [_dot(nq[k], wq[hx(k)]) for k in range(4)])
            qb[s] = acc.astype(BF)
            for k in (2, 1):
                out_q(s, k).start()
            out_q_local(s).start()

    def out_q_from(s, k):
        rows = outq_ref.at[hx(k) * NS + s]
        return remote(qb.at[s], rows, qs.at[k, s], qr.at[k, s], dev(f, hx(k)))

    def q_fwd(s):
        rows = outq_ref.at[hx(2) * NS + s]
        return remote(rows, rows, qs.at[3, s], qr.at[3, s], core)

    def p_q(u):
        @pl.when(done(u))
        def _():
            out_q_from(u // 4, 2).wait_recv()
            q_fwd(u // 4).start()

    @pl.loop(0, NU + 18)
    def _(t):
        at(t, 0, p_compute)
        for lag, fn in ((2, p_y), (4, p_h2), (6, p_h3), (7, p_fin), (9, p_g1), (10, p_g2), (12, p_g3),
                        (13, p_out), (22, p_q)):
            at(t, lag, fn, hi=NU - ND)
        for lag, fn in ((2, d_y), (4, d_fin), (6, d_g), (8, d_out), (10, p_q)):
            at(t, lag, fn, lo=NU - ND)

    for cp in gcopies:
        cp.wait_send()
    x_core.wait_send()
    x_cross(2).wait_send()
    x_cross(3).wait_send()
    for i in range(4):
        x_y(i).wait_send()
    for i in range(1, 4):
        x_z(i).wait_send()
    for j in range(NJ):
        for i in range(2):
            w_send(i, j, across, 0).wait_send()
            w_send(i, j, core, 1).wait_send()
            w_fwd(i, j).wait_send()
    for i in range(3):
        b_send(i, across, 0).wait_send()
        b_send(i, core, 1).wait_send()
        b_fwd(i).wait_send()

    def line_sent(u):
        for zz in range(3):
            @pl.when(z == zz)
            def _():
                st_up(u, zz).wait_send()

            @pl.when(z == zz + 1)
            def _():
                st_dn(u, zz + 1).wait_send()

        ag_y(u).wait_send()
        for d in range(3):
            @pl.when((z >= d) & (z < 3))
            def _():
                ag_z(u, z - d, 0).wait_send()

            @pl.when((z + d <= 3) & (z > 0))
            def _():
                ag_z(u, z + d, 1).wait_send()

    def straight_sent(u):
        for i in range(1, 4):
            d_rs(u, i).wait_send()
            d_ag(u, i).wait_send()
        d_agy(u).wait_send()

    @pl.loop(0, NU)
    def _(u):
        st_y(u).wait_send()

        @pl.when(straight(u))
        def _():
            straight_sent(u)

        @pl.when(jnp.logical_not(straight(u)))
        def _():
            line_sent(u)

        @pl.when(u % 4 == 0)
        def _():
            out_x_local(u).wait()

        @pl.when(u % 4 != 0)
        def _():
            k = u % 4
            rows = outx_ref.at[hx(k) * NS + u // 4]
            remote(xg.at[u], rows, ps.at[4, u], pr.at[4, u], dev(f, hx(k))).wait()

    @pl.loop(0, NS)
    def _(s):
        out_q_local(s).wait()
        out_q_from(s, 1).wait()
        out_q_from(s, 2).wait_send()
        q_fwd(s).wait_send()
        out_q_from(s, 3).wait_recv()


def _block(x, g1, g2, w_gate, w_up, w_down, o, w_o, w_qkv):
    tokens, dh = x.shape
    tq = tokens // 4
    ur = tq // NS
    ch = ur // 8
    ff, ko, nqk = w_gate.shape[1], o.shape[1], w_qkv.shape[1]
    jw = ff // NJ
    any_ = pl.BlockSpec(memory_space=pl.ANY)
    dma = pltpu.SemaphoreType.DMA
    scratch = [
        pltpu.VMEM((4, NS, 8, ch, dh), BF),
        pltpu.VMEM((NS, ur, 4 * dh), BF),
        pltpu.VMEM((4, 1, dh), F32),
        pltpu.VMEM((4, 1, dh), F32),
        pltpu.VMEM((NJ, 4, dh, jw), BF),
        pltpu.VMEM((NJ, 4, dh, jw), BF),
        pltpu.VMEM((4, ff, dh), BF),
        pltpu.VMEM((4, ko, dh), BF),
        pltpu.VMEM((4, dh, nqk), BF),
        pltpu.VMEM((NS, ur, ko), BF),
        pltpu.VMEM((NS, ur, ff), BF),
        pltpu.VMEM((NU, 8, ch, dh), F32),
        pltpu.VMEM((NU, 4, ch, dh), F32),
        pltpu.VMEM((NU, 3, ch, dh), F32),
        pltpu.VMEM((NU, 3, ch, dh), F32),
        pltpu.VMEM((ND, 3, ch, dh), F32),
        pltpu.VMEM((NU, 2, 4, ch, dh), BF),
        pltpu.VMEM((4, ur, dh), BF),
        pltpu.VMEM((NS, ur, nqk), BF),
        dma((15,)),
        dma((2, 4)), dma((2, 4)),
        dma((11,)), dma((11,)),
        dma((3, 2, NJ)), dma((3, 2, NJ)),
        dma((3, 3)), dma((3, 3)),
        dma((STAGES, NU)), dma((STAGES, NU)),
        dma((2, NU, 4)), dma((NU, 4)),
        dma((2, ND, 4)), dma((2, ND, 4)),
        dma((4, NS)), dma((4, NS)),
    ]
    outx, outq = pl.pallas_call(
        functools.partial(_kernel, 4 * dh),
        name="block",
        out_shape=(pltpu.VMEM((4 * NS, 2, 4, ch, dh), BF),
                   pltpu.VMEM((4 * NS, ur, nqk), BF)),
        in_specs=[any_] * 9,
        out_specs=(any_, any_),
        scratch_shapes=scratch,
        compiler_params=pltpu.CompilerParams(collective_id=0, has_side_effects=True,
                                             vmem_limit_bytes=56 * 2**20),
    )(x.reshape(4, NS, 8, ch, dh), g1.reshape(1, dh), g2.reshape(1, dh), w_gate, w_up, w_down,
      o.reshape(4, NS, ur, ko), w_o, w_qkv)
    return outx.reshape(tokens, dh), outq.reshape(tokens, nqk)


def solution(mesh):
    in_specs = (P(None, 'h'), P('h'), P('h'), P('h', 'f'), P('h', 'f'), P('f', 'h'),
                P(None, 'f'), P('f', 'h'), P('h', 'f'))
    return jax.shard_map(_block, mesh=mesh, in_specs=in_specs,
                         out_specs=(P(None, 'h'), P(None, 'f')), check_vma=False)
```

```python
import functools

import jax
import jax.numpy as jnp
from jax import lax
from jax.experimental import pallas as pl
from jax.experimental.pallas import tpu as pltpu
from jax.sharding import PartitionSpec as P

EPS = 1e-6
BF, F32 = jnp.bfloat16, jnp.float32
MESH = pl.DeviceIdType.MESH

NS = 8
NU = 32
NE = 3
ND = 4
NJ = 4
STAGES = 5


def _dot(a, b):
    return jnp.dot(a, b, preferred_element_type=F32)


def _kernel(d_model, x_ref, g1_ref, g2_ref, wg_ref, wu_ref, wd_ref, o_ref, wo_ref, wq_ref,
            outx_ref, outq_ref,
            xt, n, g1b, g2b, wg, wu, wd, wo, wq, ot, a, yb, yr, upr, dnr, dbuf, xg, nq, qb,
            loc, gs, gr, xs, xr, ws, wr, bs, br, ps, pr, zs, zr, ds, dr, qs, qr):
    f, h = lax.axis_index('f'), lax.axis_index('h')
    z, y = f // 2, f % 2
    xx, c = h // 2, h % 2

    def hx(k):
        return 2 * ((xx + k // 2) % 2) + (c + k % 2) % 2

    def dev(ff, hh):
        return (ff, hh)

    ypeer = dev(z * 2 + (1 - y), h)
    above, below = dev((f + 2) % 8, h), dev((f + 6) % 8, h)
    core, across = dev(f, hx(1)), dev(f, hx(2))

    def remote(src, dst, ssem, rsem, to):
        return pltpu.make_async_remote_copy(src_ref=src, dst_ref=dst, send_sem=ssem, recv_sem=rsem,
                                            device_id=to, device_id_type=MESH)

    bar = pltpu.get_barrier_semaphore()
    for k in range(1, 4):
        pl.semaphore_signal(bar, inc=1, device_id=dev(f, hx(k)), device_id_type=MESH)
    for i in range(1, 8):
        pl.semaphore_signal(bar, inc=1, device_id=dev((f + i) % 8, h), device_id_type=MESH)
    pl.semaphore_wait(bar, 10)

    jw = wg.shape[-1]

    def wcols(ref, j):
        return ref.at[:, pl.ds(j * jw, jw)]


    def x_cross(k):
        return remote(x_ref.at[hx(k), f], xt.at[h, f],
                      xs.at[k], xr.at[k], dev(f, hx(k)))

    x_core = remote(x_ref.at[hx(1)], xt.at[h], xs.at[1], xr.at[1], core)
    x_cross(2).start()
    x_cross(3).start()
    gcopies = []
    for k in range(1, 4):
        gcopies.append(remote(g1_ref, g1b.at[h], gs.at[0, k], gr.at[0, k], dev(f, hx(k))))
        gcopies.append(remote(g2_ref, g2b.at[h], gs.at[1, k], gr.at[1, k], dev(f, hx(k))))
    for cp in gcopies:
        cp.start()
    x_core.start()

    def w_send(i, j, to, lane):
        src, dst = ((wg_ref, wg), (wu_ref, wu))[i]
        return remote(wcols(src, j), dst.at[j, h], ws.at[lane, i, j], wr.at[lane, i, j], to)

    def w_fwd(i, j):
        dst = (wg, wu)[i]
        return remote(dst.at[j, hx(2)], dst.at[j, hx(2)], ws.at[2, i, j], wr.at[2, i, j], core)

    big = ((wo_ref, wo), (wd_ref, wd), (wq_ref, wq))

    def b_send(i, to, lane):
        return remote(big[i][0], big[i][1].at[h], bs.at[lane, i], br.at[lane, i], to)

    def b_fwd(i):
        dst = big[i][1]
        return remote(dst.at[hx(2)], dst.at[hx(2)], bs.at[2, i], br.at[2, i], core)

    for j in range(NJ):
        for i in range(2):
            w_send(i, j, across, 0).start()
    for i in range(3):
        b_send(i, across, 0).start()

    lcopies = [pltpu.make_async_copy(x_ref.at[h], xt.at[h], loc.at[0]),
               pltpu.make_async_copy(g1_ref, g1b.at[h], loc.at[1]),
               pltpu.make_async_copy(g2_ref, g2b.at[h], loc.at[2]),
               pltpu.make_async_copy(o_ref.at[h], ot, loc.at[3])]
    for i in range(3):
        lcopies.append(pltpu.make_async_copy(big[i][0], big[i][1].at[h], loc.at[4 + i]))
    for j in range(NJ):
        lcopies.append(pltpu.make_async_copy(wcols(wg_ref, j), wg.at[j, h], loc.at[7 + 2 * j]))
        lcopies.append(pltpu.make_async_copy(wcols(wu_ref, j), wu.at[j, h], loc.at[8 + 2 * j]))
    for cp in lcopies:
        cp.start()
    for j in range(NJ):
        for i in range(2):
            w_send(i, j, core, 1).start()
    for i in range(3):
        b_send(i, core, 1).start()

    x_cross(2).wait_recv()
    x_cross(3).wait_recv()
    oth = pl.ds(2 * (1 - xx), 2)

    def x_z(i):
        view = xt.at[oth, f]
        return remote(view, view, xs.at[3 + i], xr.at[3 + i], dev((f + 2 * i) % 8, h))

    def x_y(i):
        src = (f + 8 - 2 * i) % 8
        view = xt.at[oth, src]
        return remote(view, view, xs.at[7 + i], xr.at[7 + i], ypeer)

    for i in (1, 3, 2):
        x_z(i).start()
    x_y(0).start()
    for i in (1, 3, 2):
        x_z(i).wait_recv()
        x_y(i).start()

    for i in range(2):
        w_send(i, 0, across, 0).wait_recv()
        w_fwd(i, 0).start()

    for cp in lcopies:
        cp.wait()
    for cp in gcopies:
        cp.wait_recv()
    x_core.wait_recv()
    for i in range(4):
        x_y(i).wait_recv()

    dh = xt.shape[-1]
    urows = 8 * xt.shape[3]

    @pl.loop(0, NS)
    def _(s):
        blocks = [xt[b, s].reshape(urows, dh).astype(F32) for b in range(4)]
        ss = functools.reduce(jnp.add, [jnp.sum(v * v, axis=-1, keepdims=True) for v in blocks])
        r = lax.rsqrt(ss / d_model + EPS)
        for b in range(4):
            n[s, :, b * dh:(b + 1) * dh] = (blocks[b] * r * g1b[b]).astype(BF)

    for j in range(NJ):
        for i in range(2):
            if j > 0:
                w_send(i, j, across, 0).wait_recv()
                w_fwd(i, j).start()
        for i in range(2):
            w_send(i, j, core, 1).wait_recv()
            w_fwd(i, j).wait_recv()
        wgj = wg.at[j]
        wuj = wu.at[j]

        @pl.loop(0, NS // 2)
        def _(i):
            ns = n[pl.ds(2 * i, 2)].reshape(2 * urows, 4 * dh)
            gt = _dot(ns, wgj[...].reshape(4 * dh, jw))
            up = _dot(ns, wuj[...].reshape(4 * dh, jw))
            v = (jax.nn.silu(gt) * up).astype(BF)
            a[pl.ds(2 * i, 2), :, j * jw:(j + 1) * jw] = v.reshape(2, urows, jw)

    for i in range(3):
        b_send(i, core, 1).wait_recv()

    def st_y(u):
        return remote(yb.at[u, pl.ds((1 - y) * 4, 4)], yr.at[u], ps.at[0, u], pr.at[0, u], ypeer)

    def st_up(u, zz):
        return remote(yb.at[u, pl.ds(y * 4 + zz + 1, 3 - zz)], upr.at[u, pl.ds(zz, 3 - zz)],
                      ps.at[1, u], pr.at[1, u], above)

    def st_dn(u, zz):
        return remote(yb.at[u, pl.ds(y * 4, zz)], dnr.at[u, pl.ds(0, zz)],
                      ps.at[2, u], pr.at[2, u], below)

    def ag_y(u):
        v = xg.at[u, y, pl.ds(z, 1)]
        return remote(v, v, ps.at[3, u], pr.at[3, u], ypeer)

    def ag_z(u, src, way):
        v = xg.at[u, :, pl.ds(src, 1)]
        return remote(v, v, zs.at[way, u, src], zr.at[u, src], (above, below)[way])

    def out_x(u, to_h):
        return remote(xg.at[u], outx_ref.at[h * NS + u // 4], ps.at[4, u], pr.at[4, u], dev(f, to_h))

    def out_x_local(u):
        return pltpu.make_async_copy(xg.at[u], outx_ref.at[h * NS + u // 4], ps.at[4, u])

    def out_q(s, k):
        return remote(qb.at[s], outq_ref.at[h * NS + s], qs.at[k, s], qr.at[k, s], dev(f, hx(k)))

    def out_q_local(s):
        return pltpu.make_async_copy(qb.at[s], outq_ref.at[h * NS + s], qs.at[0, s])

    def at(t, lag, fn, lo=0, hi=NU):
        i = t - lag

        @pl.when((i >= lo) & (i < hi))
        def _():
            p = i // 2
            q = (p + NS - NE) // NS
            far = q % 2
            s = p - NE * q - (NS - 2 * NE) * (q // 2)
            fn(4 * s + 2 * far + i % 2)

    def p_compute(u):
        s, b = u // 4, hx(u % 4)

        @pl.when(u == 2)
        def _():
            for i in range(2):
                b_send(i, across, 0).wait_recv()
                b_fwd(i).start()

        @pl.when(u == 3)
        def _():
            for i in range(2):
                b_fwd(i).wait_recv()

        v = _dot(a[s], wd[b]) + _dot(ot[s], wo[b])
        yb[u] = v.reshape(yb.shape[1:])
        st_y(u).start()

    def send_up(u, zz):
        @pl.when(z == zz)
        def _():
            if zz > 0:
                st_up(u, zz - 1).wait_recv()
                for q in range(zz + 1, 4):
                    yb[u, y * 4 + q] = yb[u, y * 4 + q] + upr[u, q - 1]
            st_up(u, zz).start()

    def send_dn(u, zz):
        @pl.when(z == zz)
        def _():
            if zz < 3:
                st_dn(u, zz + 1).wait_recv()
                for q in range(zz):
                    yb[u, y * 4 + q] = yb[u, y * 4 + q] + dnr[u, q]
            st_dn(u, zz).start()

    def p_y(u):
        st_y(u).wait_recv()
        rows = pl.ds(y * 4, 4)
        yb[u, rows] = yb[u, rows] + yr[u]
        send_up(u, 0)
        send_dn(u, 3)

    def p_h2(u):
        send_up(u, 1)
        send_dn(u, 2)

    def p_h3(u):
        send_up(u, 2)
        send_dn(u, 1)

    def p_fin(u):
        s, b = u // 4, hx(u % 4)
        own = xt[b, s, y * 4 + z].astype(F32)

        @pl.when(z == 0)
        def _():
            st_dn(u, 1).wait_recv()
            xg[u, y, 0] = (own + (yb[u, y * 4] + dnr[u, 0])).astype(BF)

        @pl.when(z == 3)
        def _():
            st_up(u, 2).wait_recv()
            xg[u, y, 3] = (own + (yb[u, y * 4 + 3] + upr[u, 2])).astype(BF)

        @pl.when((z == 1) | (z == 2))
        def _():
            v = yb[u, y * 4 + z] + upr[u, z - 1] + dnr[u, z]
            xg[u, y, z] = (own + v).astype(BF)

        ag_y(u).start()

    def p_g1(u):
        @pl.when(u == 3)
        def _():
            b_send(2, across, 0).wait_recv()
            b_fwd(2).start()

        ag_y(u).wait_recv()

        @pl.when(z < 3)
        def _():
            ag_z(u, z, 0).start()

        @pl.when(z > 0)
        def _():
            ag_z(u, z, 1).start()

    def p_fwd(u, d):
        @pl.when(z >= d)
        def _():
            ag_z(u, z - d, 0).wait_recv()

        @pl.when((z >= d) & (z < 3))
        def _():
            ag_z(u, z - d, 0).start()

        @pl.when(z + d <= 3)
        def _():
            ag_z(u, z + d, 1).wait_recv()

        @pl.when((z + d <= 3) & (z > 0))
        def _():
            ag_z(u, z + d, 1).start()

    def p_g2(u):
        p_fwd(u, 1)

    def p_g3(u):
        p_fwd(u, 2)

    def done(u):
        return ((u % 4 == 3) & (u < 4 * NE)) | ((u % 4 == 1) & (u >= 4 * NE))

    def p_out(u):
        p_fwd(u, 3)

        @pl.when(u == 3)
        def _():
            b_fwd(2).wait_recv()

        finish(u)

    def nth(u):
        return (u - (NU - 2 * ND)) // 4 * 2 + u % 4

    def d_rs(u, i):
        e = nth(u)
        return remote(yb.at[u, y * 4 + (z + i) % 4], dbuf.at[e, i - 1], ds.at[0, e, i], dr.at[0, e, i],
                      dev((f + 2 * i) % 8, h))

    def d_ag(u, i):
        e = nth(u)
        v = xg.at[u, y, z]
        return remote(v, v, ds.at[1, e, i], dr.at[1, e, i], dev((f + 2 * i) % 8, h))

    def d_agy(u):
        return remote(xg.at[u, y], xg.at[u, y], ps.at[3, u], pr.at[3, u], ypeer)

    def d_y(u):
        st_y(u).wait_recv()
        rows = pl.ds(y * 4, 4)
        yb[u, rows] = yb[u, rows] + yr[u]
        for i in (2, 1, 3):
            d_rs(u, i).start()

    def d_fin(u):
        s, b, e = u // 4, hx(u % 4), nth(u)
        for i in range(1, 4):
            d_rs(u, i).wait_recv()
        v = (yb[u, y * 4 + z] + dbuf[e, 0]) + (dbuf[e, 1] + dbuf[e, 2])
        xg[u, y, z] = (xt[b, s, y * 4 + z].astype(F32) + v).astype(BF)
        for i in (2, 1, 3):
            d_ag(u, i).start()

    def d_g(u):
        for i in range(1, 4):
            d_ag(u, i).wait_recv()
        d_agy(u).start()

    def d_out(u):
        d_agy(u).wait_recv()
        finish(u)

    def finish(u):
        @pl.when(u % 4 == 0)
        def _():
            out_x_local(u).start()

        @pl.when(u % 4 != 0)
        def _():
            out_x(u, hx(u % 4)).start()

        @pl.when(done(u))
        def _():
            s = u // 4
            blocks = [xg[4 * s + k].reshape(urows, dh).astype(F32) for k in range(4)]
            ss = functools.reduce(jnp.add, [jnp.sum(v * v, axis=-1, keepdims=True) for v in blocks])
            r = lax.rsqrt(ss / d_model + EPS)
            for k in range(4):
                nq[k] = (blocks[k] * r * g2b[hx(k)]).astype(BF)
            acc = functools.reduce(jnp.add, [_dot(nq[k], wq[hx(k)]) for k in range(4)])
            qb[s] = acc.astype(BF)
            for k in (2, 1):
                out_q(s, k).start()
            out_q_local(s).start()

    def out_q_from(s, k):
        rows = outq_ref.at[hx(k) * NS + s]
        return remote(qb.at[s], rows, qs.at[k, s], qr.at[k, s], dev(f, hx(k)))

    def q_fwd(s):
        rows = outq_ref.at[hx(2) * NS + s]
        return remote(rows, rows, qs.at[3, s], qr.at[3, s], core)

    def hand_q(s):
        out_q_from(s, 2).wait_recv()
        q_fwd(s).start()

    def p_q(u):
        @pl.when(done(u))
        def _():
            hand_q(u // 4)

    def prologue_sent():
        for cp in gcopies:
            cp.wait_send()
        x_core.wait_send()
        x_cross(2).wait_send()
        x_cross(3).wait_send()
        for i in range(4):
            x_y(i).wait_send()
        for i in range(1, 4):
            x_z(i).wait_send()
        for j in range(NJ):
            for i in range(2):
                w_send(i, j, across, 0).wait_send()
                w_send(i, j, core, 1).wait_send()
                w_fwd(i, j).wait_send()
        for i in range(3):
            b_send(i, across, 0).wait_send()
            b_send(i, core, 1).wait_send()
            b_fwd(i).wait_send()

    def line_sent(u):
        st_y(u).wait_send()
        for zz in range(3):
            @pl.when(z == zz)
            def _():
                st_up(u, zz).wait_send()

            @pl.when(z == zz + 1)
            def _():
                st_dn(u, zz + 1).wait_send()

        ag_y(u).wait_send()
        for d in range(3):
            @pl.when((z >= d) & (z < 3))
            def _():
                ag_z(u, z - d, 0).wait_send()

            @pl.when((z + d <= 3) & (z > 0))
            def _():
                ag_z(u, z + d, 1).wait_send()

    def straight_sent(u):
        st_y(u).wait_send()
        for i in range(1, 4):
            d_rs(u, i).wait_send()
            d_ag(u, i).wait_send()
        d_agy(u).wait_send()

    @pl.loop(0, NU + 9)
    def _(t):
        at(t, 0, p_compute)
        for lag, fn in ((2, p_y), (4, p_h2), (6, p_h3), (7, p_fin), (9, p_g1), (10, p_g2), (12, p_g3),
                        (13, p_out)):
            at(t, lag, fn, hi=NU - ND)
        for lag, fn in ((2, d_y), (4, d_fin), (6, d_g), (8, d_out)):
            at(t, lag, fn, lo=NU - ND)
        at(t, 20, line_sent)
        at(t, 22, p_q)

        @pl.when(t == NU - 4)
        def _():
            prologue_sent()

    for s in range(NE, NS):
        hand_q(s)

    @pl.loop(NU + 9, NU + 20)
    def _(t):
        at(t, 20, line_sent, hi=NU - ND)
        at(t, 20, straight_sent, lo=NU - ND)

    @pl.loop(0, NU)
    def _(u):
        @pl.when(u % 4 == 0)
        def _():
            out_x_local(u).wait()

        @pl.when(u % 4 != 0)
        def _():
            k = u % 4
            rows = outx_ref.at[hx(k) * NS + u // 4]
            remote(xg.at[u], rows, ps.at[4, u], pr.at[4, u], dev(f, hx(k))).wait()

    @pl.loop(0, NS)
    def _(s):
        out_q_local(s).wait()
        out_q_from(s, 1).wait()
        out_q_from(s, 2).wait_send()
        q_fwd(s).wait_send()
        out_q_from(s, 3).wait_recv()


def _block(x, g1, g2, w_gate, w_up, w_down, o, w_o, w_qkv):
    tokens, dh = x.shape
    tq = tokens // 4
    ur = tq // NS
    ch = ur // 8
    ff, ko, nqk = w_gate.shape[1], o.shape[1], w_qkv.shape[1]
    jw = ff // NJ
    any_ = pl.BlockSpec(memory_space=pl.ANY)
    dma = pltpu.SemaphoreType.DMA
    scratch = [
        pltpu.VMEM((4, NS, 8, ch, dh), BF),
        pltpu.VMEM((NS, ur, 4 * dh), BF),
        pltpu.VMEM((4, 1, dh), F32),
        pltpu.VMEM((4, 1, dh), F32),
        pltpu.VMEM((NJ, 4, dh, jw), BF),
        pltpu.VMEM((NJ, 4, dh, jw), BF),
        pltpu.VMEM((4, ff, dh), BF),
        pltpu.VMEM((4, ko, dh), BF),
        pltpu.VMEM((4, dh, nqk), BF),
        pltpu.VMEM((NS, ur, ko), BF),
        pltpu.VMEM((NS, ur, ff), BF),
        pltpu.VMEM((NU, 8, ch, dh), F32),
        pltpu.VMEM((NU, 4, ch, dh), F32),
        pltpu.VMEM((NU, 3, ch, dh), F32),
        pltpu.VMEM((NU, 3, ch, dh), F32),
        pltpu.VMEM((ND, 3, ch, dh), F32),
        pltpu.VMEM((NU, 2, 4, ch, dh), BF),
        pltpu.VMEM((4, ur, dh), BF),
        pltpu.VMEM((NS, ur, nqk), BF),
        dma((15,)),
        dma((2, 4)), dma((2, 4)),
        dma((11,)), dma((11,)),
        dma((3, 2, NJ)), dma((3, 2, NJ)),
        dma((3, 3)), dma((3, 3)),
        dma((STAGES, NU)), dma((STAGES, NU)),
        dma((2, NU, 4)), dma((NU, 4)),
        dma((2, ND, 4)), dma((2, ND, 4)),
        dma((4, NS)), dma((4, NS)),
    ]
    outx, outq = pl.pallas_call(
        functools.partial(_kernel, 4 * dh),
        name="block",
        out_shape=(pltpu.VMEM((4 * NS, 2, 4, ch, dh), BF),
                   pltpu.VMEM((4 * NS, ur, nqk), BF)),
        in_specs=[any_] * 9,
        out_specs=(any_, any_),
        scratch_shapes=scratch,
        compiler_params=pltpu.CompilerParams(collective_id=0, has_side_effects=True,
                                             vmem_limit_bytes=56 * 2**20),
    )(x.reshape(4, NS, 8, ch, dh), g1.reshape(1, dh), g2.reshape(1, dh), w_gate, w_up, w_down,
      o.reshape(4, NS, ur, ko), w_o, w_qkv)
    return outx.reshape(tokens, dh), outq.reshape(tokens, nqk)


def solution(mesh):
    in_specs = (P(None, 'h'), P('h'), P('h'), P('h', 'f'), P('h', 'f'), P('f', 'h'),
                P(None, 'f'), P('f', 'h'), P('h', 'f'))
    return jax.shard_map(_block, mesh=mesh, in_specs=in_specs,
                         out_specs=(P(None, 'h'), P(None, 'f')), check_vma=False)
```

```python
import functools

import jax
import jax.numpy as jnp
from jax import lax
from jax.experimental import pallas as pl
from jax.experimental.pallas import tpu as pltpu
from jax.sharding import PartitionSpec as P

EPS = 1e-6
BF, F32 = jnp.bfloat16, jnp.float32
MESH = pl.DeviceIdType.MESH

NS = 8
NU = 32
ND = 4
NJ = 4
STAGES = 5


def _dot(a, b):
    return jnp.dot(a, b, preferred_element_type=F32)


def _kernel(d_model, x_ref, g1_ref, g2_ref, wg_ref, wu_ref, wd_ref, o_ref, wo_ref, wq_ref,
            outx_ref, outq_ref,
            xt, n, g1b, g2b, wg, wu, wd, wo, wq, ot, a, yb, yr, upr, dnr, dbuf, xg, nq, qb,
            loc, gs, gr, xs, xr, ws, wr, bs, br, ps, pr, zs, zr, ds, dr, qs, qr):
    f, h = lax.axis_index('f'), lax.axis_index('h')
    z, y = f // 2, f % 2
    xx, c = h // 2, h % 2

    def hx(k):
        return 2 * ((xx + k // 2) % 2) + (c + k % 2) % 2

    def dev(ff, hh):
        return (ff, hh)

    ypeer = dev(z * 2 + (1 - y), h)
    above, below = dev((f + 2) % 8, h), dev((f + 6) % 8, h)
    core, across = dev(f, hx(1)), dev(f, hx(2))

    def remote(src, dst, ssem, rsem, to):
        return pltpu.make_async_remote_copy(src_ref=src, dst_ref=dst, send_sem=ssem, recv_sem=rsem,
                                            device_id=to, device_id_type=MESH)

    bar = pltpu.get_barrier_semaphore()
    for k in range(1, 4):
        pl.semaphore_signal(bar, inc=1, device_id=dev(f, hx(k)), device_id_type=MESH)
    for i in range(1, 8):
        pl.semaphore_signal(bar, inc=1, device_id=dev((f + i) % 8, h), device_id_type=MESH)
    pl.semaphore_wait(bar, 10)

    jw = wg.shape[-1]

    def wcols(ref, j):
        return ref.at[:, pl.ds(j * jw, jw)]


    def x_cross(k):
        return remote(x_ref.at[hx(k), f], xt.at[h, f],
                      xs.at[k], xr.at[k], dev(f, hx(k)))

    x_core = remote(x_ref.at[hx(1)], xt.at[h], xs.at[1], xr.at[1], core)
    x_cross(2).start()
    x_cross(3).start()
    gcopies = []
    for k in range(1, 4):
        gcopies.append(remote(g1_ref, g1b.at[h], gs.at[0, k], gr.at[0, k], dev(f, hx(k))))
        gcopies.append(remote(g2_ref, g2b.at[h], gs.at[1, k], gr.at[1, k], dev(f, hx(k))))
    for cp in gcopies:
        cp.start()
    x_core.start()

    def w_send(i, j, to, lane):
        src, dst = ((wg_ref, wg), (wu_ref, wu))[i]
        return remote(wcols(src, j), dst.at[j, h], ws.at[lane, i, j], wr.at[lane, i, j], to)

    def w_fwd(i, j):
        dst = (wg, wu)[i]
        return remote(dst.at[j, hx(2)], dst.at[j, hx(2)], ws.at[2, i, j], wr.at[2, i, j], core)

    big = ((wo_ref, wo), (wd_ref, wd), (wq_ref, wq))

    def b_send(i, to, lane):
        return remote(big[i][0], big[i][1].at[h], bs.at[lane, i], br.at[lane, i], to)

    def b_fwd(i):
        dst = big[i][1]
        return remote(dst.at[hx(2)], dst.at[hx(2)], bs.at[2, i], br.at[2, i], core)

    for j in range(NJ):
        for i in range(2):
            w_send(i, j, across, 0).start()
    for i in range(3):
        b_send(i, across, 0).start()

    lcopies = [pltpu.make_async_copy(x_ref.at[h], xt.at[h], loc.at[0]),
               pltpu.make_async_copy(g1_ref, g1b.at[h], loc.at[1]),
               pltpu.make_async_copy(g2_ref, g2b.at[h], loc.at[2]),
               pltpu.make_async_copy(o_ref.at[h], ot, loc.at[3])]
    for i in range(3):
        lcopies.append(pltpu.make_async_copy(big[i][0], big[i][1].at[h], loc.at[4 + i]))
    for j in range(NJ):
        lcopies.append(pltpu.make_async_copy(wcols(wg_ref, j), wg.at[j, h], loc.at[7 + 2 * j]))
        lcopies.append(pltpu.make_async_copy(wcols(wu_ref, j), wu.at[j, h], loc.at[8 + 2 * j]))
    for cp in lcopies:
        cp.start()
    for j in range(NJ):
        for i in range(2):
            w_send(i, j, core, 1).start()
    for i in range(3):
        b_send(i, core, 1).start()

    x_cross(2).wait_recv()
    x_cross(3).wait_recv()
    oth = pl.ds(2 * (1 - xx), 2)

    def x_z(i):
        view = xt.at[oth, f]
        return remote(view, view, xs.at[3 + i], xr.at[3 + i], dev((f + 2 * i) % 8, h))

    def x_y(i):
        src = (f + 8 - 2 * i) % 8
        view = xt.at[oth, src]
        return remote(view, view, xs.at[7 + i], xr.at[7 + i], ypeer)

    for i in (1, 3, 2):
        x_z(i).start()
    x_y(0).start()
    for i in (1, 3, 2):
        x_z(i).wait_recv()
        x_y(i).start()

    for i in range(2):
        w_send(i, 0, across, 0).wait_recv()
        w_fwd(i, 0).start()

    for cp in lcopies:
        cp.wait()
    for cp in gcopies:
        cp.wait_recv()
    x_core.wait_recv()
    for i in range(4):
        x_y(i).wait_recv()

    dh = xt.shape[-1]
    urows = 8 * xt.shape[3]

    @pl.loop(0, NS)
    def _(s):
        blocks = [xt[b, s].reshape(urows, dh).astype(F32) for b in range(4)]
        ss = functools.reduce(jnp.add, [jnp.sum(v * v, axis=-1, keepdims=True) for v in blocks])
        r = lax.rsqrt(ss / d_model + EPS)
        for b in range(4):
            n[s, :, b * dh:(b + 1) * dh] = (blocks[b] * r * g1b[b]).astype(BF)

    for j in range(NJ):
        for i in range(2):
            if j > 0:
                w_send(i, j, across, 0).wait_recv()
                w_fwd(i, j).start()
        for i in range(2):
            w_send(i, j, core, 1).wait_recv()
            w_fwd(i, j).wait_recv()
        wgj = wg.at[j]
        wuj = wu.at[j]

        @pl.loop(0, NS // 2)
        def _(i):
            ns = n[pl.ds(2 * i, 2)].reshape(2 * urows, 4 * dh)
            gt = _dot(ns, wgj[...].reshape(4 * dh, jw))
            up = _dot(ns, wuj[...].reshape(4 * dh, jw))
            v = (jax.nn.silu(gt) * up).astype(BF)
            a[pl.ds(2 * i, 2), :, j * jw:(j + 1) * jw] = v.reshape(2, urows, jw)

    for i in range(3):
        b_send(i, core, 1).wait_recv()

    def st_y(u):
        return remote(yb.at[u, pl.ds((1 - y) * 4, 4)], yr.at[u], ps.at[0, u], pr.at[0, u], ypeer)

    def st_up(u, zz):
        return remote(yb.at[u, pl.ds(y * 4 + zz + 1, 3 - zz)], upr.at[u, pl.ds(zz, 3 - zz)],
                      ps.at[1, u], pr.at[1, u], above)

    def st_dn(u, zz):
        return remote(yb.at[u, pl.ds(y * 4, zz)], dnr.at[u, pl.ds(0, zz)],
                      ps.at[2, u], pr.at[2, u], below)

    def ag_y(u):
        v = xg.at[u, y, pl.ds(z, 1)]
        return remote(v, v, ps.at[3, u], pr.at[3, u], ypeer)

    def ag_z(u, src, way):
        v = xg.at[u, :, pl.ds(src, 1)]
        return remote(v, v, zs.at[way, u, src], zr.at[u, src], (above, below)[way])

    def out_x(u, to_h):
        return remote(xg.at[u], outx_ref.at[h * NS + u // 4], ps.at[4, u], pr.at[4, u], dev(f, to_h))

    def out_x_local(u):
        return pltpu.make_async_copy(xg.at[u], outx_ref.at[h * NS + u // 4], ps.at[4, u])

    def out_q(s, k):
        return remote(qb.at[s], outq_ref.at[h * NS + s], qs.at[k, s], qr.at[k, s], dev(f, hx(k)))

    def out_q_local(s):
        return pltpu.make_async_copy(qb.at[s], outq_ref.at[h * NS + s], qs.at[0, s])

    def at(t, lag, fn, lo=0, hi=NU):
        i = t - lag

        @pl.when((i >= lo) & (i < hi))
        def _():
            p = i // 2
            q = (2 * p) // NS
            far = (q + 2) // 3 - q // 3
            s = p - (NS // 2) * ((q + 2) // 3 + q // 3)
            fn(4 * s + 2 * far + i % 2)

    def p_compute(u):
        s, b = u // 4, hx(u % 4)

        @pl.when(u == 2)
        def _():
            for i in range(2):
                b_send(i, across, 0).wait_recv()
                b_fwd(i).start()

        @pl.when(u == 3)
        def _():
            for i in range(2):
                b_fwd(i).wait_recv()

        v = _dot(a[s], wd[b]) + _dot(ot[s], wo[b])
        yb[u] = v.reshape(yb.shape[1:])
        st_y(u).start()

    def send_up(u, zz):
        @pl.when(z == zz)
        def _():
            if zz > 0:
                st_up(u, zz - 1).wait_recv()
                for q in range(zz + 1, 4):
                    yb[u, y * 4 + q] = yb[u, y * 4 + q] + upr[u, q - 1]
            st_up(u, zz).start()

    def send_dn(u, zz):
        @pl.when(z == zz)
        def _():
            if zz < 3:
                st_dn(u, zz + 1).wait_recv()
                for q in range(zz):
                    yb[u, y * 4 + q] = yb[u, y * 4 + q] + dnr[u, q]
            st_dn(u, zz).start()

    def p_y(u):
        st_y(u).wait_recv()
        rows = pl.ds(y * 4, 4)
        yb[u, rows] = yb[u, rows] + yr[u]
        send_up(u, 0)
        send_dn(u, 3)

    def p_h2(u):
        send_up(u, 1)
        send_dn(u, 2)

    def p_h3(u):
        send_up(u, 2)
        send_dn(u, 1)

    def p_fin(u):
        s, b = u // 4, hx(u % 4)
        own = xt[b, s, y * 4 + z].astype(F32)

        @pl.when(z == 0)
        def _():
            st_dn(u, 1).wait_recv()
            xg[u, y, 0] = (own + (yb[u, y * 4] + dnr[u, 0])).astype(BF)

        @pl.when(z == 3)
        def _():
            st_up(u, 2).wait_recv()
            xg[u, y, 3] = (own + (yb[u, y * 4 + 3] + upr[u, 2])).astype(BF)

        @pl.when((z == 1) | (z == 2))
        def _():
            v = yb[u, y * 4 + z] + upr[u, z - 1] + dnr[u, z]
            xg[u, y, z] = (own + v).astype(BF)

        ag_y(u).start()

    def p_g1(u):
        @pl.when(u == 3)
        def _():
            b_send(2, across, 0).wait_recv()
            b_fwd(2).start()

        ag_y(u).wait_recv()

        @pl.when(z < 3)
        def _():
            ag_z(u, z, 0).start()

        @pl.when(z > 0)
        def _():
            ag_z(u, z, 1).start()

    def p_fwd(u, d):
        @pl.when(z >= d)
        def _():
            ag_z(u, z - d, 0).wait_recv()

        @pl.when((z >= d) & (z < 3))
        def _():
            ag_z(u, z - d, 0).start()

        @pl.when(z + d <= 3)
        def _():
            ag_z(u, z + d, 1).wait_recv()

        @pl.when((z + d <= 3) & (z > 0))
        def _():
            ag_z(u, z + d, 1).start()

    def p_g2(u):
        p_fwd(u, 1)

    def p_g3(u):
        p_fwd(u, 2)

    def done(u):
        return ((u % 4 == 3) & (u < NU // 2)) | ((u % 4 == 1) & (u >= NU // 2))

    def straight(u):
        return (u >= NU - 2 * ND) & (u % 4 < 2)

    def p_out(u):
        p_fwd(u, 3)

        @pl.when(u == 3)
        def _():
            b_fwd(2).wait_recv()

        finish(u)

    def nth(u):
        return (u - (NU - 2 * ND)) // 4 * 2 + u % 4

    def d_rs(u, i):
        e = nth(u)
        return remote(yb.at[u, y * 4 + (z + i) % 4], dbuf.at[e, i - 1], ds.at[0, e, i], dr.at[0, e, i],
                      dev((f + 2 * i) % 8, h))

    def d_ag(u, i):
        e = nth(u)
        v = xg.at[u, y, z]
        return remote(v, v, ds.at[1, e, i], dr.at[1, e, i], dev((f + 2 * i) % 8, h))

    def d_agy(u):
        return remote(xg.at[u, y], xg.at[u, y], ps.at[3, u], pr.at[3, u], ypeer)

    def d_y(u):
        st_y(u).wait_recv()
        rows = pl.ds(y * 4, 4)
        yb[u, rows] = yb[u, rows] + yr[u]
        for i in (2, 1, 3):
            d_rs(u, i).start()

    def d_fin(u):
        s, b, e = u // 4, hx(u % 4), nth(u)
        for i in range(1, 4):
            d_rs(u, i).wait_recv()
        v = (yb[u, y * 4 + z] + dbuf[e, 0]) + (dbuf[e, 1] + dbuf[e, 2])
        xg[u, y, z] = (xt[b, s, y * 4 + z].astype(F32) + v).astype(BF)
        for i in (2, 1, 3):
            d_ag(u, i).start()

    def d_g(u):
        for i in range(1, 4):
            d_ag(u, i).wait_recv()
        d_agy(u).start()

    def d_out(u):
        d_agy(u).wait_recv()
        finish(u)

    def finish(u):
        @pl.when(u % 4 == 0)
        def _():
            out_x_local(u).start()

        @pl.when(u % 4 != 0)
        def _():
            out_x(u, hx(u % 4)).start()

        @pl.when(done(u))
        def _():
            s = u // 4
            blocks = [xg[4 * s + k].reshape(urows, dh).astype(F32) for k in range(4)]
            ss = functools.reduce(jnp.add, [jnp.sum(v * v, axis=-1, keepdims=True) for v in blocks])
            r = lax.rsqrt(ss / d_model + EPS)
            for k in range(4):
                nq[k] = (blocks[k] * r * g2b[hx(k)]).astype(BF)
            acc = functools.reduce(jnp.add, [_dot(nq[k], wq[hx(k)]) for k in range(4)])
            qb[s] = acc.astype(BF)
            for k in (2, 1):
                out_q(s, k).start()
            out_q_local(s).start()

    def out_q_from(s, k):
        rows = outq_ref.at[hx(k) * NS + s]
        return remote(qb.at[s], rows, qs.at[k, s], qr.at[k, s], dev(f, hx(k)))

    def q_fwd(s):
        rows = outq_ref.at[hx(2) * NS + s]
        return remote(rows, rows, qs.at[3, s], qr.at[3, s], core)

    def p_q(u):
        @pl.when(done(u))
        def _():
            out_q_from(u // 4, 2).wait_recv()
            q_fwd(u // 4).start()

    @pl.loop(0, NU + 18)
    def _(t):
        at(t, 0, p_compute)
        for lag, fn in ((2, p_y), (4, p_h2), (6, p_h3), (8, p_fin), (10, p_g1), (11, p_g2), (13, p_g3),
                        (14, p_out), (22, p_q)):
            at(t, lag, fn, hi=NU - ND)
        for lag, fn in ((2, d_y), (4, d_fin), (6, d_g), (8, d_out), (10, p_q)):
            at(t, lag, fn, lo=NU - ND)

    for cp in gcopies:
        cp.wait_send()
    x_core.wait_send()
    x_cross(2).wait_send()
    x_cross(3).wait_send()
    for i in range(4):
        x_y(i).wait_send()
    for i in range(1, 4):
        x_z(i).wait_send()
    for j in range(NJ):
        for i in range(2):
            w_send(i, j, across, 0).wait_send()
            w_send(i, j, core, 1).wait_send()
            w_fwd(i, j).wait_send()
    for i in range(3):
        b_send(i, across, 0).wait_send()
        b_send(i, core, 1).wait_send()
        b_fwd(i).wait_send()

    def line_sent(u):
        for zz in range(3):
            @pl.when(z == zz)
            def _():
                st_up(u, zz).wait_send()

            @pl.when(z == zz + 1)
            def _():
                st_dn(u, zz + 1).wait_send()

        ag_y(u).wait_send()
        for d in range(3):
            @pl.when((z >= d) & (z < 3))
            def _():
                ag_z(u, z - d, 0).wait_send()

            @pl.when((z + d <= 3) & (z > 0))
            def _():
                ag_z(u, z + d, 1).wait_send()

    def straight_sent(u):
        for i in range(1, 4):
            d_rs(u, i).wait_send()
            d_ag(u, i).wait_send()
        d_agy(u).wait_send()

    @pl.loop(0, NU)
    def _(u):
        st_y(u).wait_send()

        @pl.when(straight(u))
        def _():
            straight_sent(u)

        @pl.when(jnp.logical_not(straight(u)))
        def _():
            line_sent(u)

        @pl.when(u % 4 == 0)
        def _():
            out_x_local(u).wait()

        @pl.when(u % 4 != 0)
        def _():
            k = u % 4
            rows = outx_ref.at[hx(k) * NS + u // 4]
            remote(xg.at[u], rows, ps.at[4, u], pr.at[4, u], dev(f, hx(k))).wait()

    @pl.loop(0, NS)
    def _(s):
        out_q_local(s).wait()
        out_q_from(s, 1).wait()
        out_q_from(s, 2).wait_send()
        q_fwd(s).wait_send()
        out_q_from(s, 3).wait_recv()


def _block(x, g1, g2, w_gate, w_up, w_down, o, w_o, w_qkv):
    tokens, dh = x.shape
    tq = tokens // 4
    ur = tq // NS
    ch = ur // 8
    ff, ko, nqk = w_gate.shape[1], o.shape[1], w_qkv.shape[1]
    jw = ff // NJ
    any_ = pl.BlockSpec(memory_space=pl.ANY)
    dma = pltpu.SemaphoreType.DMA
    scratch = [
        pltpu.VMEM((4, NS, 8, ch, dh), BF),
        pltpu.VMEM((NS, ur, 4 * dh), BF),
        pltpu.VMEM((4, 1, dh), F32),
        pltpu.VMEM((4, 1, dh), F32),
        pltpu.VMEM((NJ, 4, dh, jw), BF),
        pltpu.VMEM((NJ, 4, dh, jw), BF),
        pltpu.VMEM((4, ff, dh), BF),
        pltpu.VMEM((4, ko, dh), BF),
        pltpu.VMEM((4, dh, nqk), BF),
        pltpu.VMEM((NS, ur, ko), BF),
        pltpu.VMEM((NS, ur, ff), BF),
        pltpu.VMEM((NU, 8, ch, dh), F32),
        pltpu.VMEM((NU, 4, ch, dh), F32),
        pltpu.VMEM((NU, 3, ch, dh), F32),
        pltpu.VMEM((NU, 3, ch, dh), F32),
        pltpu.VMEM((ND, 3, ch, dh), F32),
        pltpu.VMEM((NU, 2, 4, ch, dh), BF),
        pltpu.VMEM((4, ur, dh), BF),
        pltpu.VMEM((NS, ur, nqk), BF),
        dma((15,)),
        dma((2, 4)), dma((2, 4)),
        dma((11,)), dma((11,)),
        dma((3, 2, NJ)), dma((3, 2, NJ)),
        dma((3, 3)), dma((3, 3)),
        dma((STAGES, NU)), dma((STAGES, NU)),
        dma((2, NU, 4)), dma((NU, 4)),
        dma((2, ND, 4)), dma((2, ND, 4)),
        dma((4, NS)), dma((4, NS)),
    ]
    outx, outq = pl.pallas_call(
        functools.partial(_kernel, 4 * dh),
        name="block",
        out_shape=(pltpu.VMEM((4 * NS, 2, 4, ch, dh), BF),
                   pltpu.VMEM((4 * NS, ur, nqk), BF)),
        in_specs=[any_] * 9,
        out_specs=(any_, any_),
        scratch_shapes=scratch,
        compiler_params=pltpu.CompilerParams(collective_id=0, has_side_effects=True,
                                             vmem_limit_bytes=56 * 2**20),
    )(x.reshape(4, NS, 8, ch, dh), g1.reshape(1, dh), g2.reshape(1, dh), w_gate, w_up, w_down,
      o.reshape(4, NS, ur, ko), w_o, w_qkv)
    return outx.reshape(tokens, dh), outq.reshape(tokens, nqk)


def solution(mesh):
    in_specs = (P(None, 'h'), P('h'), P('h'), P('h', 'f'), P('h', 'f'), P('f', 'h'),
                P(None, 'f'), P('f', 'h'), P('h', 'f'))
    return jax.shard_map(_block, mesh=mesh, in_specs=in_specs,
                         out_specs=(P(None, 'h'), P(None, 'f')), check_vma=False)
```
